32 devices in a mesh: tx: 8 (over y, x, core), ty: 4 (over z).
Axes of the slice: x: 2, y: 2, z: 4, core: 2. Of those that a mesh axis runs over, the one named last changes fastest.
Arguments:
- potential: float32 [512, 1024], P('tx', 'ty'), may hold values from -6 to 6
- elevation: float32 [512, 1024], P('tx', 'ty'), may hold values from -5 to 5
- normal_flux: float32 [512, 1024], P('tx', 'ty'), may hold values from -4 to 4
- box_owner: int32 [512, 1024], P('tx', 'ty'), may hold values from 0 to 31, as said below
- box_place: int32 [512, 1024], P('tx', 'ty'), may hold values from 0 to 16383, as said below
- near_boxes: int32 [4096, 8], P(('tx', 'ty')), may hold values from 0 to 4095, as said below
Outputs:
- elevation_rate: float32 [512, 1024], P('tx', 'ty')
- potential_rate: float32 [512, 1024], P('tx', 'ty')
The draws below stay inside these ranges and needn't reach their ends.
Inputs may be any that keep to these rules, and one draw needn't show every extreme that they name: Devices are numbered p times the number of ty devices plus q, for position p along tx and q along ty. box_owner 64 * 256 + box_place is a permutation of the 524288 positions. A node in the tile of device (p, q) has its owner at position (p or p - 1, q or q - 1) along tx and ty, taken modulo the axis sizes. The nodes of one tile with one owner other than the tile's own device number at most 6400, and exactly 6400 for some pair of devices. `box_place`: see box_owner. near_boxes[b, 0] = b; the other entries are distinct boxes other than b, each within 128 of b in box number, a distance of exactly 128 occurring in both directions.
All inputs are finite; a program needn't handle non-finite values.
Results may differ from the reference program's by a relative error of at most 0.0049.
Values sent between devices are 32-bit elements; how exact they have to be, the bound alone decides.
No kernel may reach another device: no remote copies, remote signals or barrier semaphores. Data moves between devices by JAX's collectives and lax.ppermute only.
A program may use at most 128 MiB of HBM per device.

```python
import math
import jax
import jax.numpy as jnp
from jax import lax

TR = 64
TC = 256
NEAR = 8
NX = 512
NY = 1024


def slot_table(key):
    tile_count_across = NX // TR
    count_ty = NY // TC
    jitter_rows = TR // 8
    jitter_cols = TC // 8
    row_shift = TR // 2 + jax.random.randint(jax.random.fold_in(key, 11), (NY,), 0, jitter_rows + 1)
    row_shift = row_shift.at[:TC].set(TR // 2 + jitter_rows)
    rel_all = (jnp.arange(NX, dtype=jnp.int32)[:, None] - row_shift[None, :]) % NX
    owner_row = rel_all // TR
    rel_row = rel_all % TR
    col_shift = TC // 2 + jax.random.randint(jax.random.fold_in(key, 12), (tile_count_across, TR), 0, jitter_cols + 1)
    col_shift = col_shift.at[tile_count_across - 1, :].set(TC // 2 + jitter_cols)
    local_shift = col_shift[owner_row, rel_row]
    rel_col_all = (jnp.arange(NY, dtype=jnp.int32)[None, :] - local_shift) % NY
    owner_col = rel_col_all // TC
    rel_col = rel_col_all % TC
    owner_grid = owner_row * count_ty + owner_col
    box_local = rel_row // 8 * (TC // 16) + rel_col // 16
    place_grid = box_local * 128 + rel_row % 8 * 16 + rel_col % 16
    return (owner_grid.astype(jnp.int32), place_grid.astype(jnp.int32))


def draw_box_owner(key, part):
    return slot_table(jax.random.fold_in(key, 5))[0]


def draw_box_place(key, part):
    return slot_table(jax.random.fold_in(key, 5))[1]


def draw_near_boxes(key, part):
    box_dev = TR * TC // 128
    box_count = box_dev * (NX // TR) * (NY // TC)
    width = 2 * box_dev
    offsets = jnp.concatenate([jnp.arange(-box_dev, 0, dtype=jnp.int32), jnp.arange(1, box_dev + 1, dtype=jnp.int32)])
    scores = jax.random.randint(jax.random.fold_in(key, 21), (box_count, width), 0, 2 ** 18) * width + jnp.arange(width, dtype=jnp.int32)[None, :]
    targets = jnp.arange(box_count, dtype=jnp.int32)[:, None] + offsets[None, :]
    inside = (targets >= 0) & (targets < box_count)
    scores = jnp.where(inside, scores, -1)
    scores = scores.at[0, width - 1].set(2 ** 30).at[box_count - 1, 0].set(2 ** 30)
    top_values, chosen = lax.top_k(scores, NEAR - 1)
    picked = jnp.take_along_axis(targets, chosen, 1)
    return jnp.concatenate([jnp.arange(box_count, dtype=jnp.int32)[:, None], picked], 1).astype(jnp.int32)


def steps_of(rng, shape, cuts, smallest, high):
    def one(position, blocks):
        draws = jax.random.uniform(jax.random.fold_in(jax.random.fold_in(rng, 6), position), (blocks,), jnp.float32, smallest / len(cuts), high / len(cuts))
        return jnp.repeat(jnp.exp(draws), shape[position] // blocks).reshape((-1,) + (1,) * (len(shape) - position - 1))

    loudness = one(*cuts[0])
    for cut in cuts[1:]:
        loudness = loudness * one(*cut)
    return loudness


def bell_draw(own_key, shape, spread, limit, split=(), held_as=jnp.bfloat16):
    level = steps_of(own_key, shape, split, -0.22, 0.18) if split else 1.0
    entries = jax.random.normal(own_key, shape, jnp.float32) * spread * level
    return jnp.minimum(jnp.maximum(entries, -limit), limit).astype(held_as)


def setup_inputs(seed: int = 0) -> dict:
    arg_keys = jax.random.split(jax.random.key(seed), 7)
    return {
        "potential": bell_draw(arg_keys[0], (NX, NY), 1.0, 6.0, ((0, 8), (1, 4)), jnp.float32),
        "elevation": bell_draw(arg_keys[1], (NX, NY), 1.0, 5.0, ((0, 8), (1, 4)), jnp.float32),
        "normal_flux": bell_draw(arg_keys[2], (NX, NY), 0.5, 4.0, ((0, 8), (1, 4)), jnp.float32),
        "box_owner": draw_box_owner(jax.random.fold_in(arg_keys[6], 71), 0),
        "box_place": draw_box_place(jax.random.fold_in(arg_keys[6], 71), 0),
        "near_boxes": draw_near_boxes(jax.random.fold_in(arg_keys[6], 71), 0),
    }


def slope(field, axis_id):
    return (jnp.roll(field, 2, axis_id) - 8.0 * jnp.roll(field, 1, axis_id) + 8.0 * jnp.roll(field, -1, axis_id) - jnp.roll(field, -2, axis_id)) / 12.0

def kernel_apply(targets, sources):
    delta_x = targets[0][:, None, :, None] - sources[0][:, :, None, :]
    delta_y = targets[1][:, None, :, None] - sources[1][:, :, None, :]
    delta_z = targets[2][:, None, :, None] - sources[2][:, :, None, :]
    squared = delta_x * delta_x + delta_y * delta_y + delta_z * delta_z + 0.04
    inverse = lax.rsqrt(squared)
    single = inverse.astype(jnp.bfloat16).astype(jnp.float32)
    double = (delta_z * inverse * inverse * inverse).astype(jnp.bfloat16).astype(jnp.float32)
    flux_low = sources[4].astype(jnp.bfloat16).astype(jnp.float32)
    pot_low = sources[3].astype(jnp.bfloat16).astype(jnp.float32)
    first = jnp.einsum('bkts,bks->bt', single, flux_low, precision=lax.Precision.HIGHEST)
    second = jnp.einsum('bkts,bks->bt', double, pot_low, precision=lax.Precision.HIGHEST)
    return (first - second) * (1.0 / math.sqrt(NEAR * 128))

def reference(potential, elevation, normal_flux, box_owner, box_place, near_boxes):
    grid_rows = (jnp.arange(NX, dtype=jnp.int32).astype(jnp.float32) + 0.5) / NX
    grid_cols = (jnp.arange(NY, dtype=jnp.int32).astype(jnp.float32) + 0.5) / NY
    pos_x = jnp.broadcast_to(grid_rows[:, None], (NX, NY))
    pos_y = jnp.broadcast_to(grid_cols[None, :], (NX, NY))
    pos_z = 0.25 * elevation
    node_features = jnp.stack([pos_x, pos_y, pos_z, potential, normal_flux]).reshape(5, NX * NY)
    slots = (box_owner.reshape(NX * NY).astype(jnp.int32) * (TR * TC) + box_place.reshape(NX * NY).astype(jnp.int32)).astype(jnp.int32)
    boxed = jnp.zeros((5, NX * NY), jnp.float32).at[:, slots].set(node_features)
    box_count = NX * NY // 128
    boxed_three = boxed.reshape(5, box_count, 128)
    block_boxes = math.gcd(box_count, 32)

    def near_block(block_id):
        start = block_id * block_boxes
        targets = lax.dynamic_slice_in_dim(boxed_three, start, block_boxes, 1)
        listed = lax.dynamic_slice_in_dim(near_boxes, start, block_boxes, 0).astype(jnp.int32)
        sources = jnp.take(boxed_three, listed, axis=1)
        return kernel_apply(targets, sources)
    near_field = lax.map(near_block, jnp.arange(box_count // block_boxes, dtype=jnp.int32)).reshape(NX * NY)
    vertical = near_field[slots].reshape(NX, NY)
    pot_x = slope(potential, 0)
    pot_y = slope(potential, 1)
    elev_x = slope(elevation, 0)
    elev_y = slope(elevation, 1)
    lift = 1.0 + elev_x * elev_x + elev_y * elev_y
    elevation_rate = vertical * lift - (pot_x * elev_x + pot_y * elev_y)
    potential_rate = -elevation - 0.5 * (pot_x * pot_x + pot_y * pot_y) + 0.5 * vertical * vertical * lift
    return (elevation_rate, potential_rate)
```

```python
import math

import jax
import jax.numpy as jnp
from jax import lax
from jax.experimental import pallas as pl
from jax.experimental.pallas import tpu as pltpu
from jax.sharding import PartitionSpec as P

LANES = 128
WIDE = 256
PIECES = 6
FEATURES = 32
BF16 = jnp.bfloat16
F32 = jnp.float32


def shifted(value, axis, steps):
    count = lax.axis_size(axis)
    pairs = [(source, (source + steps) % count) for source in range(count)]
    return lax.ppermute(value, axis, pairs)


def rounded(value):
    return value.astype(BF16).astype(F32)


def scatter_kernel(first, last, sizes, info, tile, *refs):
    if first:
        acc = refs[0]
    else:
        acc_in, acc = refs[:2]
    rows, cols, high_count, node_rows, node_cols = sizes
    base = info[0].astype(F32)
    off_i = info[1].astype(F32)
    off_j = info[2].astype(F32)
    acc[...] = jnp.zeros(acc.shape, F32) if first else acc_in[...]
    units = [(r, c) for r in range(rows // 8) for c in range(cols // LANES)]

    def split(r, c):
        rel = tile[0, 8 * r : 8 * r + 8, LANES * c : LANES * c + LANES] - base
        high = jnp.floor(rel * (1.0 / WIDE))
        return high, rel - high * WIDE

    flags = []
    for r, c in units:
        high, _ = split(r, c)
        mine = (high >= 0.0) & (high < high_count)
        flags.append(jnp.max(jnp.where(mine, 1.0, 0.0)) > 0.0)

    for (r, c), flag in zip(units, flags):

        @pl.when(flag)
        def _():
            high, low = split(r, c)
            window = (slice(8 * r, 8 * r + 8), slice(LANES * c, LANES * c + LANES))
            z = 0.25 * tile[(1,) + window]
            z_high = rounded(z)
            z_low = z - z_high
            pot = tile[(2,) + window]
            flux = tile[(3,) + window]
            col_index = (lax.broadcasted_iota(jnp.int32, (high_count, LANES), 1) + LANES * c).astype(F32) + off_j
            high_iota = lax.broadcasted_iota(jnp.int32, (high_count, LANES), 0).astype(F32)
            low_iota = lax.broadcasted_iota(jnp.int32, (WIDE, LANES), 0).astype(F32)
            lefts = []
            rights = []
            for s in range(8):

                def row(v):
                    return v[s : s + 1, :]

                hit = high_iota == row(high)
                row_index = jnp.full((1, LANES), 8 * r + s, F32) + off_i
                values = [row_index, col_index, row(z_high), row(z_low), row(pot), row(flux)]
                lefts.append(
                    jnp.concatenate([jnp.where(hit, v, 0.0).astype(BF16) for v in values], axis=0)
                )
                rights.append(jnp.where(low_iota == row(low), 1.0, 0.0).astype(BF16))
            acc[...] += lax.dot_general(
                jnp.concatenate(lefts, axis=1),
                jnp.concatenate(rights, axis=1),
                (((1,), (1,)), ((), ())),
                preferred_element_type=F32,
            )

    if last:
        boxed = refs[-1]
        h = high_count
        row0 = info[3].astype(F32)
        col0 = info[4].astype(F32)
        i = acc[0:h] + row0
        i = jnp.where(i >= node_rows, i - node_rows, i)
        j = acc[h : 2 * h] + col0
        j = jnp.where(j >= node_cols, j - node_cols, j)
        fields = [
            (i + 0.5) / node_rows,
            (j + 0.5) / node_cols,
            acc[2 * h : 3 * h] + acc[3 * h : 4 * h],
            acc[4 * h : 5 * h],
            acc[5 * h : 6 * h],
        ]
        for k, f in enumerate(fields):
            boxed[k, 0:h, :] = f[:, :LANES]
            boxed[k, h : 2 * h, :] = f[:, LANES:]


def scatter(info, tile, acc, last, node_rows, node_cols):
    _, rows, cols = tile.shape
    high_count = rows * cols // WIDE
    first = acc is None
    vmem = pl.BlockSpec(memory_space=pltpu.VMEM)
    smem = pl.BlockSpec(memory_space=pltpu.SMEM)
    out_shape = [jax.ShapeDtypeStruct((PIECES * high_count, WIDE), F32)]
    if last:
        out_shape.append(jax.ShapeDtypeStruct((5, 2 * high_count, LANES), F32))
    args = (info, tile) if first else (info, tile, acc)
    out = pl.pallas_call(
        lambda *refs: scatter_kernel(
            first, last, (rows, cols, high_count, node_rows, node_cols), *refs
        ),
        out_shape=out_shape,
        in_specs=[smem] + [vmem] * (len(args) - 1),
        out_specs=[vmem] * len(out_shape),
        name="scatter_last" if last else "scatter_first" if first else "scatter",
        cost_estimate=pl.CostEstimate(
            flops=2 * PIECES * high_count * WIDE * rows * cols // 2,
            transcendentals=0,
            bytes_accessed=4 * (2 * PIECES * high_count * WIDE + 4 * rows * cols),
        ),
    )(*args)
    return out[1] if last else out[0]


def thirds(value):
    high = rounded(value)
    middle = rounded(value - high)
    return high, middle, value - high - middle


def near_kernel(near, listed, own, lower, upper, out, tfeat, sfeat, smeta, even, odd):
    boxes = out.shape[0]
    scale = 1.0 / math.sqrt(near * LANES)

    def features(ref, group):
        window = (slice(8 * group, 8 * group + 8), slice(None))
        x = ref[(0,) + window]
        y = ref[(1,) + window]
        z = ref[(2,) + window]
        pieces = []
        total = None
        for v in (x, y, z):
            high = rounded(v)
            low = rounded(v - high)
            kept = high + low
            pieces.append((high, low))
            total = kept * kept if total is None else total + kept * kept
        return pieces, total, ref[(3,) + window], ref[(4,) + window]

    zeros = jnp.zeros((8, LANES), F32)
    ones = jnp.ones((8, LANES), F32)

    for which, ref in enumerate((lower, own, upper)):
        for group in range(boxes // 8):
            pieces, total, pot, flux = features(ref, group)
            start = which * boxes + 8 * group
            source = []
            for high, low in pieces:
                source += [-2.0 * high, -2.0 * low, -2.0 * high, -2.0 * low]
            source += list(thirds(total)) + [ones, ones, ones]
            source += [zeros] * (FEATURES - len(source))
            for k, v in enumerate(source):
                sfeat[pl.ds(start * FEATURES + k, 8, stride=FEATURES), :] = v
            z = pieces[2][0] + pieces[2][1]
            smeta[0, start : start + 8, :] = pot
            smeta[1, start : start + 8, :] = pot * z
            smeta[2, start : start + 8, :] = flux
            if which == 1:
                target = []
                for high, low in pieces:
                    target += [high, high, low, low]
                target += [ones, ones, ones] + list(thirds(total + 0.04)) + [z]
                target += [zeros] * (FEATURES - len(target))
                for k, v in enumerate(target):
                    tfeat[pl.ds(8 * group * FEATURES + k, 8, stride=FEATURES), :] = v

    def distances(box, squared, z_ref):
        left = tfeat[pl.ds(pl.multiple_of(box * FEATURES, FEATURES), FEATURES), :].T
        z_ref[...] = jnp.broadcast_to(left[:, 18:19], (LANES, LANES))
        rights = []
        for k in range(near):
            n = listed[box * near + k]
            rights.append(
                sfeat[pl.ds(pl.multiple_of(n * FEATURES, FEATURES), FEATURES), :].astype(BF16)
            )
        squared[...] = jnp.dot(
            left.astype(BF16), jnp.concatenate(rights, axis=1), preferred_element_type=F32
        )

    def apply(box, squared, z_ref):
        metas = []
        for k in range(near):
            n = listed[box * near + k]
            metas.append(
                [jnp.broadcast_to(smeta[m, pl.ds(n, 1), :], (8, LANES)) for m in range(3)]
            )
        parts = []
        for t in range(LANES // 8):
            rows = slice(8 * t, 8 * t + 8)
            z = z_ref[rows, :]
            total = None
            for k in range(near):
                pot, pot_z, flux = metas[k]
                inverse = lax.rsqrt(squared[rows, LANES * k : LANES * k + LANES])
                value = inverse * (flux - (inverse * inverse) * (z * pot - pot_z))
                total = value if total is None else total + value
            parts.append(total)
        summed = jnp.concatenate(parts, axis=0).T
        out[pl.ds(box, 1), :] = jnp.sum(summed, axis=0, keepdims=True) * scale

    (even_sq, even_z), (odd_sq, odd_z) = even, odd
    distances(0, even_sq, even_z)

    def step(i, carry):
        distances(2 * i + 1, odd_sq, odd_z)
        apply(2 * i, even_sq, even_z)
        distances(jnp.minimum(2 * i + 2, boxes - 1), even_sq, even_z)
        apply(2 * i + 1, odd_sq, odd_z)
        return carry

    lax.fori_loop(0, boxes // 2, step, 0)


def near_apply(listed, own, lower, upper, near):
    boxes = own.shape[1]
    vmem = pl.BlockSpec(memory_space=pltpu.VMEM)
    smem = pl.BlockSpec(memory_space=pltpu.SMEM)
    buffers = [pltpu.VMEM((LANES, near * LANES), F32), pltpu.VMEM((LANES, LANES), F32)]

    def kernel(listed, own, lower, upper, out, tfeat, sfeat, smeta, e0, e1, o0, o1):
        near_kernel(near, listed, own, lower, upper, out, tfeat, sfeat, smeta, (e0, e1), (o0, o1))

    pairs = boxes * near * LANES * LANES
    return pl.pallas_call(
        kernel,
        out_shape=jax.ShapeDtypeStruct((boxes, LANES), F32),
        in_specs=[smem] + [vmem] * 3,
        out_specs=vmem,
        scratch_shapes=[
            pltpu.VMEM((boxes * FEATURES, LANES), F32),
            pltpu.VMEM((3 * boxes * FEATURES, LANES), F32),
            pltpu.VMEM((3, 3 * boxes, LANES), F32),
        ]
        + buffers
        + buffers,
        name="near_field",
        cost_estimate=pl.CostEstimate(
            flops=pairs * 2 * FEATURES * 4, transcendentals=pairs, bytes_accessed=4 * 16 * boxes * LANES
        ),
    )(listed, own, lower, upper)


def gather_kernel(bases, slot, own, behind_x, behind_y, behind_xy, out):
    rows, cols = slot.shape
    boxes = own.shape[0]
    half = boxes // 2
    count = boxes * LANES
    tiles = [(r, c) for r in range(rows // 8) for c in range(cols // LANES)]
    lanes = []
    wanted = []
    for r, c in tiles:
        value = slot[8 * r : 8 * r + 8, LANES * c : LANES * c + LANES]
        row = jnp.full((8, LANES), -1, jnp.int32)
        lane = jnp.zeros((8, LANES), jnp.int32)
        for which in range(4):
            rel = value - bases[which].astype(F32)
            inside = (rel >= 0.0) & (rel < count)
            rel = jnp.where(inside, rel, 0.0).astype(jnp.int32)
            box = rel // LANES
            place = (box % 2) * half + box // 2
            row = jnp.where(inside, place + which * boxes, row)
            lane = jnp.where(inside, rel % LANES, lane)
        lanes.append(lane)
        wanted.append(row)
    found = [jnp.zeros((8, LANES), F32) for _ in tiles]
    for which, table in enumerate((own, behind_x, behind_y, behind_xy)):

        def step(g, found):
            for s in range(8):
                index = g * 8 + s
                line = jnp.broadcast_to(table[pl.ds(index, 1), :], (8, LANES))
                found = [
                    jnp.where(w == index + which * boxes, jnp.take_along_axis(line, l, axis=1), f)
                    for w, l, f in zip(wanted, lanes, found)
                ]
            return found

        found = lax.fori_loop(0, boxes // 8, step, found)
    for (r, c), f in zip(tiles, found):
        out[8 * r : 8 * r + 8, LANES * c : LANES * c + LANES] = f


def gather(bases, slot, tables):
    vmem = pl.BlockSpec(memory_space=pltpu.VMEM)
    smem = pl.BlockSpec(memory_space=pltpu.SMEM)
    return pl.pallas_call(
        gather_kernel,
        out_shape=jax.ShapeDtypeStruct(slot.shape, F32),
        in_specs=[smem] + [vmem] * 5,
        out_specs=vmem,
        name="gather",
    )(bases, slot, *tables)


def padded_2(block, sides, width):
    for axis, dim in sides:
        low = shifted(lax.slice_in_dim(block, block.shape[dim] - width, None, axis=dim), axis, 1)
        high = shifted(lax.slice_in_dim(block, 0, width, axis=dim), axis, -1)
        block = jnp.concatenate([low, block, high], axis=dim)
    return block


def surface_slopes(fields):
    padded = padded_2(fields, (("tx", 1), ("ty", 2)), 2)
    middle_cols = padded[:, :, 2:-2]
    along_rows = (
        middle_cols[:, 0:-4] - 8.0 * middle_cols[:, 1:-3] + 8.0 * middle_cols[:, 3:-1] - middle_cols[:, 4:]
    ) / 12.0
    central_rows = padded[:, 2:-2, :]
    along_cols = (
        central_rows[:, :, 0:-4]
        - 8.0 * central_rows[:, :, 1:-3]
        + 8.0 * central_rows[:, :, 3:-1]
        - central_rows[:, :, 4:]
    ) / 12.0
    return (along_rows, along_cols)


def shards(potential, elevation, normal_flux, box_owner, box_place, near_boxes):
    rows, cols = potential.shape
    count_tx = lax.axis_size("tx")
    count_ty = lax.axis_size("ty")
    node_count = rows * cols
    boxes = node_count // LANES
    near = near_boxes.shape[1]
    half = boxes // 2
    assert node_count % WIDE == 0 and cols <= 256 and 2 * rows <= 256
    assert node_count * count_tx * count_ty < 2**24
    p = lax.axis_index("tx")
    q = lax.axis_index("ty")
    rank = p * count_ty + q
    base = rank * node_count

    slot = (box_owner * node_count + box_place).astype(F32)
    tile = jnp.stack([slot, elevation, potential, normal_flux])
    ahead_x = shifted(tile, "tx", -1)
    ahead_y = shifted(tile, "ty", -1)
    ahead_xy = shifted(ahead_y, "tx", -1)

    def info(di, dj):
        return jnp.stack(
            [base, jnp.int32(di * rows), jnp.int32((dj - 1) * cols), p * rows, (q + 1) * cols]
        ).astype(jnp.int32)

    sizes = (rows * count_tx, cols * count_ty)
    acc = scatter(info(0, 0), tile, None, False, *sizes)
    acc = scatter(info(1, 0), ahead_x, acc, False, *sizes)
    acc = scatter(info(0, 1), ahead_y, acc, False, *sizes)
    boxed = scatter(info(1, 1), ahead_xy, acc, True, *sizes)

    total = count_tx * count_ty
    both = ("tx", "ty")
    lower = lax.ppermute(boxed, both, [(i, i + 1) for i in range(total - 1)])
    upper = lax.ppermute(boxed, both, [(i + 1, i) for i in range(total - 1)])

    local = near_boxes - (rank - 1) * boxes
    inner = local % boxes
    listed = (local // boxes) * boxes + (inner % 2) * half + inner // 2
    listed = listed.reshape(half, 2, near).transpose(1, 0, 2).reshape(boxes * near)
    near_value = near_apply(listed, boxed, lower, upper, near)

    behind_x = shifted(near_value, "tx", 1)
    behind_y = shifted(near_value, "ty", 1)
    behind_xy = shifted(behind_x, "ty", 1)
    before_p = (p - 1) % count_tx
    before_q = (q - 1) % count_ty
    bases = (
        jnp.stack([rank, before_p * count_ty + q, p * count_ty + before_q, before_p * count_ty + before_q])
        * node_count
    ).astype(jnp.int32)
    vertical = gather(bases, slot, (near_value, behind_x, behind_y, behind_xy))

    along_rows, along_cols = surface_slopes(tile[1:3])
    elev_x, pot_x = (along_rows[0], along_rows[1])
    elev_y, pot_y = (along_cols[0], along_cols[1])
    lift = 1.0 + elev_x * elev_x + elev_y * elev_y
    elevation_rate = vertical * lift - (pot_x * elev_x + pot_y * elev_y)
    potential_rate = (
        -elevation - 0.5 * (pot_x * pot_x + pot_y * pot_y) + 0.5 * vertical * vertical * lift
    )
    return (elevation_rate, potential_rate)


def solution(mesh):
    in_specs = (
        P("tx", "ty"),
        P("tx", "ty"),
        P("tx", "ty"),
        P("tx", "ty"),
        P("tx", "ty"),
        P(("tx", "ty"), None),
    )
    out_specs = (P("tx", "ty"), P("tx", "ty"))
    return jax.shard_map(shards, mesh=mesh, in_specs=in_specs, out_specs=out_specs, check_vma=False)
```

```python
import math

import jax
import jax.numpy as jnp
from jax import lax
from jax.experimental import pallas as pl
from jax.experimental.pallas import tpu as pltpu
from jax.sharding import PartitionSpec as P

LANES = 128
WIDE = 256
PIECES = 6
FEATURES = 32
USED = 24
EXTRA = 16
BF16 = jnp.bfloat16
F32 = jnp.float32


def shifted(value, axis, steps):
    count = lax.axis_size(axis)
    pairs = [(source, (source + steps) % count) for source in range(count)]
    return lax.ppermute(value, axis, pairs)


def ahead(axis, steps):
    index = lax.axis_index(axis) + steps
    count = lax.axis_size(axis)
    return jnp.where(index < 0, index + count, jnp.where(index >= count, index - count, index))


def pinned(value):
    return pltpu.with_memory_space_constraint(value, pltpu.VMEM)


def rounded(value):
    return value.astype(BF16).astype(F32)


def scatter_kernel(first, last, sizes, steps, tile, *refs):
    if first:
        acc = refs[0]
    else:
        acc_in, acc = refs[:2]
    rows, cols, high_count, node_rows, node_cols = sizes
    p = lax.axis_index("tx")
    q = lax.axis_index("ty")
    base = ((p * lax.axis_size("ty") + q) * (rows * cols)).astype(F32)
    off_i = float(steps[0] * rows)
    off_j = float((steps[1] - 1) * cols)
    acc[...] = jnp.zeros(acc.shape, F32) if first else acc_in[...]
    units = [(r, c) for r in range(rows // 8) for c in range(cols // LANES)]

    def split(r, c):
        rel = tile[0, 8 * r : 8 * r + 8, LANES * c : LANES * c + LANES] - base
        high = jnp.floor(rel * (1.0 / WIDE))
        return high, rel - high * WIDE

    flags = []
    for r, c in units:
        high, _ = split(r, c)
        mine = (high >= 0.0) & (high < high_count)
        flags.append(jnp.max(jnp.where(mine, 1.0, 0.0)) > 0.0)

    for (r, c), flag in zip(units, flags):

        @pl.when(flag)
        def _():
            high, low = split(r, c)
            window = (slice(8 * r, 8 * r + 8), slice(LANES * c, LANES * c + LANES))
            z = 0.25 * tile[(1,) + window]
            z_high = rounded(z)
            z_low = z - z_high
            pot = tile[(2,) + window]
            flux = tile[(3,) + window]
            col_index = (lax.broadcasted_iota(jnp.int32, (high_count, LANES), 1) + LANES * c).astype(F32) + off_j
            high_iota = lax.broadcasted_iota(jnp.int32, (high_count, LANES), 0).astype(F32)
            low_iota = lax.broadcasted_iota(jnp.int32, (WIDE, LANES), 0).astype(F32)
            lefts = []
            rights = []
            for s in range(8):

                def row(v):
                    return v[s : s + 1, :]

                hit = high_iota == row(high)
                row_index = jnp.full((1, LANES), 8 * r + s, F32) + off_i
                values = [row_index, col_index, row(z_high), row(z_low), row(pot), row(flux)]
                lefts.append(
                    jnp.concatenate([jnp.where(hit, v, 0.0).astype(BF16) for v in values], axis=0)
                )
                rights.append(jnp.where(low_iota == row(low), 1.0, 0.0).astype(BF16))
            acc[...] += lax.dot_general(
                jnp.concatenate(lefts, axis=1),
                jnp.concatenate(rights, axis=1),
                (((1,), (1,)), ((), ())),
                preferred_element_type=F32,
            )

    if last:
        boxed = refs[-1]
        h = high_count
        row0 = (p * rows).astype(F32)
        col0 = ((q + 1) * cols).astype(F32)
        i = acc[0:h] + row0
        i = jnp.where(i >= node_rows, i - node_rows, i)
        j = acc[h : 2 * h] + col0
        j = jnp.where(j >= node_cols, j - node_cols, j)
        fields = [
            (i + 0.5) / node_rows,
            (j + 0.5) / node_cols,
            acc[2 * h : 3 * h] + acc[3 * h : 4 * h],
            acc[4 * h : 5 * h],
            acc[5 * h : 6 * h],
        ]
        for k, f in enumerate(fields):
            boxed[k, 0:h, :] = f[:, :LANES]
            boxed[k, h : 2 * h, :] = f[:, LANES:]


def scatter(steps, tile, acc, last, node_rows, node_cols):
    _, rows, cols = tile.shape
    high_count = rows * cols // WIDE
    first = acc is None
    vmem = pl.BlockSpec(memory_space=pltpu.VMEM)
    out_shape = [pltpu.VMEM((PIECES * high_count, WIDE), F32)]
    if last:
        out_shape.append(pltpu.VMEM((5, 2 * high_count, LANES), F32))
    args = (tile,) if first else (tile, pinned(acc))
    out = pl.pallas_call(
        lambda *refs: scatter_kernel(
            first, last, (rows, cols, high_count, node_rows, node_cols), steps, *refs
        ),
        out_shape=out_shape,
        in_specs=[vmem] * len(args),
        out_specs=[vmem] * len(out_shape),
        name="scatter_last" if last else "scatter_first" if first else "scatter",
        cost_estimate=pl.CostEstimate(
            flops=2 * PIECES * high_count * WIDE * rows * cols // 2,
            transcendentals=0,
            bytes_accessed=4 * (2 * PIECES * high_count * WIDE + 4 * rows * cols),
        ),
    )(*args)
    return out[1] if last else out[0]


def thirds(value):
    high = rounded(value)
    middle = rounded(value - high)
    return high, middle, value - high - middle


def near_kernel(near, listed, own, lower, upper, tile, out, tfeat, sfeat, smeta, even, odd):
    boxes = own.shape[1]
    scale = 1.0 / math.sqrt(near * LANES)
    tpitch = tfeat.shape[0] // USED
    spitch = sfeat.shape[0] // USED

    zeros = jnp.zeros((8, LANES), F32)
    ones = jnp.ones((8, LANES), F32)

    for which, ref in enumerate((lower, own, upper)):
        for group in range(boxes // 8):
            window = (slice(8 * group, 8 * group + 8), slice(None))
            x, y, z, pot, flux = (ref[(f,) + window] for f in range(5))
            pieces = []
            total = None
            for v in (x, y, z):
                high = rounded(v)
                low = rounded(v - high)
                kept = high + low
                pieces.append((high, low))
                total = kept * kept if total is None else total + kept * kept
            start = which * boxes + 8 * group
            source = []
            for high, low in pieces:
                source += [-2.0 * high, -2.0 * low, -2.0 * high, -2.0 * low]
            source += list(thirds(total)) + [ones, ones, ones]
            source += [zeros] * (USED - len(source))
            for k, v in enumerate(source):
                sfeat[k * spitch + start : k * spitch + start + 8, :] = v
            z = pieces[2][0] + pieces[2][1]
            smeta[0, start : start + 8, :] = pot
            smeta[1, start : start + 8, :] = pot * z
            smeta[2, start : start + 8, :] = flux
            if which == 1:
                target = []
                for high, low in pieces:
                    target += [high, high, low, low]
                target += [ones, ones, ones] + list(thirds(total + 0.04)) + [z]
                target += [zeros] * (USED - len(target))
                for k, v in enumerate(target):
                    tfeat[k * tpitch + 8 * group : k * tpitch + 8 * group + 8, :] = v

    def load(ref, pitch, n):
        rows = [ref[pl.ds(8 * g * pitch + n, 8, stride=pitch), :] for g in range(USED // 8)]
        return jnp.concatenate(rows + [zeros] * ((FEATURES - USED) // 8), axis=0)

    def distances(box, squared, z_ref):
        left = load(tfeat, tpitch, box).T
        z_ref[...] = jnp.broadcast_to(left[:, 18:19], (LANES, LANES))
        rights = []
        for k in range(near):
            n = listed[box * near + k]
            rights.append(load(sfeat, spitch, n).astype(BF16))
        squared[...] = jnp.dot(
            left.astype(BF16), jnp.concatenate(rights, axis=1), preferred_element_type=F32
        )

    def apply(box, squared, z_ref):
        metas = []
        for k in range(near):
            n = listed[box * near + k]
            metas.append(
                [jnp.broadcast_to(smeta[m, pl.ds(n, 1), :], (8, LANES)) for m in range(3)]
            )
        parts = []
        for t in range(LANES // 8):
            rows = slice(8 * t, 8 * t + 8)
            z = z_ref[rows, :]
            total = None
            for k in range(near):
                pot, pot_z, flux = metas[k]
                inverse = lax.rsqrt(squared[rows, LANES * k : LANES * k + LANES])
                value = inverse * (flux - (inverse * inverse) * (z * pot - pot_z))
                total = value if total is None else total + value
            parts.append(total)
        summed = jnp.concatenate(parts, axis=0).T
        out[pl.ds(box, 1), :] = jnp.sum(summed, axis=0, keepdims=True) * scale

    (even_sq, even_z), (odd_sq, odd_z) = even, odd
    distances(0, even_sq, even_z)

    def step(i, carry):
        distances(2 * i + 1, odd_sq, odd_z)
        apply(2 * i, even_sq, even_z)
        distances(jnp.minimum(2 * i + 2, boxes - 1), even_sq, even_z)
        apply(2 * i + 1, odd_sq, odd_z)
        return carry

    lax.fori_loop(0, boxes // 2, step, 0)

    _, rows, cols = tile.shape
    out[boxes : boxes + EXTRA, :] = jnp.zeros((EXTRA, LANES), F32)
    place = boxes
    for f in (1, 2):
        for r in (rows - 2, rows - 1):
            for c in range(cols // LANES):
                out[place : place + 1, :] = tile[f, r : r + 1, LANES * c : LANES * c + LANES]
                place += 1
    place = boxes + EXTRA - 8
    for f in (1, 2):
        turned = tile[f, :, cols - LANES : cols].T
        out[place : place + 2, 0:rows] = turned[LANES - 2 : LANES, :]
        place += 2


def near_apply(listed, own, lower, upper, tile, near):
    boxes = own.shape[1]
    vmem = pl.BlockSpec(memory_space=pltpu.VMEM)
    smem = pl.BlockSpec(memory_space=pltpu.SMEM)
    buffers = [pltpu.VMEM((LANES, near * LANES), F32), pltpu.VMEM((LANES, LANES), F32)]

    def kernel(listed, own, lower, upper, tile, out, tfeat, sfeat, smeta, e0, e1, o0, o1):
        near_kernel(
            near, listed, own, lower, upper, tile, out, tfeat, sfeat, smeta, (e0, e1), (o0, o1)
        )

    pairs = boxes * near * LANES * LANES
    return pl.pallas_call(
        kernel,
        out_shape=pltpu.VMEM((boxes + EXTRA, LANES), F32),
        in_specs=[smem] + [vmem] * 4,
        out_specs=vmem,
        scratch_shapes=[
            pltpu.VMEM((USED * (boxes + 8), LANES), F32),
            pltpu.VMEM((USED * (3 * boxes + 8), LANES), F32),
            pltpu.VMEM((3, 3 * boxes, LANES), F32),
        ]
        + buffers
        + buffers,
        name="near_field",
        cost_estimate=pl.CostEstimate(
            flops=pairs * 2 * FEATURES * 4, transcendentals=pairs, bytes_accessed=4 * 16 * boxes * LANES
        ),
    )(listed, pinned(own), pinned(lower), pinned(upper), tile)


def lookup(slot, bases, tables, pieces, out):
    rows, cols = slot.shape
    high_count = rows * cols // WIDE
    units = [(r, c) for r in range(rows // 8) for c in range(cols // LANES)]
    for which, table in enumerate(tables):
        whole = jnp.concatenate([table[0:high_count, :], table[high_count : 2 * high_count, :]], axis=1)
        top = rounded(whole)
        pieces[which, 0:high_count, :] = top.astype(BF16)
        pieces[which, high_count : 2 * high_count, :] = (whole - top).astype(BF16)

    def split(r, c, which):
        rel = slot[8 * r : 8 * r + 8, LANES * c : LANES * c + LANES] - bases[which]
        high = jnp.floor(rel * (1.0 / WIDE))
        return high, rel - high * WIDE

    flags = {}
    for r, c in units:
        for which in range(len(tables)):
            high, _ = split(r, c, which)
            there = (high >= 0.0) & (high < high_count)
            flags[r, c, which] = jnp.max(jnp.where(there, 1.0, 0.0)) > 0.0

    for r, c in units:
        for which in range(len(tables)):

            @pl.when(flags[r, c, which])
            def _():
                high, low = split(r, c, which)
                low_iota = lax.broadcasted_iota(jnp.int32, (WIDE, LANES), 0).astype(F32)
                high_iota = lax.broadcasted_iota(jnp.int32, (high_count, LANES), 0).astype(F32)
                hits = jnp.concatenate(
                    [jnp.where(low_iota == low[s : s + 1, :], 1.0, 0.0).astype(BF16) for s in range(8)],
                    axis=1,
                )
                picked = jnp.dot(pieces[which], hits, preferred_element_type=F32)
                lines = []
                for s in range(8):
                    window = slice(LANES * s, LANES * s + LANES)
                    both = picked[0:high_count, window] + picked[high_count : 2 * high_count, window]
                    mine = high_iota == high[s : s + 1, :]
                    lines.append(jnp.sum(jnp.where(mine, both, 0.0), axis=0, keepdims=True))
                out[8 * r : 8 * r + 8, LANES * c : LANES * c + LANES] += jnp.concatenate(lines, axis=0)


def base_of(node_count, steps):
    rank = ahead("tx", -steps[0]) * lax.axis_size("ty") + ahead("ty", -steps[1])
    return (rank * node_count).astype(F32)


def gather_own_kernel(tile, own, out, pieces):
    out[...] = jnp.zeros(out.shape, F32)
    lookup(tile.at[0], [base_of(out.shape[0] * out.shape[1], (0, 0))], [own], pieces, out)


def gather_own(tile, own):
    _, rows, cols = tile.shape
    vmem = pl.BlockSpec(memory_space=pltpu.VMEM)
    return pl.pallas_call(
        gather_own_kernel,
        out_shape=pltpu.VMEM((rows, cols), F32),
        in_specs=[vmem] * 2,
        out_specs=vmem,
        scratch_shapes=[pltpu.VMEM((1, 2 * rows * cols // WIDE, WIDE), BF16)],
        name="gather_own",
        cost_estimate=pl.CostEstimate(
            flops=rows * cols * rows * cols, transcendentals=0, bytes_accessed=4 * 4 * rows * cols
        ),
    )(tile, pinned(own))


def finish_kernel(
    tile, ahead_x, ahead_y, partial, behind_x, behind_y, behind_xy, elev_rate, pot_rate, pieces, total, padded
):
    _, rows, cols = tile.shape
    boxes = rows * cols // LANES
    total[...] = partial[...]
    bases = [base_of(rows * cols, steps) for steps in ((1, 0), (0, 1), (1, 1))]
    lookup(tile.at[0], bases, [behind_x, behind_y, behind_xy], pieces, total)

    left_cols = behind_y[boxes + EXTRA - 8 : boxes + EXTRA, 0:rows].T
    col = lax.broadcasted_iota(jnp.int32, (rows, cols), 1)
    slopes = []
    for f in (1, 2):
        here = tile[f]
        padded[8 : 8 + rows, :] = here
        for r in range(2):
            for c in range(cols // LANES):
                source = boxes + ((f - 1) * 2 + r) * (cols // LANES) + c
                padded[6 + r : 7 + r, LANES * c : LANES * c + LANES] = behind_x[source : source + 1, :]
        padded[8 + rows : 10 + rows, :] = ahead_x[f, 0:2, :]
        along_rows = (
            padded[6 : 6 + rows, :]
            - 8.0 * padded[7 : 7 + rows, :]
            + 8.0 * padded[9 : 9 + rows, :]
            - padded[10 : 10 + rows, :]
        ) / 12.0
        left = left_cols[:, 2 * (f - 1) : 2 * f]
        right = ahead_y[f, :, 0:2]
        less_1 = jnp.where(col == 0, left[:, 1:2], pltpu.roll(here, 1, 1))
        less_2 = jnp.where(
            col == 0, left[:, 0:1], jnp.where(col == 1, left[:, 1:2], pltpu.roll(here, 2, 1))
        )
        more_1 = jnp.where(col == cols - 1, right[:, 0:1], pltpu.roll(here, cols - 1, 1))
        more_2 = jnp.where(
            col == cols - 2,
            right[:, 0:1],
            jnp.where(col == cols - 1, right[:, 1:2], pltpu.roll(here, cols - 2, 1)),
        )
        along_cols = (less_2 - 8.0 * less_1 + 8.0 * more_1 - more_2) / 12.0
        slopes.append((along_rows, along_cols))
    (elev_x, elev_y), (pot_x, pot_y) = slopes
    vertical = total[...]
    lift = 1.0 + elev_x * elev_x + elev_y * elev_y
    elev_rate[...] = vertical * lift - (pot_x * elev_x + pot_y * elev_y)
    pot_rate[...] = (
        -tile[1] - 0.5 * (pot_x * pot_x + pot_y * pot_y) + 0.5 * vertical * vertical * lift
    )


def finish(tile, ahead_x, ahead_y, partial, behind):
    _, rows, cols = tile.shape
    vmem = pl.BlockSpec(memory_space=pltpu.VMEM)
    shape = jax.ShapeDtypeStruct((rows, cols), F32)
    return pl.pallas_call(
        finish_kernel,
        out_shape=(shape, shape),
        in_specs=[vmem] * 7,
        out_specs=(vmem, vmem),
        scratch_shapes=[
            pltpu.VMEM((3, 2 * rows * cols // WIDE, WIDE), BF16),
            pltpu.VMEM((rows, cols), F32),
            pltpu.VMEM((rows + 16, cols), F32),
        ],
        name="finish",
        cost_estimate=pl.CostEstimate(
            flops=3 * rows * cols * rows * cols, transcendentals=0, bytes_accessed=4 * 8 * rows * cols
        ),
    )(tile, ahead_x, ahead_y, pinned(partial), *[pinned(b) for b in behind])


def shards(potential, elevation, normal_flux, box_owner, box_place, near_boxes):
    rows, cols = potential.shape
    count_tx = lax.axis_size("tx")
    count_ty = lax.axis_size("ty")
    node_count = rows * cols
    boxes = node_count // LANES
    near = near_boxes.shape[1]
    half = boxes // 2
    assert node_count % WIDE == 0 and cols <= 256 and rows <= 128
    assert 4 * (cols // LANES) <= EXTRA - 8
    assert node_count * count_tx * count_ty < 2**24
    rank = lax.axis_index("tx") * count_ty + lax.axis_index("ty")

    slot = (box_owner * node_count + box_place).astype(F32)
    tile = jnp.stack([slot, elevation, potential, normal_flux])
    ahead_x = shifted(tile, "tx", -1)
    ahead_y = shifted(tile, "ty", -1)
    ahead_xy = shifted(ahead_y, "tx", -1)
    tile, ahead_x, ahead_y, ahead_xy = map(pinned, (tile, ahead_x, ahead_y, ahead_xy))

    sizes = (rows * count_tx, cols * count_ty)
    acc = scatter((0, 0), tile, None, False, *sizes)
    acc = scatter((1, 0), ahead_x, acc, False, *sizes)
    acc = scatter((0, 1), ahead_y, acc, False, *sizes)
    boxed = scatter((1, 1), ahead_xy, acc, True, *sizes)

    total = count_tx * count_ty
    both = ("tx", "ty")
    lower = lax.ppermute(boxed, both, [(i, i + 1) for i in range(total - 1)])
    upper = lax.ppermute(boxed, both, [(i + 1, i) for i in range(total - 1)])

    local = near_boxes - (rank - 1) * boxes
    inner = local % boxes
    listed = (local // boxes) * boxes + (inner % 2) * half + inner // 2
    listed = listed.reshape(half, 2, near).transpose(1, 0, 2).reshape(boxes * near)
    value = near_apply(listed, boxed, lower, upper, tile, near)

    behind_x = shifted(value, "tx", 1)
    behind_y = shifted(value, "ty", 1)
    diagonal = [
        (i * count_ty + j, (i + 1) % count_tx * count_ty + (j + 1) % count_ty)
        for i in range(count_tx)
        for j in range(count_ty)
    ]
    behind_xy = lax.ppermute(value, both, diagonal)
    partial = gather_own(tile, value)
    return finish(tile, ahead_x, ahead_y, partial, (behind_x, behind_y, behind_xy))


def solution(mesh):
    in_specs = (
        P("tx", "ty"),
        P("tx", "ty"),
        P("tx", "ty"),
        P("tx", "ty"),
        P("tx", "ty"),
        P(("tx", "ty"), None),
    )
    out_specs = (P("tx", "ty"), P("tx", "ty"))
    return jax.shard_map(shards, mesh=mesh, in_specs=in_specs, out_specs=out_specs, check_vma=False)
```

```python
import math

import jax
import jax.numpy as jnp
from jax import lax
from jax.experimental import pallas as pl
from jax.experimental.pallas import tpu as pltpu
from jax.sharding import PartitionSpec as P

LANES = 128
WIDE = 256
PIECES = 6
FEATURES = 32
USED = 24
EXTRA = 16
GROUP = 4
VMEM_LIMIT = 24 << 20
BF16 = jnp.bfloat16
F32 = jnp.float32


def shifted(value, axis, steps):
    count = lax.axis_size(axis)
    pairs = [(source, (source + steps) % count) for source in range(count)]
    return lax.ppermute(value, axis, pairs)


def ahead(axis, steps):
    index = lax.axis_index(axis) + steps
    count = lax.axis_size(axis)
    return jnp.where(index < 0, index + count, jnp.where(index >= count, index - count, index))


def pinned(value):
    return pltpu.with_memory_space_constraint(value, pltpu.VMEM)


def rounded(value):
    return value.astype(BF16).astype(F32)


def box_split(rel, high_count):
    box = jnp.floor(rel * (1.0 / LANES))
    second = box >= high_count
    high = jnp.where(second, box - high_count, box)
    low = rel - box * LANES
    return high, jnp.where(second, low + LANES, low)


def scatter_kernel(first, last, sizes, steps, tile, *refs):
    if first:
        acc = refs[0]
    else:
        acc_in, acc = refs[:2]
    rows, cols, high_count, node_rows, node_cols = sizes
    p = lax.axis_index("tx")
    q = lax.axis_index("ty")
    base = ((p * lax.axis_size("ty") + q) * (rows * cols)).astype(F32)
    off_i = float(steps[0] * rows)
    off_j = float((steps[1] - 1) * cols)
    acc[...] = jnp.zeros(acc.shape, F32) if first else acc_in[...]
    units = [(r, c) for r in range(rows // 8) for c in range(cols // LANES)]

    def split(r, c):
        return box_split(tile[0, 8 * r : 8 * r + 8, LANES * c : LANES * c + LANES] - base, high_count)

    flags = []
    for r, c in units:
        high, _ = split(r, c)
        mine = (high >= 0.0) & (high < high_count)
        flags.append(jnp.max(jnp.where(mine, 1.0, 0.0)) > 0.0)

    for (r, c), flag in zip(units, flags):

        @pl.when(flag)
        def _():
            high, low = split(r, c)
            window = (slice(8 * r, 8 * r + 8), slice(LANES * c, LANES * c + LANES))
            z = 0.25 * tile[(1,) + window]
            z_high = rounded(z)
            z_low = z - z_high
            pot = tile[(2,) + window]
            flux = tile[(3,) + window]
            col_index = (lax.broadcasted_iota(jnp.int32, (high_count, LANES), 1) + LANES * c).astype(F32) + off_j
            high_iota = lax.broadcasted_iota(jnp.int32, (high_count, LANES), 0).astype(F32)
            low_iota = lax.broadcasted_iota(jnp.int32, (WIDE, LANES), 0).astype(F32)
            lefts = []
            rights = []
            for s in range(8):

                def row(v):
                    return v[s : s + 1, :]

                hit = high_iota == row(high)
                row_index = jnp.full((1, LANES), 8 * r + s, F32) + off_i
                values = [row_index, col_index, row(z_high), row(z_low), row(pot), row(flux)]
                lefts.append(
                    jnp.concatenate([jnp.where(hit, v, 0.0).astype(BF16) for v in values], axis=0)
                )
                rights.append(jnp.where(low_iota == row(low), 1.0, 0.0).astype(BF16))
            acc[...] += lax.dot_general(
                jnp.concatenate(lefts, axis=1),
                jnp.concatenate(rights, axis=1),
                (((1,), (1,)), ((), ())),
                preferred_element_type=F32,
            )

    if last:
        boxed = refs[-1]
        h = high_count
        row0 = (p * rows).astype(F32)
        col0 = ((q + 1) * cols).astype(F32)
        i = acc[0:h] + row0
        i = jnp.where(i >= node_rows, i - node_rows, i)
        j = acc[h : 2 * h] + col0
        j = jnp.where(j >= node_cols, j - node_cols, j)
        fields = [
            (i + 0.5) / node_rows,
            (j + 0.5) / node_cols,
            acc[2 * h : 3 * h] + acc[3 * h : 4 * h],
            acc[4 * h : 5 * h],
            acc[5 * h : 6 * h],
        ]
        for k, f in enumerate(fields):
            boxed[k, 0:h, :] = f[:, :LANES]
            boxed[k, h : 2 * h, :] = f[:, LANES:]


def scatter(steps, tile, acc, last, node_rows, node_cols):
    _, rows, cols = tile.shape
    high_count = rows * cols // WIDE
    first = acc is None
    vmem = pl.BlockSpec(memory_space=pltpu.VMEM)
    out_shape = [pltpu.VMEM((PIECES * high_count, WIDE), F32)]
    if last:
        out_shape.append(pltpu.VMEM((5, 2 * high_count, LANES), F32))
    args = (tile,) if first else (tile, pinned(acc))
    out = pl.pallas_call(
        lambda *refs: scatter_kernel(
            first, last, (rows, cols, high_count, node_rows, node_cols), steps, *refs
        ),
        out_shape=out_shape,
        in_specs=[vmem] * len(args),
        out_specs=[vmem] * len(out_shape),
        compiler_params=pltpu.CompilerParams(vmem_limit_bytes=VMEM_LIMIT),
        name="scatter_last" if last else "scatter_first" if first else "scatter",
        cost_estimate=pl.CostEstimate(
            flops=2 * PIECES * high_count * WIDE * rows * cols // 2,
            transcendentals=0,
            bytes_accessed=4 * (2 * PIECES * high_count * WIDE + 4 * rows * cols),
        ),
    )(*args)
    return out[1] if last else out[0]


def thirds(value):
    high = rounded(value)
    middle = rounded(value - high)
    return high, middle, value - high - middle


def layout(boxes, near):
    items = boxes * ((near + 1) // 2) + 4 * GROUP
    return items, (8, 8 + items), (8 + 3 * items, 8 + 4 * items), 8 + 6 * items


def plan_kernel(boxes, near, listed, plan):
    _, own_at, other_at, _ = layout(boxes, near)
    rank = lax.axis_index("tx") * lax.axis_size("ty") + lax.axis_index("ty")
    offset = (rank - 1) * boxes
    deepest = (near + 1) // 2

    def one(b, carry):
        own_items, other_items = carry
        own = 2 * own_items
        other = 2 * other_items
        for k in range(near):
            n = listed[k * boxes + b] - offset
            mine = jnp.where((n >= boxes) & (n < 2 * boxes), 1, 0)
            plan[own_at[1] + own] = n - boxes
            plan[other_at[1] + other] = jnp.where(n < boxes, n, n - boxes)
            own = own + mine
            other = other + 1 - mine
        plan[own_at[1] + own] = boxes
        plan[other_at[1] + other] = 2 * boxes
        for i in range(deepest):
            plan[own_at[0] + own_items + i] = b
            plan[other_at[0] + other_items + i] = b
        return (own + 1) // 2, (other + 1) // 2

    own_items, other_items = lax.fori_loop(0, boxes, one, (jnp.int32(0), jnp.int32(0)))
    for at, count, empty in ((own_at, own_items, boxes), (other_at, other_items, 2 * boxes)):
        for i in range(3 * GROUP):
            plan[at[0] + count + i] = boxes
            plan[at[1] + 2 * (count + i)] = empty
            plan[at[1] + 2 * (count + i) + 1] = empty
    plan[0] = (own_items + 2 * GROUP - 1) // (2 * GROUP)
    plan[1] = (other_items + 2 * GROUP - 1) // (2 * GROUP)


def make_plan(near_boxes):
    boxes, near = near_boxes.shape
    smem = pl.BlockSpec(memory_space=pltpu.SMEM)
    return pl.pallas_call(
        lambda *refs: plan_kernel(boxes, near, *refs),
        out_shape=jax.ShapeDtypeStruct((layout(boxes, near)[-1],), jnp.int32),
        in_specs=[smem],
        out_specs=smem,
        compiler_params=pltpu.CompilerParams(vmem_limit_bytes=VMEM_LIMIT),
        name="plan",
        cost_estimate=pl.CostEstimate(flops=10**7, transcendentals=0, bytes_accessed=16 * boxes * near),
    )(near_boxes.T.reshape(boxes * near))


def pieces_of(ref, group):
    window = (slice(8 * group, 8 * group + 8), slice(None))
    x, y, z, pot, flux = (ref[(f,) + window] for f in range(5))
    pieces = []
    total = None
    for v in (x, y, z):
        high = rounded(v)
        low = rounded(v - high)
        kept = high + low
        pieces.append((high, low))
        total = kept * kept if total is None else total + kept * kept
    return pieces, total, pot, flux


def padded_rows(values):
    return values + [jnp.zeros_like(values[0])] * (USED - len(values))


def strided(ref, n):
    pitch = ref.shape[0] // USED
    rows = [ref[pl.ds(8 * g * pitch + n, 8, stride=pitch), :] for g in range(USED // 8)]
    return jnp.concatenate(rows + [jnp.zeros((8, LANES), F32)] * ((FEATURES - USED) // 8), axis=0)


def store_sources(refs, sfeat, smeta):
    pitch = sfeat.shape[0] // USED
    ones = jnp.ones((8, LANES), F32)
    zeros = jnp.zeros((8, LANES), F32)
    start = 0
    for ref in refs:
        for group in range(ref.shape[1] // 8):
            pieces, total, pot, flux = pieces_of(ref, group)
            source = []
            for high, low in pieces:
                source += [-2.0 * high, -2.0 * low, -2.0 * high, -2.0 * low]
            for k, v in enumerate(padded_rows(source + list(thirds(total)) + [ones, ones, ones])):
                sfeat[k * pitch + start : k * pitch + start + 8, :] = v
            z = pieces[2][0] + pieces[2][1]
            smeta[0, start : start + 8, :] = pot
            smeta[1, start : start + 8, :] = pot * z
            smeta[2, start : start + 8, :] = flux
            start += 8
    for k in range(USED):
        sfeat[k * pitch + start : k * pitch + start + 8, :] = ones if k == 12 else zeros
    for m in range(3):
        smeta[m, start : start + 8, :] = zeros


def store_targets(own, tfeat, turned):
    boxes = own.shape[1]
    pitch = tfeat.shape[0] // USED
    ones = jnp.ones((8, LANES), F32)
    for group in range(boxes // 8):
        pieces, total, _, _ = pieces_of(own, group)
        target = []
        for high, low in pieces:
            target += [high, high, low, low]
        for k, v in enumerate(padded_rows(target + [ones, ones, ones] + list(thirds(total + 0.04)))):
            tfeat[k * pitch + 8 * group : k * pitch + 8 * group + 8, :] = v
    turned[boxes] = jnp.zeros((LANES, FEATURES), BF16)

    def turn(i, carry):
        for u in range(8):
            turned[8 * i + u] = strided(tfeat, 8 * i + u).T.astype(BF16)
        return carry

    lax.fori_loop(0, boxes // 8, turn, 0)


def run_items(plan, iterations, at, turned, ztop, sfeat, smeta, sums, squares, totals):
    empty_row = sums.shape[0] - 8

    def distances(group, squared):
        for i in range(GROUP):
            item = group * GROUP + i
            target = plan[at[0] + item]
            sides = [strided(sfeat, plan[at[1] + 2 * item + k]).astype(BF16) for k in range(2)]
            squared[i] = jnp.dot(
                turned[target], jnp.concatenate(sides, axis=1), preferred_element_type=F32
            )

    def apply(group, squared, total):
        for i in range(GROUP):
            item = group * GROUP + i
            target = plan[at[0] + item]
            lane = jnp.full((8, LANES), jnp.minimum(target, LANES - 1), jnp.int32)
            metas = []
            for k in range(2):
                n = plan[at[1] + 2 * item + k]
                metas.append([jnp.broadcast_to(smeta[m, pl.ds(n, 1), :], (8, LANES)) for m in range(3)])
            for t in range(LANES // 8):
                rows = slice(8 * t, 8 * t + 8)
                z = jnp.take_along_axis(ztop[rows, :], lane, axis=1)
                value = None
                for k in range(2):
                    pot, pot_z, flux = metas[k]
                    inverse = lax.rsqrt(squared[i, rows, LANES * k : LANES * k + LANES])
                    part = inverse * (flux - (inverse * inverse) * (z * pot - pot_z))
                    value = part if value is None else value + part
                total[i, rows, :] = value

    def reduce(group, total, live):
        for i in range(GROUP):
            target = plan[at[0] + jnp.maximum(group * GROUP + i, 0)]
            target = jnp.where(live, target, empty_row)
            row = jnp.sum(total[i].T, axis=0, keepdims=True)
            sums[pl.ds(target, 1), :] += row

    (even_sq, odd_sq), (even_tot, odd_tot) = squares, totals
    odd_tot[...] = jnp.zeros(odd_tot.shape, F32)
    distances(0, even_sq)

    def step(i, carry):
        distances(2 * i + 1, odd_sq)
        apply(2 * i, even_sq, even_tot)
        reduce(2 * i - 1, odd_tot, i > 0)
        distances(2 * i + 2, even_sq)
        apply(2 * i + 1, odd_sq, odd_tot)
        reduce(2 * i, even_tot, True)
        return carry

    lax.fori_loop(0, iterations, step, 0)
    reduce(2 * iterations - 1, odd_tot, iterations > 0)


def near_own_kernel(near, plan, own, sums, turned, ztop, tfeat, sfeat, smeta, s0, s1, t0, t1):
    boxes = own.shape[1]
    sums[...] = jnp.zeros(sums.shape, F32)
    store_targets(own, tfeat, turned)
    high = rounded(own[2])
    ztop[...] = (high + rounded(own[2] - high)).T
    store_sources([own], sfeat, smeta)
    _, own_at, _, _ = layout(boxes, near)
    run_items(plan, plan[0], own_at, turned, ztop, sfeat, smeta, sums, (s0, s1), (t0, t1))


def near_other_kernel(
    near, plan, lower, upper, tile, sums_in, turned, ztop, out, sums, sfeat, smeta, s0, s1, t0, t1
):
    boxes = lower.shape[1]
    sums[...] = sums_in[...]
    store_sources([lower, upper], sfeat, smeta)
    _, _, other_at, _ = layout(boxes, near)
    run_items(plan, plan[1], other_at, turned, ztop, sfeat, smeta, sums, (s0, s1), (t0, t1))
    out[0:boxes, :] = sums[0:boxes, :] * (1.0 / math.sqrt(near * LANES))

    _, rows, cols = tile.shape
    out[boxes : boxes + EXTRA, :] = jnp.zeros((EXTRA, LANES), F32)
    place = boxes
    for f in (1, 2):
        for r in (rows - 2, rows - 1):
            for c in range(cols // LANES):
                out[place : place + 1, :] = tile[f, r : r + 1, LANES * c : LANES * c + LANES]
                place += 1
    place = boxes + EXTRA - 8
    for f in (1, 2):
        turned_cols = tile[f, :, cols - LANES : cols].T
        out[place : place + 2, 0:rows] = turned_cols[LANES - 2 : LANES, :]
        place += 2


def item_scratch(sources):
    return [
        pltpu.VMEM((USED * (sources + 8), LANES), F32),
        pltpu.VMEM((3, sources + 8, LANES), F32),
        pltpu.VMEM((GROUP, LANES, 2 * LANES), F32),
        pltpu.VMEM((GROUP, LANES, 2 * LANES), F32),
        pltpu.VMEM((GROUP, LANES, LANES), F32),
        pltpu.VMEM((GROUP, LANES, LANES), F32),
    ]


def near_cost(boxes, near):
    pairs = boxes * near * LANES * LANES // 2
    return pl.CostEstimate(
        flops=pairs * 2 * FEATURES * 4, transcendentals=pairs, bytes_accessed=4 * 16 * boxes * LANES
    )


def near_own(plan, own, near):
    boxes = own.shape[1]
    assert boxes == LANES
    vmem = pl.BlockSpec(memory_space=pltpu.VMEM)
    smem = pl.BlockSpec(memory_space=pltpu.SMEM)
    return pl.pallas_call(
        lambda *refs: near_own_kernel(near, *refs),
        out_shape=(
            pltpu.VMEM((boxes + 8, LANES), F32),
            pltpu.VMEM((boxes + 1, LANES, FEATURES), BF16),
            pltpu.VMEM((LANES, boxes), F32),
        ),
        in_specs=[smem, vmem],
        out_specs=(vmem,) * 3,
        scratch_shapes=[pltpu.VMEM((USED * (boxes + 8), LANES), F32)] + item_scratch(boxes),
        compiler_params=pltpu.CompilerParams(vmem_limit_bytes=VMEM_LIMIT),
        name="near_own",
        cost_estimate=near_cost(boxes, near),
    )(plan, pinned(own))


def near_other(plan, lower, upper, tile, sums, turned, ztop, near):
    boxes = lower.shape[1]
    vmem = pl.BlockSpec(memory_space=pltpu.VMEM)
    smem = pl.BlockSpec(memory_space=pltpu.SMEM)
    return pl.pallas_call(
        lambda *refs: near_other_kernel(near, *refs),
        out_shape=pltpu.VMEM((boxes + EXTRA, LANES), F32),
        in_specs=[smem] + [vmem] * 6,
        out_specs=vmem,
        scratch_shapes=[pltpu.VMEM((boxes + 8, LANES), F32)] + item_scratch(2 * boxes),
        compiler_params=pltpu.CompilerParams(vmem_limit_bytes=VMEM_LIMIT),
        name="near_other",
        cost_estimate=near_cost(boxes, near),
    )(plan, *map(pinned, (lower, upper, tile, sums, turned, ztop)))


def lookup(slot, bases, tables, pieces, out):
    rows, cols = slot.shape
    high_count = rows * cols // WIDE
    units = [(r, c) for r in range(rows // 8) for c in range(cols // LANES)]
    for which, table in enumerate(tables):
        whole = jnp.concatenate([table[0:high_count, :], table[high_count : 2 * high_count, :]], axis=1)
        top = rounded(whole)
        pieces[which, 0:high_count, :] = top.astype(BF16)
        pieces[which, high_count : 2 * high_count, :] = (whole - top).astype(BF16)

    def split(r, c, which):
        window = (slice(8 * r, 8 * r + 8), slice(LANES * c, LANES * c + LANES))
        return box_split(slot[window] - bases[which], high_count)

    flags = {}
    for r, c in units:
        for which in range(len(tables)):
            high, _ = split(r, c, which)
            there = (high >= 0.0) & (high < high_count)
            flags[r, c, which] = jnp.max(jnp.where(there, 1.0, 0.0)) > 0.0

    for r, c in units:
        for which in range(len(tables)):

            @pl.when(flags[r, c, which])
            def _():
                high, low = split(r, c, which)
                low_iota = lax.broadcasted_iota(jnp.int32, (WIDE, LANES), 0).astype(F32)
                high_iota = lax.broadcasted_iota(jnp.int32, (high_count, LANES), 0).astype(F32)
                hits = jnp.concatenate(
                    [jnp.where(low_iota == low[s : s + 1, :], 1.0, 0.0).astype(BF16) for s in range(8)],
                    axis=1,
                )
                picked = jnp.dot(pieces[which], hits, preferred_element_type=F32)
                lines = []
                for s in range(8):
                    window = slice(LANES * s, LANES * s + LANES)
                    both = picked[0:high_count, window] + picked[high_count : 2 * high_count, window]
                    mine = high_iota == high[s : s + 1, :]
                    lines.append(jnp.sum(jnp.where(mine, both, 0.0), axis=0, keepdims=True))
                out[8 * r : 8 * r + 8, LANES * c : LANES * c + LANES] += jnp.concatenate(lines, axis=0)


def base_of(node_count, steps):
    rank = ahead("tx", -steps[0]) * lax.axis_size("ty") + ahead("ty", -steps[1])
    return (rank * node_count).astype(F32)


def gather_own_kernel(tile, own, out, pieces):
    out[...] = jnp.zeros(out.shape, F32)
    lookup(tile.at[0], [base_of(out.shape[0] * out.shape[1], (0, 0))], [own], pieces, out)


def gather_own(tile, own):
    _, rows, cols = tile.shape
    vmem = pl.BlockSpec(memory_space=pltpu.VMEM)
    return pl.pallas_call(
        gather_own_kernel,
        out_shape=pltpu.VMEM((rows, cols), F32),
        in_specs=[vmem] * 2,
        out_specs=vmem,
        scratch_shapes=[pltpu.VMEM((1, 2 * rows * cols // WIDE, WIDE), BF16)],
        compiler_params=pltpu.CompilerParams(vmem_limit_bytes=VMEM_LIMIT),
        name="gather_own",
        cost_estimate=pl.CostEstimate(
            flops=rows * cols * rows * cols, transcendentals=0, bytes_accessed=4 * 4 * rows * cols
        ),
    )(tile, pinned(own))


def finish_kernel(
    tile, ahead_x, ahead_y, partial, behind_x, behind_y, behind_xy, elev_rate, pot_rate, pieces, total, padded
):
    _, rows, cols = tile.shape
    boxes = rows * cols // LANES
    total[...] = partial[...]
    bases = [base_of(rows * cols, steps) for steps in ((1, 0), (0, 1), (1, 1))]
    lookup(tile.at[0], bases, [behind_x, behind_y, behind_xy], pieces, total)

    left_cols = behind_y[boxes + EXTRA - 8 : boxes + EXTRA, 0:rows].T
    col = lax.broadcasted_iota(jnp.int32, (rows, cols), 1)
    slopes = []
    for f in (1, 2):
        here = tile[f]
        padded[8 : 8 + rows, :] = here
        for r in range(2):
            for c in range(cols // LANES):
                source = boxes + ((f - 1) * 2 + r) * (cols // LANES) + c
                padded[6 + r : 7 + r, LANES * c : LANES * c + LANES] = behind_x[source : source + 1, :]
        padded[8 + rows : 10 + rows, :] = ahead_x[f, 0:2, :]
        along_rows = (
            padded[6 : 6 + rows, :]
            - 8.0 * padded[7 : 7 + rows, :]
            + 8.0 * padded[9 : 9 + rows, :]
            - padded[10 : 10 + rows, :]
        ) / 12.0
        left = left_cols[:, 2 * (f - 1) : 2 * f]
        right = ahead_y[f, :, 0:2]
        less_1 = jnp.where(col == 0, left[:, 1:2], pltpu.roll(here, 1, 1))
        less_2 = jnp.where(
            col == 0, left[:, 0:1], jnp.where(col == 1, left[:, 1:2], pltpu.roll(here, 2, 1))
        )
        more_1 = jnp.where(col == cols - 1, right[:, 0:1], pltpu.roll(here, cols - 1, 1))
        more_2 = jnp.where(
            col == cols - 2,
            right[:, 0:1],
            jnp.where(col == cols - 1, right[:, 1:2], pltpu.roll(here, cols - 2, 1)),
        )
        along_cols = (less_2 - 8.0 * less_1 + 8.0 * more_1 - more_2) / 12.0
        slopes.append((along_rows, along_cols))
    (elev_x, elev_y), (pot_x, pot_y) = slopes
    vertical = total[...]
    lift = 1.0 + elev_x * elev_x + elev_y * elev_y
    elev_rate[...] = vertical * lift - (pot_x * elev_x + pot_y * elev_y)
    pot_rate[...] = (
        -tile[1] - 0.5 * (pot_x * pot_x + pot_y * pot_y) + 0.5 * vertical * vertical * lift
    )


def finish(tile, ahead_x, ahead_y, partial, behind):
    _, rows, cols = tile.shape
    vmem = pl.BlockSpec(memory_space=pltpu.VMEM)
    shape = jax.ShapeDtypeStruct((rows, cols), F32)
    return pl.pallas_call(
        finish_kernel,
        out_shape=(shape, shape),
        in_specs=[vmem] * 7,
        out_specs=(vmem, vmem),
        scratch_shapes=[
            pltpu.VMEM((3, 2 * rows * cols // WIDE, WIDE), BF16),
            pltpu.VMEM((rows, cols), F32),
            pltpu.VMEM((rows + 16, cols), F32),
        ],
        compiler_params=pltpu.CompilerParams(vmem_limit_bytes=VMEM_LIMIT),
        name="finish",
        cost_estimate=pl.CostEstimate(
            flops=3 * rows * cols * rows * cols, transcendentals=0, bytes_accessed=4 * 8 * rows * cols
        ),
    )(tile, ahead_x, ahead_y, pinned(partial), *[pinned(b) for b in behind])


def shards(potential, elevation, normal_flux, box_owner, box_place, near_boxes):
    rows, cols = potential.shape
    count_tx = lax.axis_size("tx")
    count_ty = lax.axis_size("ty")
    node_count = rows * cols
    boxes = node_count // LANES
    near = near_boxes.shape[1]
    assert node_count % WIDE == 0 and cols <= 256 and rows <= 128
    assert 4 * (cols // LANES) <= EXTRA - 8
    assert node_count * count_tx * count_ty < 2**24

    plan = make_plan(near_boxes)
    slot = (box_owner * node_count + box_place).astype(F32)
    tile = jnp.stack([slot, elevation, potential, normal_flux])
    ahead_x = shifted(tile, "tx", -1)
    ahead_y = shifted(tile, "ty", -1)
    ahead_xy = shifted(ahead_y, "tx", -1)
    tile, ahead_x, ahead_y, ahead_xy = map(pinned, (tile, ahead_x, ahead_y, ahead_xy))

    sizes = (rows * count_tx, cols * count_ty)
    acc = scatter((0, 0), tile, None, False, *sizes)
    acc = scatter((1, 0), ahead_x, acc, False, *sizes)
    acc = scatter((0, 1), ahead_y, acc, False, *sizes)
    boxed = scatter((1, 1), ahead_xy, acc, True, *sizes)

    total = count_tx * count_ty
    both = ("tx", "ty")
    lower = lax.ppermute(boxed, both, [(i, i + 1) for i in range(total - 1)])
    upper = lax.ppermute(boxed, both, [(i + 1, i) for i in range(total - 1)])

    sums, turned, ztop = near_own(plan, boxed, near)
    value = near_other(plan, lower, upper, tile, sums, turned, ztop, near)

    behind_x = shifted(value, "tx", 1)
    behind_y = shifted(value, "ty", 1)
    diagonal = [
        (i * count_ty + j, (i + 1) % count_tx * count_ty + (j + 1) % count_ty)
        for i in range(count_tx)
        for j in range(count_ty)
    ]
    behind_xy = lax.ppermute(value, both, diagonal)
    partial = gather_own(tile, value)
    return finish(tile, ahead_x, ahead_y, partial, (behind_x, behind_y, behind_xy))


def solution(mesh):
    in_specs = (
        P("tx", "ty"),
        P("tx", "ty"),
        P("tx", "ty"),
        P("tx", "ty"),
        P("tx", "ty"),
        P(("tx", "ty"), None),
    )
    out_specs = (P("tx", "ty"), P("tx", "ty"))
    return jax.shard_map(shards, mesh=mesh, in_specs=in_specs, out_specs=out_specs, check_vma=False)
```

```python
import math

import jax
import jax.numpy as jnp
from jax import lax
from jax.experimental import pallas as pl
from jax.experimental.pallas import tpu as pltpu
from jax.sharding import PartitionSpec as P

LANES = 128
WIDE = 256
PIECES = 6
FEATURES = 32
USED = 24
EXTRA = 16
GROUP = 2
VMEM_LIMIT = 24 << 20
BF16 = jnp.bfloat16
F32 = jnp.float32


def shifted(value, axis, steps):
    count = lax.axis_size(axis)
    pairs = [(source, (source + steps) % count) for source in range(count)]
    return lax.ppermute(value, axis, pairs)


def ahead(axis, steps):
    index = lax.axis_index(axis) + steps
    count = lax.axis_size(axis)
    return jnp.where(index < 0, index + count, jnp.where(index >= count, index - count, index))


def pinned(value):
    return pltpu.with_memory_space_constraint(value, pltpu.VMEM)


def rounded(value):
    return value.astype(BF16).astype(F32)


def box_split(rel, high_count):
    box = jnp.floor(rel * (1.0 / LANES))
    second = box >= high_count
    high = jnp.where(second, box - high_count, box)
    low = rel - box * LANES
    return high, jnp.where(second, low + LANES, low)


def scatter_kernel(first, last, sizes, steps, tile, *refs):
    if first:
        listed, acc, plan = refs
        plan_rows(listed, plan)
    else:
        acc_in, acc = refs[:2]
    rows, cols, high_count, node_rows, node_cols = sizes
    p = lax.axis_index("tx")
    q = lax.axis_index("ty")
    base = ((p * lax.axis_size("ty") + q) * (rows * cols)).astype(F32)
    off_i = float(steps[0] * rows)
    off_j = float((steps[1] - 1) * cols)
    acc[...] = jnp.zeros(acc.shape, F32) if first else acc_in[...]
    units = [(r, c) for r in range(rows // 8) for c in range(cols // LANES)]

    def split(r, c):
        return box_split(tile[0, 8 * r : 8 * r + 8, LANES * c : LANES * c + LANES] - base, high_count)

    flags = []
    for r, c in units:
        high, _ = split(r, c)
        mine = (high >= 0.0) & (high < high_count)
        flags.append(jnp.max(jnp.where(mine, 1.0, 0.0)) > 0.0)

    for (r, c), flag in zip(units, flags):

        @pl.when(flag)
        def _():
            high, low = split(r, c)
            window = (slice(8 * r, 8 * r + 8), slice(LANES * c, LANES * c + LANES))
            z = 0.25 * tile[(1,) + window]
            z_high = rounded(z)
            z_low = z - z_high
            pot = tile[(2,) + window]
            flux = tile[(3,) + window]
            col_index = (lax.broadcasted_iota(jnp.int32, (high_count, LANES), 1) + LANES * c).astype(F32) + off_j
            high_iota = lax.broadcasted_iota(jnp.int32, (high_count, LANES), 0).astype(F32)
            low_iota = lax.broadcasted_iota(jnp.int32, (WIDE, LANES), 0).astype(F32)
            lefts = []
            rights = []
            for s in range(8):

                def row(v):
                    return v[s : s + 1, :]

                hit = high_iota == row(high)
                row_index = jnp.full((1, LANES), 8 * r + s, F32) + off_i
                values = [row_index, col_index, row(z_high), row(z_low), row(pot), row(flux)]
                lefts.append(
                    jnp.concatenate([jnp.where(hit, v, 0.0).astype(BF16) for v in values], axis=0)
                )
                rights.append(jnp.where(low_iota == row(low), 1.0, 0.0).astype(BF16))
            acc[...] += lax.dot_general(
                jnp.concatenate(lefts, axis=1),
                jnp.concatenate(rights, axis=1),
                (((1,), (1,)), ((), ())),
                preferred_element_type=F32,
            )

    if last:
        boxed = refs[-1]
        h = high_count
        row0 = (p * rows).astype(F32)
        col0 = ((q + 1) * cols).astype(F32)
        i = acc[0:h] + row0
        i = jnp.where(i >= node_rows, i - node_rows, i)
        j = acc[h : 2 * h] + col0
        j = jnp.where(j >= node_cols, j - node_cols, j)
        fields = [
            (i + 0.5) / node_rows,
            (j + 0.5) / node_cols,
            acc[2 * h : 3 * h] + acc[3 * h : 4 * h],
            acc[4 * h : 5 * h],
            acc[5 * h : 6 * h],
        ]
        for k, f in enumerate(fields):
            boxed[k, 0:h, :] = f[:, :LANES]
            boxed[k, h : 2 * h, :] = f[:, LANES:]


def scatter(steps, tile, acc, last, node_rows, node_cols, listed=None):
    _, rows, cols = tile.shape
    high_count = rows * cols // WIDE
    first = acc is None
    vmem = pl.BlockSpec(memory_space=pltpu.VMEM)
    out_shape = [pltpu.VMEM((PIECES * high_count, WIDE), F32)]
    if last:
        out_shape.append(pltpu.VMEM((5, 2 * high_count, LANES), F32))
    if first:
        near, boxes = listed.shape
        out_shape.append(jax.ShapeDtypeStruct(((near // 2 + near + 2 + 7) // 8 * 8, boxes), jnp.int32))
    args = (tile, listed) if first else (tile, pinned(acc))
    out = pl.pallas_call(
        lambda *refs: scatter_kernel(
            first, last, (rows, cols, high_count, node_rows, node_cols), steps, *refs
        ),
        out_shape=out_shape,
        in_specs=[vmem] * len(args),
        out_specs=[vmem] * len(out_shape),
        compiler_params=pltpu.CompilerParams(vmem_limit_bytes=VMEM_LIMIT),
        name="scatter_last" if last else "scatter_first" if first else "scatter",
        cost_estimate=pl.CostEstimate(
            flops=2 * PIECES * high_count * WIDE * rows * cols // 2,
            transcendentals=0,
            bytes_accessed=4 * (2 * PIECES * high_count * WIDE + 4 * rows * cols),
        ),
    )(*args)
    return out[1] if last else out if first else out[0]


def thirds(value):
    high = rounded(value)
    middle = rounded(value - high)
    return high, middle, value - high - middle


def plan_rows(listed, plan):
    near, boxes = listed.shape
    half = near // 2
    rank = lax.axis_index("tx") * lax.axis_size("ty") + lax.axis_index("ty")
    n = listed[...] - (rank - 1) * boxes
    taken = jnp.zeros((1, boxes), jnp.int32)
    left = jnp.zeros((1, boxes), jnp.int32)
    first = [jnp.full((1, boxes), boxes, jnp.int32) for _ in range(half)]
    rest = [jnp.full((1, boxes), 3 * boxes, jnp.int32) for _ in range(near)]
    for k in range(near):
        row = n[k : k + 1, :]
        take = (row >= boxes) & (row < 2 * boxes) & (taken < half)
        first = [jnp.where(take & (taken == j), row - boxes, v) for j, v in enumerate(first)]
        rest = [jnp.where(take | (left != j), v, row) for j, v in enumerate(rest)]
        step = jnp.where(take, 1, 0)
        taken = taken + step
        left = left + 1 - step
    for j, v in enumerate(first + rest):
        plan[j : j + 1, :] = v
    over = left > half
    flags = jnp.broadcast_to(jnp.where(over, 1.0, 0.0), (8, boxes)).astype(BF16)
    down = lax.broadcasted_iota(jnp.int32, (boxes, boxes), 0)
    across = lax.broadcasted_iota(jnp.int32, (boxes, boxes), 1)
    before = jnp.where(down < across, 1.0, 0.0).astype(BF16)
    offset = jnp.dot(flags, before, preferred_element_type=F32)[0:1, :]
    count = jnp.dot(flags, jnp.ones((boxes, boxes), BF16), preferred_element_type=F32)[0:1, :]
    hit = jnp.where((down.astype(F32) == offset) & over, 1.0, 0.0).astype(BF16)
    names = lax.broadcasted_iota(jnp.int32, (8, boxes), 1).astype(F32).astype(BF16)
    found = lax.dot_general(names, hit, (((1,), (1,)), ((), ())), preferred_element_type=F32)[0:1, :]
    count = count.astype(jnp.int32)
    plan[half + near : half + near + 1, :] = jnp.where(across[0:1, :] < count, found.astype(jnp.int32), boxes)
    plan[half + near + 1 : half + near + 2, :] = count


def pieces_of(ref, group):
    window = (slice(8 * group, 8 * group + 8), slice(None))
    x, y, z, pot, flux = (ref[(f,) + window] for f in range(5))
    pieces = []
    total = None
    for v in (x, y, z):
        high = rounded(v)
        low = rounded(v - high)
        kept = high + low
        pieces.append((high, low))
        total = kept * kept if total is None else total + kept * kept
    return pieces, total, pot, flux


def padded_rows(values):
    return values + [jnp.zeros_like(values[0])] * (USED - len(values))


def strided(ref, n):
    pitch = ref.shape[0] // USED
    rows = [ref[pl.ds(8 * g * pitch + n, 8, stride=pitch), :] for g in range(USED // 8)]
    return jnp.concatenate(rows + [jnp.zeros((8, LANES), F32)] * ((FEATURES - USED) // 8), axis=0)


def store_sources(refs, sfeat, smeta):
    pitch = sfeat.shape[0] // USED
    ones = jnp.ones((8, LANES), F32)
    zeros = jnp.zeros((8, LANES), F32)
    start = 0
    for ref in refs:
        for group in range(ref.shape[1] // 8):
            pieces, total, pot, flux = pieces_of(ref, group)
            source = []
            for high, low in pieces:
                source += [-2.0 * high, -2.0 * low, -2.0 * high, -2.0 * low]
            for k, v in enumerate(padded_rows(source + list(thirds(total)) + [ones, ones, ones])):
                sfeat[k * pitch + start : k * pitch + start + 8, :] = v
            z = pieces[2][0] + pieces[2][1]
            smeta[0, start : start + 8, :] = pot
            smeta[1, start : start + 8, :] = pot * z
            smeta[2, start : start + 8, :] = flux
            start += 8
    for k in range(USED):
        sfeat[k * pitch + start : k * pitch + start + 8, :] = ones if k == 12 else zeros
    for m in range(3):
        smeta[m, start : start + 8, :] = zeros


def store_targets(own, tfeat, turned):
    boxes = own.shape[1]
    pitch = tfeat.shape[0] // USED
    ones = jnp.ones((8, LANES), F32)
    for group in range(boxes // 8):
        pieces, total, _, _ = pieces_of(own, group)
        target = []
        for high, low in pieces:
            target += [high, high, low, low]
        for k, v in enumerate(padded_rows(target + [ones, ones, ones] + list(thirds(total + 0.04)))):
            tfeat[k * pitch + 8 * group : k * pitch + 8 * group + 8, :] = v
    turned[boxes] = jnp.zeros((LANES, FEATURES), BF16)

    def turn(i, carry):
        for u in range(8):
            turned[8 * i + u] = strided(tfeat, 8 * i + u).T.astype(BF16)
        return carry

    lax.fori_loop(0, boxes // 8, turn, 0)


def run_items(target_of, source_of, half, iterations, turned, ztop, sfeat, smeta, sums, squares, totals):
    empty_row = sums.shape[0] - 8

    def distances(group, squared):
        for i in range(GROUP):
            item = group * GROUP + i
            sides = [strided(sfeat, source_of(item, k)).astype(BF16) for k in range(half)]
            squared[i] = jnp.dot(
                turned[target_of(item)], jnp.concatenate(sides, axis=1), preferred_element_type=F32
            )

    def apply(group, squared, total):
        for i in range(GROUP):
            item = group * GROUP + i
            lane = jnp.full((8, LANES), jnp.minimum(target_of(item), LANES - 1), jnp.int32)
            metas = []
            for k in range(half):
                n = source_of(item, k)
                metas.append([jnp.broadcast_to(smeta[m, pl.ds(n, 1), :], (8, LANES)) for m in range(3)])
            for t in range(LANES // 8):
                rows = slice(8 * t, 8 * t + 8)
                z = jnp.take_along_axis(ztop[rows, :], lane, axis=1)
                value = None
                for k in range(half):
                    pot, pot_z, flux = metas[k]
                    inverse = lax.rsqrt(squared[i, rows, LANES * k : LANES * k + LANES])
                    part = inverse * (flux - (inverse * inverse) * (z * pot - pot_z))
                    value = part if value is None else value + part
                total[i, rows, :] = value

    def reduce(group, total, live):
        for i in range(GROUP):
            target = jnp.where(live, target_of(jnp.maximum(group * GROUP + i, 0)), empty_row)
            row = jnp.sum(total[i].T, axis=0, keepdims=True)
            sums[pl.ds(target, 1), :] += row

    (even_sq, odd_sq), (even_tot, odd_tot) = squares, totals
    odd_tot[...] = jnp.zeros(odd_tot.shape, F32)
    distances(0, even_sq)

    def step(i, carry):
        distances(2 * i + 1, odd_sq)
        apply(2 * i, even_sq, even_tot)
        reduce(2 * i - 1, odd_tot, i > 0)
        distances(2 * i + 2, even_sq)
        apply(2 * i + 1, odd_sq, odd_tot)
        reduce(2 * i, even_tot, True)
        return carry

    lax.fori_loop(0, iterations, step, 0)
    reduce(2 * iterations - 1, odd_tot, iterations > 0)


def near_own_kernel(plan, own, sums, turned, ztop, tfeat, sfeat, smeta, s0, s1, t0, t1):
    boxes = own.shape[1]
    half = s0.shape[2] // LANES
    sums[...] = jnp.zeros(sums.shape, F32)
    store_targets(own, tfeat, turned)
    high = rounded(own[2])
    ztop[...] = (high + rounded(own[2] - high)).T
    store_sources([own], sfeat, smeta)

    def target_of(item):
        return jnp.minimum(item, boxes - 1)

    def source_of(item, k):
        return plan[k, jnp.minimum(item, boxes - 1)]

    run_items(
        target_of, source_of, half, boxes // (2 * GROUP), turned, ztop, sfeat, smeta, sums, (s0, s1), (t0, t1)
    )


def near_other_kernel(
    near, plan, own, lower, upper, tile, sums_in, turned, ztop, out, sums, sfeat, smeta, s0, s1, t0, t1
):
    boxes = lower.shape[1]
    half = s0.shape[2] // LANES
    sums[...] = sums_in[...]
    store_sources([lower, own, upper], sfeat, smeta)
    items = boxes + plan[half + near + 1, 0]

    def box_of(item):
        extra = plan[half + near, jnp.clip(item - boxes, 0, boxes - 1)]
        return jnp.where(item < boxes, item, extra)

    def target_of(item):
        return jnp.where(item < items, box_of(item), boxes)

    def source_of(item, k):
        row = jnp.where(item < boxes, half, 2 * half) + k
        return plan[row, jnp.minimum(box_of(item), boxes - 1)]

    iterations = (items + 2 * GROUP - 1) // (2 * GROUP)
    run_items(
        target_of, source_of, half, iterations, turned, ztop, sfeat, smeta, sums, (s0, s1), (t0, t1)
    )
    out[0:boxes, :] = sums[0:boxes, :] * (1.0 / math.sqrt(near * LANES))

    _, rows, cols = tile.shape
    out[boxes : boxes + EXTRA, :] = jnp.zeros((EXTRA, LANES), F32)
    place = boxes
    for f in (1, 2):
        for r in (rows - 2, rows - 1):
            for c in range(cols // LANES):
                out[place : place + 1, :] = tile[f, r : r + 1, LANES * c : LANES * c + LANES]
                place += 1
    place = boxes + EXTRA - 8
    for f in (1, 2):
        turned_cols = tile[f, :, cols - LANES : cols].T
        out[place : place + 2, 0:rows] = turned_cols[LANES - 2 : LANES, :]
        place += 2


def item_scratch(sources, half):
    return [
        pltpu.VMEM((USED * (sources + 8), LANES), F32),
        pltpu.VMEM((3, sources + 8, LANES), F32),
        pltpu.VMEM((GROUP, LANES, half * LANES), F32),
        pltpu.VMEM((GROUP, LANES, half * LANES), F32),
        pltpu.VMEM((GROUP, LANES, LANES), F32),
        pltpu.VMEM((GROUP, LANES, LANES), F32),
    ]


def near_cost(boxes, near):
    pairs = boxes * near * LANES * LANES // 2
    return pl.CostEstimate(
        flops=pairs * 2 * FEATURES * 4, transcendentals=pairs, bytes_accessed=4 * 16 * boxes * LANES
    )


def near_own(plan, own, near):
    boxes = own.shape[1]
    assert boxes == LANES and boxes % (2 * GROUP) == 0 and near % 2 == 0
    vmem = pl.BlockSpec(memory_space=pltpu.VMEM)
    smem = pl.BlockSpec(memory_space=pltpu.SMEM)
    return pl.pallas_call(
        near_own_kernel,
        out_shape=(
            pltpu.VMEM((boxes + 8, LANES), F32),
            pltpu.VMEM((boxes + 1, LANES, FEATURES), BF16),
            pltpu.VMEM((LANES, boxes), F32),
        ),
        in_specs=[smem, vmem],
        out_specs=(vmem,) * 3,
        scratch_shapes=[pltpu.VMEM((USED * (boxes + 8), LANES), F32)] + item_scratch(boxes, near // 2),
        compiler_params=pltpu.CompilerParams(vmem_limit_bytes=VMEM_LIMIT),
        name="near_own",
        cost_estimate=near_cost(boxes, near),
    )(plan, pinned(own))


def near_other(plan, own, lower, upper, tile, sums, turned, ztop, near):
    boxes = lower.shape[1]
    vmem = pl.BlockSpec(memory_space=pltpu.VMEM)
    smem = pl.BlockSpec(memory_space=pltpu.SMEM)
    return pl.pallas_call(
        lambda *refs: near_other_kernel(near, *refs),
        out_shape=pltpu.VMEM((boxes + EXTRA, LANES), F32),
        in_specs=[smem] + [vmem] * 7,
        out_specs=vmem,
        scratch_shapes=[pltpu.VMEM((boxes + 8, LANES), F32)] + item_scratch(3 * boxes, near // 2),
        compiler_params=pltpu.CompilerParams(vmem_limit_bytes=VMEM_LIMIT),
        name="near_other",
        cost_estimate=near_cost(boxes, near),
    )(plan, *map(pinned, (own, lower, upper, tile, sums, turned, ztop)))


def lookup(slot, bases, tables, pieces, out):
    rows, cols = slot.shape
    high_count = rows * cols // WIDE
    units = [(r, c) for r in range(rows // 8) for c in range(cols // LANES)]
    for which, table in enumerate(tables):
        whole = jnp.concatenate([table[0:high_count, :], table[high_count : 2 * high_count, :]], axis=1)
        top = rounded(whole)
        pieces[which, 0:high_count, :] = top.astype(BF16)
        pieces[which, high_count : 2 * high_count, :] = (whole - top).astype(BF16)

    def split(r, c, which):
        window = (slice(8 * r, 8 * r + 8), slice(LANES * c, LANES * c + LANES))
        return box_split(slot[window] - bases[which], high_count)

    flags = {}
    for r, c in units:
        for which in range(len(tables)):
            high, _ = split(r, c, which)
            there = (high >= 0.0) & (high < high_count)
            flags[r, c, which] = jnp.max(jnp.where(there, 1.0, 0.0)) > 0.0

    for r, c in units:
        for which in range(len(tables)):

            @pl.when(flags[r, c, which])
            def _():
                high, low = split(r, c, which)
                low_iota = lax.broadcasted_iota(jnp.int32, (WIDE, LANES), 0).astype(F32)
                high_iota = lax.broadcasted_iota(jnp.int32, (high_count, LANES), 0).astype(F32)
                hits = jnp.concatenate(
                    [jnp.where(low_iota == low[s : s + 1, :], 1.0, 0.0).astype(BF16) for s in range(8)],
                    axis=1,
                )
                picked = jnp.dot(pieces[which], hits, preferred_element_type=F32)
                lines = []
                for s in range(8):
                    window = slice(LANES * s, LANES * s + LANES)
                    both = picked[0:high_count, window] + picked[high_count : 2 * high_count, window]
                    mine = high_iota == high[s : s + 1, :]
                    lines.append(jnp.sum(jnp.where(mine, both, 0.0), axis=0, keepdims=True))
                out[8 * r : 8 * r + 8, LANES * c : LANES * c + LANES] += jnp.concatenate(lines, axis=0)


def base_of(node_count, steps):
    rank = ahead("tx", -steps[0]) * lax.axis_size("ty") + ahead("ty", -steps[1])
    return (rank * node_count).astype(F32)


def gather_own_kernel(tile, own, out, pieces):
    out[...] = jnp.zeros(out.shape, F32)
    lookup(tile.at[0], [base_of(out.shape[0] * out.shape[1], (0, 0))], [own], pieces, out)


def gather_own(tile, own):
    _, rows, cols = tile.shape
    vmem = pl.BlockSpec(memory_space=pltpu.VMEM)
    return pl.pallas_call(
        gather_own_kernel,
        out_shape=pltpu.VMEM((rows, cols), F32),
        in_specs=[vmem] * 2,
        out_specs=vmem,
        scratch_shapes=[pltpu.VMEM((1, 2 * rows * cols // WIDE, WIDE), BF16)],
        compiler_params=pltpu.CompilerParams(vmem_limit_bytes=VMEM_LIMIT),
        name="gather_own",
        cost_estimate=pl.CostEstimate(
            flops=rows * cols * rows * cols, transcendentals=0, bytes_accessed=4 * 4 * rows * cols
        ),
    )(tile, pinned(own))


def finish_kernel(
    tile, ahead_x, ahead_y, partial, behind_x, behind_y, behind_xy, elev_rate, pot_rate, pieces, total, padded
):
    _, rows, cols = tile.shape
    boxes = rows * cols // LANES
    total[...] = partial[...]
    bases = [base_of(rows * cols, steps) for steps in ((1, 0), (0, 1), (1, 1))]
    lookup(tile.at[0], bases, [behind_x, behind_y, behind_xy], pieces, total)

    left_cols = behind_y[boxes + EXTRA - 8 : boxes + EXTRA, 0:rows].T
    col = lax.broadcasted_iota(jnp.int32, (rows, cols), 1)
    slopes = []
    for f in (1, 2):
        here = tile[f]
        padded[8 : 8 + rows, :] = here
        for r in range(2):
            for c in range(cols // LANES):
                source = boxes + ((f - 1) * 2 + r) * (cols // LANES) + c
                padded[6 + r : 7 + r, LANES * c : LANES * c + LANES] = behind_x[source : source + 1, :]
        padded[8 + rows : 10 + rows, :] = ahead_x[f, 0:2, :]
        along_rows = (
            padded[6 : 6 + rows, :]
            - 8.0 * padded[7 : 7 + rows, :]
            + 8.0 * padded[9 : 9 + rows, :]
            - padded[10 : 10 + rows, :]
        ) / 12.0
        left = left_cols[:, 2 * (f - 1) : 2 * f]
        right = ahead_y[f, :, 0:2]
        less_1 = jnp.where(col == 0, left[:, 1:2], pltpu.roll(here, 1, 1))
        less_2 = jnp.where(
            col == 0, left[:, 0:1], jnp.where(col == 1, left[:, 1:2], pltpu.roll(here, 2, 1))
        )
        more_1 = jnp.where(col == cols - 1, right[:, 0:1], pltpu.roll(here, cols - 1, 1))
        more_2 = jnp.where(
            col == cols - 2,
            right[:, 0:1],
            jnp.where(col == cols - 1, right[:, 1:2], pltpu.roll(here, cols - 2, 1)),
        )
        along_cols = (less_2 - 8.0 * less_1 + 8.0 * more_1 - more_2) / 12.0
        slopes.append((along_rows, along_cols))
    (elev_x, elev_y), (pot_x, pot_y) = slopes
    vertical = total[...]
    lift = 1.0 + elev_x * elev_x + elev_y * elev_y
    elev_rate[...] = vertical * lift - (pot_x * elev_x + pot_y * elev_y)
    pot_rate[...] = (
        -tile[1] - 0.5 * (pot_x * pot_x + pot_y * pot_y) + 0.5 * vertical * vertical * lift
    )


def finish(tile, ahead_x, ahead_y, partial, behind):
    _, rows, cols = tile.shape
    vmem = pl.BlockSpec(memory_space=pltpu.VMEM)
    shape = jax.ShapeDtypeStruct((rows, cols), F32)
    return pl.pallas_call(
        finish_kernel,
        out_shape=(shape, shape),
        in_specs=[vmem] * 7,
        out_specs=(vmem, vmem),
        scratch_shapes=[
            pltpu.VMEM((3, 2 * rows * cols // WIDE, WIDE), BF16),
            pltpu.VMEM((rows, cols), F32),
            pltpu.VMEM((rows + 16, cols), F32),
        ],
        compiler_params=pltpu.CompilerParams(vmem_limit_bytes=VMEM_LIMIT),
        name="finish",
        cost_estimate=pl.CostEstimate(
            flops=3 * rows * cols * rows * cols, transcendentals=0, bytes_accessed=4 * 8 * rows * cols
        ),
    )(tile, ahead_x, ahead_y, pinned(partial), *[pinned(b) for b in behind])


def shards(potential, elevation, normal_flux, box_owner, box_place, near_boxes):
    rows, cols = potential.shape
    count_tx = lax.axis_size("tx")
    count_ty = lax.axis_size("ty")
    node_count = rows * cols
    boxes = node_count // LANES
    near = near_boxes.shape[1]
    assert node_count % WIDE == 0 and cols <= 256 and rows <= 128
    assert 4 * (cols // LANES) <= EXTRA - 8
    assert node_count * count_tx * count_ty < 2**24

    slot = (box_owner * node_count + box_place).astype(F32)
    tile = jnp.stack([slot, elevation, potential, normal_flux])
    ahead_x = shifted(tile, "tx", -1)
    ahead_y = shifted(tile, "ty", -1)
    ahead_xy = shifted(ahead_y, "tx", -1)
    tile, ahead_x, ahead_y, ahead_xy = map(pinned, (tile, ahead_x, ahead_y, ahead_xy))

    sizes = (rows * count_tx, cols * count_ty)
    acc, plan = scatter((0, 0), tile, None, False, *sizes, near_boxes.T)
    acc = scatter((1, 0), ahead_x, acc, False, *sizes)
    acc = scatter((0, 1), ahead_y, acc, False, *sizes)
    boxed = scatter((1, 1), ahead_xy, acc, True, *sizes)

    total = count_tx * count_ty
    both = ("tx", "ty")
    lower = lax.ppermute(boxed, both, [(i, i + 1) for i in range(total - 1)])
    upper = lax.ppermute(boxed, both, [(i + 1, i) for i in range(total - 1)])

    sums, turned, ztop = near_own(plan, boxed, near)
    value = near_other(plan, boxed, lower, upper, tile, sums, turned, ztop, near)

    behind_x = shifted(value, "tx", 1)
    behind_y = shifted(value, "ty", 1)
    diagonal = [
        (i * count_ty + j, (i + 1) % count_tx * count_ty + (j + 1) % count_ty)
        for i in range(count_tx)
        for j in range(count_ty)
    ]
    behind_xy = lax.ppermute(value, both, diagonal)
    partial = gather_own(tile, value)
    return finish(tile, ahead_x, ahead_y, partial, (behind_x, behind_y, behind_xy))


def solution(mesh):
    in_specs = (
        P("tx", "ty"),
        P("tx", "ty"),
        P("tx", "ty"),
        P("tx", "ty"),
        P("tx", "ty"),
        P(("tx", "ty"), None),
    )
    out_specs = (P("tx", "ty"), P("tx", "ty"))
    return jax.shard_map(shards, mesh=mesh, in_specs=in_specs, out_specs=out_specs, check_vma=False)
```

```python
import math

import jax
import jax.numpy as jnp
from jax import lax
from jax.experimental import pallas as pl
from jax.experimental.pallas import tpu as pltpu
from jax.sharding import PartitionSpec as P

LANES = 128
WIDE = 256
PIECES = 6
FEATURES = 32
USED = 24
STORED = USED + 8
EXTRA = 16
GROUP = 8
VMEM_LIMIT = 24 << 20
BF16 = jnp.bfloat16
F32 = jnp.float32


def shifted(value, axis, steps):
    count = lax.axis_size(axis)
    pairs = [(source, (source + steps) % count) for source in range(count)]
    return lax.ppermute(value, axis, pairs)


def ahead(axis, steps):
    index = lax.axis_index(axis) + steps
    count = lax.axis_size(axis)
    return jnp.where(index < 0, index + count, jnp.where(index >= count, index - count, index))


def pinned(value):
    return pltpu.with_memory_space_constraint(value, pltpu.VMEM)


def rounded(value):
    return value.astype(BF16).astype(F32)


def box_split(rel, high_count):
    box = jnp.floor(rel * (1.0 / LANES))
    second = box >= high_count
    high = jnp.where(second, box - high_count, box)
    low = rel - box * LANES
    return high, jnp.where(second, low + LANES, low)


def scatter_kernel(first, last, sizes, steps, tile, *refs):
    if first:
        listed, acc, plan = refs
        plan_rows(listed, plan)
    else:
        acc_in, acc = refs[:2]
    rows, cols, high_count, node_rows, node_cols = sizes
    p = lax.axis_index("tx")
    q = lax.axis_index("ty")
    base = ((p * lax.axis_size("ty") + q) * (rows * cols)).astype(F32)
    off_i = float(steps[0] * rows)
    off_j = float((steps[1] - 1) * cols)
    acc[...] = jnp.zeros(acc.shape, F32) if first else acc_in[...]
    units = [(r, c) for r in range(rows // 8) for c in range(cols // LANES)]

    def split(r, c):
        return box_split(tile[0, 8 * r : 8 * r + 8, LANES * c : LANES * c + LANES] - base, high_count)

    flags = []
    for r, c in units:
        high, _ = split(r, c)
        mine = (high >= 0.0) & (high < high_count)
        flags.append(jnp.max(jnp.where(mine, 1.0, 0.0)) > 0.0)

    for (r, c), flag in zip(units, flags):

        @pl.when(flag)
        def _():
            high, low = split(r, c)
            window = (slice(8 * r, 8 * r + 8), slice(LANES * c, LANES * c + LANES))
            z = 0.25 * tile[(1,) + window]
            z_high = rounded(z)
            z_low = z - z_high
            pot = tile[(2,) + window]
            flux = tile[(3,) + window]
            col_index = (lax.broadcasted_iota(jnp.int32, (high_count, LANES), 1) + LANES * c).astype(F32) + off_j
            high_iota = lax.broadcasted_iota(jnp.int32, (high_count, LANES), 0).astype(F32)
            low_iota = lax.broadcasted_iota(jnp.int32, (WIDE, LANES), 0).astype(F32)
            lefts = []
            rights = []
            for s in range(8):

                def row(v):
                    return v[s : s + 1, :]

                hit = high_iota == row(high)
                row_index = jnp.full((1, LANES), 8 * r + s, F32) + off_i
                values = [row_index, col_index, row(z_high), row(z_low), row(pot), row(flux)]
                lefts.append(
                    jnp.concatenate([jnp.where(hit, v, 0.0).astype(BF16) for v in values], axis=0)
                )
                rights.append(jnp.where(low_iota == row(low), 1.0, 0.0).astype(BF16))
            acc[...] += lax.dot_general(
                jnp.concatenate(lefts, axis=1),
                jnp.concatenate(rights, axis=1),
                (((1,), (1,)), ((), ())),
                preferred_element_type=F32,
            )

    if last:
        boxed = refs[-1]
        h = high_count
        row0 = (p * rows).astype(F32)
        col0 = ((q + 1) * cols).astype(F32)
        i = acc[0:h] + row0
        i = jnp.where(i >= node_rows, i - node_rows, i)
        j = acc[h : 2 * h] + col0
        j = jnp.where(j >= node_cols, j - node_cols, j)
        fields = [
            (i + 0.5) / node_rows,
            (j + 0.5) / node_cols,
            acc[2 * h : 3 * h] + acc[3 * h : 4 * h],
            acc[4 * h : 5 * h],
            acc[5 * h : 6 * h],
        ]
        for k, f in enumerate(fields):
            boxed[k, 0:h, :] = f[:, :LANES]
            boxed[k, h : 2 * h, :] = f[:, LANES:]


def scatter(steps, tile, acc, last, node_rows, node_cols, listed=None):
    _, rows, cols = tile.shape
    high_count = rows * cols // WIDE
    first = acc is None
    vmem = pl.BlockSpec(memory_space=pltpu.VMEM)
    out_shape = [pltpu.VMEM((PIECES * high_count, WIDE), F32)]
    if last:
        out_shape.append(pltpu.VMEM((5, 2 * high_count, LANES), F32))
    if first:
        near, boxes = listed.shape
        out_shape.append(jax.ShapeDtypeStruct(((near // 2 + near + 2 + 7) // 8 * 8, boxes), jnp.int32))
    args = (tile, listed) if first else (tile, pinned(acc))
    out = pl.pallas_call(
        lambda *refs: scatter_kernel(
            first, last, (rows, cols, high_count, node_rows, node_cols), steps, *refs
        ),
        out_shape=out_shape,
        in_specs=[vmem] * len(args),
        out_specs=[vmem] * len(out_shape),
        compiler_params=pltpu.CompilerParams(vmem_limit_bytes=VMEM_LIMIT),
        name="scatter_last" if last else "scatter_first" if first else "scatter",
        cost_estimate=pl.CostEstimate(
            flops=2 * PIECES * high_count * WIDE * rows * cols // 2,
            transcendentals=0,
            bytes_accessed=4 * (2 * PIECES * high_count * WIDE + 4 * rows * cols),
        ),
    )(*args)
    return out[1] if last else out if first else out[0]


def thirds(value):
    high = rounded(value)
    middle = rounded(value - high)
    return high, middle, value - high - middle


def plan_rows(listed, plan):
    near, boxes = listed.shape
    half = near // 2
    rank = lax.axis_index("tx") * lax.axis_size("ty") + lax.axis_index("ty")
    n = listed[...] - (rank - 1) * boxes
    taken = jnp.zeros((1, boxes), jnp.int32)
    left = jnp.zeros((1, boxes), jnp.int32)
    first = [jnp.full((1, boxes), boxes, jnp.int32) for _ in range(half)]
    rest = [jnp.full((1, boxes), 3 * boxes, jnp.int32) for _ in range(near)]
    for k in range(near):
        row = n[k : k + 1, :]
        take = (row >= boxes) & (row < 2 * boxes) & (taken < half)
        first = [jnp.where(take & (taken == j), row - boxes, v) for j, v in enumerate(first)]
        rest = [jnp.where(take | (left != j), v, row) for j, v in enumerate(rest)]
        step = jnp.where(take, 1, 0)
        taken = taken + step
        left = left + 1 - step
    for j, v in enumerate(first + rest):
        plan[j : j + 1, :] = v
    over = left > half
    flags = jnp.broadcast_to(jnp.where(over, 1.0, 0.0), (8, boxes)).astype(BF16)
    down = lax.broadcasted_iota(jnp.int32, (boxes, boxes), 0)
    across = lax.broadcasted_iota(jnp.int32, (boxes, boxes), 1)
    before = jnp.where(down < across, 1.0, 0.0).astype(BF16)
    offset = jnp.dot(flags, before, preferred_element_type=F32)[0:1, :]
    count = jnp.dot(flags, jnp.ones((boxes, boxes), BF16), preferred_element_type=F32)[0:1, :]
    hit = jnp.where((down.astype(F32) == offset) & over, 1.0, 0.0).astype(BF16)
    names = lax.broadcasted_iota(jnp.int32, (8, boxes), 1).astype(F32).astype(BF16)
    found = lax.dot_general(names, hit, (((1,), (1,)), ((), ())), preferred_element_type=F32)[0:1, :]
    count = count.astype(jnp.int32)
    plan[half + near : half + near + 1, :] = jnp.where(across[0:1, :] < count, found.astype(jnp.int32), boxes)
    plan[half + near + 1 : half + near + 2, :] = count


def pieces_of(ref, group):
    window = (slice(8 * group, 8 * group + 8), slice(None))
    x, y, z, pot, flux = (ref[(f,) + window] for f in range(5))
    pieces = []
    total = None
    for v in (x, y, z):
        high = rounded(v)
        low = rounded(v - high)
        kept = high + low
        pieces.append((high, low))
        total = kept * kept if total is None else total + kept * kept
    return pieces, total, pot, flux


def padded_rows(values):
    return values + [jnp.zeros_like(values[0])] * (USED - len(values))


def moment_side(ref, n):
    pitch = ref.shape[0] // STORED
    rows = ref[pl.ds(USED * pitch + n, 8, stride=pitch), :]
    zeros = jnp.zeros((8, LANES), F32)
    return jnp.concatenate([zeros, rows] + [zeros] * (FEATURES // 8 - 2), axis=0).astype(BF16)


def strided(ref, n, stored):
    pitch = ref.shape[0] // stored
    rows = [ref[pl.ds(8 * g * pitch + n, 8, stride=pitch), :] for g in range(USED // 8)]
    return jnp.concatenate(rows + [jnp.zeros((8, LANES), F32)] * ((FEATURES - USED) // 8), axis=0)


def store_sources(refs, sfeat, sflux):
    pitch = sfeat.shape[0] // STORED
    ones = jnp.ones((8, LANES), F32)
    zeros = jnp.zeros((8, LANES), F32)
    start = 0
    for ref in refs:
        for group in range(ref.shape[1] // 8):
            pieces, total, pot, flux = pieces_of(ref, group)
            source = []
            for high, low in pieces:
                source += [-2.0 * high, -2.0 * low, -2.0 * high, -2.0 * low]
            z = pieces[2][0] + pieces[2][1]
            rows = padded_rows(source + list(thirds(total)) + [ones, ones, ones])
            rows += [pot, zeros, pot, zeros] + list(thirds(-pot * z)) + [zeros]
            for k, v in enumerate(rows):
                sfeat[k * pitch + start : k * pitch + start + 8, :] = v
            sflux[start : start + 8, :] = flux
            start += 8
    for k in range(STORED):
        sfeat[k * pitch + start : k * pitch + start + 8, :] = ones if k == 12 else zeros
    sflux[start : start + 8, :] = zeros


def store_targets(own, tfeat, turned):
    boxes = own.shape[1]
    pitch = tfeat.shape[0] // USED
    ones = jnp.ones((8, LANES), F32)
    for group in range(boxes // 8):
        pieces, total, _, _ = pieces_of(own, group)
        target = []
        for high, low in pieces:
            target += [high, high, low, low]
        for k, v in enumerate(padded_rows(target + [ones, ones, ones] + list(thirds(total + 0.04)))):
            tfeat[k * pitch + 8 * group : k * pitch + 8 * group + 8, :] = v
    turned[boxes] = jnp.zeros((LANES, FEATURES), BF16)

    def turn(i, carry):
        for u in range(8):
            turned[8 * i + u] = strided(tfeat, 8 * i + u, USED).T.astype(BF16)
        return carry

    lax.fori_loop(0, boxes // 8, turn, 0)


def run_items(target_of, source_of, half, iterations, turned, sfeat, sflux, sums, totals):
    empty_row = sums.shape[0] - 8

    def apply(item, total):
        target = target_of(item)
        sides = [strided(sfeat, source_of(item, k), STORED).astype(BF16) for k in range(half)]
        sides += [moment_side(sfeat, source_of(item, k)) for k in range(half)]
        squared = jnp.dot(turned[target], jnp.concatenate(sides, axis=1), preferred_element_type=F32)
        fluxes = [
            jnp.broadcast_to(sflux[pl.ds(source_of(item, k), 1), :], (8, LANES)) for k in range(half)
        ]
        for t in range(LANES // 8):
            rows = slice(8 * t, 8 * t + 8)
            value = None
            for k, flux in enumerate(fluxes):
                inverse = lax.rsqrt(squared[rows, LANES * k : LANES * (k + 1)])
                moment = squared[rows, LANES * (half + k) : LANES * (half + k + 1)]
                part = inverse * (flux - (inverse * inverse) * moment)
                value = part if value is None else value + part
            total[rows, :] = value

    def reduce(item, total, live):
        target = jnp.where(live, target_of(jnp.maximum(item, 0)), empty_row)
        sums[pl.ds(target, 1), :] += jnp.sum(total[...].T, axis=0, keepdims=True)

    def step(i, carry):
        for u in range(GROUP):
            reduce(GROUP * (i - 1) + u, totals.at[u], i > 0)
        for u in range(GROUP):
            apply(GROUP * i + u, totals.at[u])
        return carry

    totals[...] = jnp.zeros(totals.shape, F32)
    lax.fori_loop(0, iterations, step, 0)
    for u in range(GROUP):
        reduce(GROUP * (iterations - 1) + u, totals.at[u], iterations > 0)


def near_own_kernel(near, plan, own, sums, turned, tfeat, sfeat, sflux, totals):
    boxes = own.shape[1]
    half = near // 2
    sums[...] = jnp.zeros(sums.shape, F32)
    store_targets(own, tfeat, turned)
    store_sources([own], sfeat, sflux)

    def target_of(item):
        return jnp.minimum(item, boxes - 1)

    def source_of(item, k):
        return plan[k, jnp.minimum(item, boxes - 1)]

    run_items(
        target_of, source_of, half, boxes // GROUP, turned, sfeat, sflux, sums, totals
    )


def near_other_kernel(
    near, plan, own, lower, upper, tile, sums_in, turned, out, sums, sfeat, sflux, totals
):
    boxes = lower.shape[1]
    half = near // 2
    sums[...] = sums_in[...]
    store_sources([lower, own, upper], sfeat, sflux)
    items = boxes + plan[half + near + 1, 0]

    def box_of(item):
        extra = plan[half + near, jnp.clip(item - boxes, 0, boxes - 1)]
        return jnp.where(item < boxes, item, extra)

    def target_of(item):
        return jnp.where(item < items, box_of(item), boxes)

    def source_of(item, k):
        row = jnp.where(item < boxes, half, 2 * half) + k
        return plan[row, jnp.minimum(box_of(item), boxes - 1)]

    iterations = (items + GROUP - 1) // GROUP
    run_items(
        target_of, source_of, half, iterations, turned, sfeat, sflux, sums, totals
    )
    out[0:boxes, :] = sums[0:boxes, :] * (1.0 / math.sqrt(near * LANES))

    _, rows, cols = tile.shape
    out[boxes : boxes + EXTRA, :] = jnp.zeros((EXTRA, LANES), F32)
    place = boxes
    for f in (1, 2):
        for r in (rows - 2, rows - 1):
            for c in range(cols // LANES):
                out[place : place + 1, :] = tile[f, r : r + 1, LANES * c : LANES * c + LANES]
                place += 1
    place = boxes + EXTRA - 8
    for f in (1, 2):
        turned_cols = tile[f, :, cols - LANES : cols].T
        out[place : place + 2, 0:rows] = turned_cols[LANES - 2 : LANES, :]
        place += 2


def item_scratch(sources):
    return [
        pltpu.VMEM((STORED * (sources + 8), LANES), F32),
        pltpu.VMEM((sources + 8, LANES), F32),
        pltpu.VMEM((GROUP, LANES, LANES), F32),
    ]


def near_cost(boxes, near):
    pairs = boxes * near * LANES * LANES // 2
    return pl.CostEstimate(
        flops=pairs * 2 * FEATURES * 4, transcendentals=pairs, bytes_accessed=4 * 16 * boxes * LANES
    )


def near_own(plan, own, near):
    boxes = own.shape[1]
    assert boxes == LANES and boxes % GROUP == 0 and near % 2 == 0
    vmem = pl.BlockSpec(memory_space=pltpu.VMEM)
    smem = pl.BlockSpec(memory_space=pltpu.SMEM)
    return pl.pallas_call(
        lambda *refs: near_own_kernel(near, *refs),
        out_shape=(
            pltpu.VMEM((boxes + 8, LANES), F32),
            pltpu.VMEM((boxes + 1, LANES, FEATURES), BF16),
        ),
        in_specs=[smem, vmem],
        out_specs=(vmem,) * 2,
        scratch_shapes=[pltpu.VMEM((USED * (boxes + 8), LANES), F32)] + item_scratch(boxes),
        compiler_params=pltpu.CompilerParams(vmem_limit_bytes=VMEM_LIMIT),
        name="near_own",
        cost_estimate=near_cost(boxes, near),
    )(plan, pinned(own))


def near_other(plan, own, lower, upper, tile, sums, turned, near):
    boxes = lower.shape[1]
    vmem = pl.BlockSpec(memory_space=pltpu.VMEM)
    smem = pl.BlockSpec(memory_space=pltpu.SMEM)
    return pl.pallas_call(
        lambda *refs: near_other_kernel(near, *refs),
        out_shape=pltpu.VMEM((boxes + EXTRA, LANES), F32),
        in_specs=[smem] + [vmem] * 6,
        out_specs=vmem,
        scratch_shapes=[pltpu.VMEM((boxes + 8, LANES), F32)] + item_scratch(3 * boxes),
        compiler_params=pltpu.CompilerParams(vmem_limit_bytes=VMEM_LIMIT),
        name="near_other",
        cost_estimate=near_cost(boxes, near),
    )(plan, *map(pinned, (own, lower, upper, tile, sums, turned)))


def lookup(slot, bases, tables, pieces, out):
    rows, cols = slot.shape
    high_count = rows * cols // WIDE
    units = [(r, c) for r in range(rows // 8) for c in range(cols // LANES)]
    for which, table in enumerate(tables):
        whole = jnp.concatenate([table[0:high_count, :], table[high_count : 2 * high_count, :]], axis=1)
        top = rounded(whole)
        pieces[which, 0:high_count, :] = top.astype(BF16)
        pieces[which, high_count : 2 * high_count, :] = (whole - top).astype(BF16)

    def split(r, c, which):
        window = (slice(8 * r, 8 * r + 8), slice(LANES * c, LANES * c + LANES))
        return box_split(slot[window] - bases[which], high_count)

    flags = {}
    for r, c in units:
        for which in range(len(tables)):
            high, _ = split(r, c, which)
            there = (high >= 0.0) & (high < high_count)
            flags[r, c, which] = jnp.max(jnp.where(there, 1.0, 0.0)) > 0.0

    for r, c in units:
        for which in range(len(tables)):

            @pl.when(flags[r, c, which])
            def _():
                high, low = split(r, c, which)
                low_iota = lax.broadcasted_iota(jnp.int32, (WIDE, LANES), 0).astype(F32)
                high_iota = lax.broadcasted_iota(jnp.int32, (high_count, LANES), 0).astype(F32)
                hits = jnp.concatenate(
                    [jnp.where(low_iota == low[s : s + 1, :], 1.0, 0.0).astype(BF16) for s in range(8)],
                    axis=1,
                )
                picked = jnp.dot(pieces[which], hits, preferred_element_type=F32)
                lines = []
                for s in range(8):
                    window = slice(LANES * s, LANES * s + LANES)
                    both = picked[0:high_count, window] + picked[high_count : 2 * high_count, window]
                    mine = high_iota == high[s : s + 1, :]
                    lines.append(jnp.sum(jnp.where(mine, both, 0.0), axis=0, keepdims=True))
                out[8 * r : 8 * r + 8, LANES * c : LANES * c + LANES] += jnp.concatenate(lines, axis=0)


def base_of(node_count, steps):
    rank = ahead("tx", -steps[0]) * lax.axis_size("ty") + ahead("ty", -steps[1])
    return (rank * node_count).astype(F32)


def own_kernel(tile, table, out, pieces):
    out[...] = jnp.zeros(out.shape, F32)
    lookup(tile.at[0], [base_of(out.shape[0] * out.shape[1], (0, 0))], [table], pieces, out)


def row_kernel(tile, ahead_x, partial, behind_x, out, slopes, pieces, padded):
    _, rows, cols = tile.shape
    boxes = rows * cols // LANES
    out[...] = partial[...]
    lookup(tile.at[0], [base_of(rows * cols, (1, 0))], [behind_x], pieces, out)
    for f in (1, 2):
        padded[8 : 8 + rows, :] = tile[f]
        for r in range(2):
            for c in range(cols // LANES):
                source = boxes + ((f - 1) * 2 + r) * (cols // LANES) + c
                padded[6 + r : 7 + r, LANES * c : LANES * c + LANES] = behind_x[source : source + 1, :]
        padded[8 + rows : 10 + rows, :] = ahead_x[f, 0:2, :]
        slopes[f - 1] = (
            padded[6 : 6 + rows, :]
            - 8.0 * padded[7 : 7 + rows, :]
            + 8.0 * padded[9 : 9 + rows, :]
            - padded[10 : 10 + rows, :]
        ) / 12.0


def col_kernel(tile, ahead_y, partial, behind_y, out, slopes, pieces):
    _, rows, cols = tile.shape
    boxes = rows * cols // LANES
    out[...] = partial[...]
    lookup(tile.at[0], [base_of(rows * cols, (0, 1))], [behind_y], pieces, out)
    left_cols = behind_y[boxes + EXTRA - 8 : boxes + EXTRA, 0:rows].T
    col = lax.broadcasted_iota(jnp.int32, (rows, cols), 1)
    for f in (1, 2):
        here = tile[f]
        left = left_cols[:, 2 * (f - 1) : 2 * f]
        right = ahead_y[f, :, 0:2]
        less_1 = jnp.where(col == 0, left[:, 1:2], pltpu.roll(here, 1, 1))
        less_2 = jnp.where(
            col == 0, left[:, 0:1], jnp.where(col == 1, left[:, 1:2], pltpu.roll(here, 2, 1))
        )
        more_1 = jnp.where(col == cols - 1, right[:, 0:1], pltpu.roll(here, cols - 1, 1))
        more_2 = jnp.where(
            col == cols - 2,
            right[:, 0:1],
            jnp.where(col == cols - 1, right[:, 1:2], pltpu.roll(here, cols - 2, 1)),
        )
        slopes[f - 1] = (less_2 - 8.0 * less_1 + 8.0 * more_1 - more_2) / 12.0


def last_kernel(tile, row_slopes, col_slopes, partial, behind_xy, elev_rate, pot_rate, pieces, total):
    _, rows, cols = tile.shape
    total[...] = partial[...]
    lookup(tile.at[0], [base_of(rows * cols, (1, 1))], [behind_xy], pieces, total)
    elev_x, pot_x = row_slopes[0], row_slopes[1]
    elev_y, pot_y = col_slopes[0], col_slopes[1]
    vertical = total[...]
    lift = 1.0 + elev_x * elev_x + elev_y * elev_y
    elev_rate[...] = vertical * lift - (pot_x * elev_x + pot_y * elev_y)
    pot_rate[...] = (
        -tile[1] - 0.5 * (pot_x * pot_x + pot_y * pot_y) + 0.5 * vertical * vertical * lift
    )


def lookup_call(kernel, name, out_shape, args, scratch):
    _, rows, cols = args[0].shape
    vmem = pl.BlockSpec(memory_space=pltpu.VMEM)
    return pl.pallas_call(
        kernel,
        out_shape=out_shape,
        in_specs=[vmem] * len(args),
        out_specs=(vmem,) * len(out_shape),
        scratch_shapes=[pltpu.VMEM((1, 2 * rows * cols // WIDE, WIDE), BF16)] + scratch,
        compiler_params=pltpu.CompilerParams(vmem_limit_bytes=VMEM_LIMIT),
        name=name,
        cost_estimate=pl.CostEstimate(
            flops=rows * cols * rows * cols, transcendentals=0, bytes_accessed=4 * 8 * rows * cols
        ),
    )(*map(pinned, args))


def look_up_all(tile, ahead_x, ahead_y, value, behind_x, behind_y, behind_xy):
    _, rows, cols = tile.shape
    values = pltpu.VMEM((rows, cols), F32)
    slopes = pltpu.VMEM((2, rows, cols), F32)
    (partial,) = lookup_call(own_kernel, "lookup_own", (values,), (tile, value), [])
    partial, row_slopes = lookup_call(
        row_kernel,
        "lookup_x",
        (values, slopes),
        (tile, ahead_x, partial, behind_x),
        [pltpu.VMEM((rows + 16, cols), F32)],
    )
    partial, col_slopes = lookup_call(
        col_kernel, "lookup_y", (values, slopes), (tile, ahead_y, partial, behind_y), []
    )
    shape = jax.ShapeDtypeStruct((rows, cols), F32)
    return lookup_call(
        last_kernel,
        "lookup_xy",
        (shape, shape),
        (tile, row_slopes, col_slopes, partial, behind_xy),
        [pltpu.VMEM((rows, cols), F32)],
    )


def pack_kernel(owner, place, elevation, potential, flux, tile):
    node_count = owner.shape[0] * owner.shape[1]
    tile[0] = (owner[...] * node_count + place[...]).astype(F32)
    tile[1] = elevation[...]
    tile[2] = potential[...]
    tile[3] = flux[...]


def pack(owner, place, elevation, potential, flux):
    vmem = pl.BlockSpec(memory_space=pltpu.VMEM)
    return pl.pallas_call(
        pack_kernel,
        out_shape=pltpu.VMEM((4,) + owner.shape, F32),
        in_specs=[vmem] * 5,
        out_specs=vmem,
        compiler_params=pltpu.CompilerParams(vmem_limit_bytes=VMEM_LIMIT),
        name="pack",
    )(owner, place, elevation, potential, flux)


def shards(potential, elevation, normal_flux, box_owner, box_place, near_boxes):
    rows, cols = potential.shape
    count_tx = lax.axis_size("tx")
    count_ty = lax.axis_size("ty")
    node_count = rows * cols
    boxes = node_count // LANES
    near = near_boxes.shape[1]
    assert node_count % WIDE == 0 and cols <= 256 and rows <= 128
    assert 4 * (cols // LANES) <= EXTRA - 8
    assert node_count * count_tx * count_ty < 2**24

    tile = pack(box_owner, box_place, elevation, potential, normal_flux)
    ahead_x = shifted(tile, "tx", -1)
    ahead_y = shifted(tile, "ty", -1)
    ahead_xy = shifted(ahead_y, "tx", -1)
    tile, ahead_x, ahead_y, ahead_xy = map(pinned, (tile, ahead_x, ahead_y, ahead_xy))

    sizes = (rows * count_tx, cols * count_ty)
    acc, plan = scatter((0, 0), tile, None, False, *sizes, near_boxes.T)
    acc = scatter((1, 0), ahead_x, acc, False, *sizes)
    acc = scatter((0, 1), ahead_y, acc, False, *sizes)
    boxed = scatter((1, 1), ahead_xy, acc, True, *sizes)

    total = count_tx * count_ty
    both = ("tx", "ty")
    lower = lax.ppermute(boxed, both, [(i, i + 1) for i in range(total - 1)])
    upper = lax.ppermute(boxed, both, [(i + 1, i) for i in range(total - 1)])

    sums, turned = near_own(plan, boxed, near)
    value = near_other(plan, boxed, lower, upper, tile, sums, turned, near)

    behind_x = shifted(value, "tx", 1)
    behind_y = shifted(value, "ty", 1)
    diagonal = [
        (i * count_ty + j, (i + 1) % count_tx * count_ty + (j + 1) % count_ty)
        for i in range(count_tx)
        for j in range(count_ty)
    ]
    behind_xy = lax.ppermute(value, both, diagonal)
    return look_up_all(tile, ahead_x, ahead_y, value, behind_x, behind_y, behind_xy)


def solution(mesh):
    in_specs = (
        P("tx", "ty"),
        P("tx", "ty"),
        P("tx", "ty"),
        P("tx", "ty"),
        P("tx", "ty"),
        P(("tx", "ty"), None),
    )
    out_specs = (P("tx", "ty"), P("tx", "ty"))
    return jax.shard_map(shards, mesh=mesh, in_specs=in_specs, out_specs=out_specs, check_vma=False)
```

```python
import math

import jax
import jax.numpy as jnp
from jax import lax
from jax.experimental import pallas as pl
from jax.experimental.pallas import tpu as pltpu
from jax.sharding import PartitionSpec as P

LANES = 128
WIDE = 256
PIECES = 6
FEATURES = 32
USED = 24
STORED = USED + 8
EXTRA = 16
GROUP = 8
VMEM_LIMIT = 24 << 20
BF16 = jnp.bfloat16
F32 = jnp.float32


def shifted(value, axis, steps):
    count = lax.axis_size(axis)
    pairs = [(source, (source + steps) % count) for source in range(count)]
    return lax.ppermute(value, axis, pairs)


def ahead(axis, steps):
    index = lax.axis_index(axis) + steps
    count = lax.axis_size(axis)
    return jnp.where(index < 0, index + count, jnp.where(index >= count, index - count, index))


def pinned(value):
    return pltpu.with_memory_space_constraint(value, pltpu.VMEM)


def rounded(value):
    return value.astype(BF16).astype(F32)


def box_split(rel, high_count):
    box = jnp.floor(rel * (1.0 / LANES))
    second = box >= high_count
    high = jnp.where(second, box - high_count, box)
    low = rel - box * LANES
    return high, jnp.where(second, low + LANES, low)


def list_active(test, count, active):
    flags = [jnp.max(jnp.where(test(unit), 1.0, 0.0)) > 0.0 for unit in range(count)]
    found = jnp.int32(0)
    for unit, flag in enumerate(flags):
        active[found] = unit
        found = found + jnp.where(flag, 1, 0)
    return found


def scatter_kernel(first, last, sizes, steps, tile, *refs):
    active = refs[-1]
    if first:
        listed, acc, plan = refs[:3]
        plan_rows(listed, plan)
    else:
        acc_in, acc = refs[:2]
    rows, cols, high_count, node_rows, node_cols = sizes
    p = lax.axis_index("tx")
    q = lax.axis_index("ty")
    base = ((p * lax.axis_size("ty") + q) * (rows * cols)).astype(F32)
    off_i = float(steps[0] * rows)
    off_j = float((steps[1] - 1) * cols)
    acc[...] = jnp.zeros(acc.shape, F32) if first else acc_in[...]
    across = cols // LANES

    def window_of(unit):
        row, col = unit // across * 8, unit % across * LANES
        if not isinstance(unit, int):
            row, col = pl.multiple_of(row, 8), pl.multiple_of(col, LANES)
        return row, col, (pl.ds(row, 8), pl.ds(col, LANES))

    def mine(unit):
        high, _ = box_split(tile[(0,) + window_of(unit)[2]] - base, high_count)
        return (high >= 0.0) & (high < high_count)

    def add(i, carry):
        row0, col0, window = window_of(active[i])
        high, low = box_split(tile[(0,) + window] - base, high_count)
        z = 0.25 * tile[(1,) + window]
        z_high = rounded(z)
        z_low = z - z_high
        pot = tile[(2,) + window]
        flux = tile[(3,) + window]
        shift = col0.astype(F32) + off_j
        col_index = lax.broadcasted_iota(jnp.int32, (high_count, LANES), 1).astype(F32) + shift
        high_iota = lax.broadcasted_iota(jnp.int32, (high_count, LANES), 0).astype(F32)
        low_iota = lax.broadcasted_iota(jnp.int32, (WIDE, LANES), 0).astype(F32)
        lefts = []
        rights = []
        for s in range(8):

            def row(v):
                return v[s : s + 1, :]

            hit = high_iota == row(high)
            row_index = jnp.full((1, LANES), (row0 + s).astype(F32) + off_i, F32)
            values = [row_index, col_index, row(z_high), row(z_low), row(pot), row(flux)]
            lefts.append(
                jnp.concatenate([jnp.where(hit, v, 0.0).astype(BF16) for v in values], axis=0)
            )
            rights.append(jnp.where(low_iota == row(low), 1.0, 0.0).astype(BF16))
        acc[...] += lax.dot_general(
            jnp.concatenate(lefts, axis=1),
            jnp.concatenate(rights, axis=1),
            (((1,), (1,)), ((), ())),
            preferred_element_type=F32,
        )
        return carry

    lax.fori_loop(0, list_active(mine, rows // 8 * across, active), add, 0)

    if last:
        boxed = refs[-2]
        h = high_count
        row0 = (p * rows).astype(F32)
        col0 = ((q + 1) * cols).astype(F32)
        i = acc[0:h] + row0
        i = jnp.where(i >= node_rows, i - node_rows, i)
        j = acc[h : 2 * h] + col0
        j = jnp.where(j >= node_cols, j - node_cols, j)
        fields = [
            (i + 0.5) / node_rows,
            (j + 0.5) / node_cols,
            acc[2 * h : 3 * h] + acc[3 * h : 4 * h],
            acc[4 * h : 5 * h],
            acc[5 * h : 6 * h],
        ]
        for k, f in enumerate(fields):
            boxed[k, 0:h, :] = f[:, :LANES]
            boxed[k, h : 2 * h, :] = f[:, LANES:]


def scatter(steps, tile, acc, last, node_rows, node_cols, listed=None):
    _, rows, cols = tile.shape
    high_count = rows * cols // WIDE
    first = acc is None
    vmem = pl.BlockSpec(memory_space=pltpu.VMEM)
    out_shape = [pltpu.VMEM((PIECES * high_count, WIDE), F32)]
    if last:
        out_shape.append(pltpu.VMEM((5, 2 * high_count, LANES), F32))
    if first:
        near, boxes = listed.shape
        out_shape.append(jax.ShapeDtypeStruct(((near // 2 + near + 2 + 7) // 8 * 8, boxes), jnp.int32))
    args = (tile, listed) if first else (tile, pinned(acc))
    out = pl.pallas_call(
        lambda *refs: scatter_kernel(
            first, last, (rows, cols, high_count, node_rows, node_cols), steps, *refs
        ),
        out_shape=out_shape,
        in_specs=[vmem] * len(args),
        out_specs=[vmem] * len(out_shape),
        scratch_shapes=[pltpu.SMEM((rows * cols // (8 * LANES),), jnp.int32)],
        compiler_params=pltpu.CompilerParams(vmem_limit_bytes=VMEM_LIMIT),
        name="scatter_last" if last else "scatter_first" if first else "scatter",
        cost_estimate=pl.CostEstimate(
            flops=2 * PIECES * high_count * WIDE * rows * cols // 2,
            transcendentals=0,
            bytes_accessed=4 * (2 * PIECES * high_count * WIDE + 4 * rows * cols),
        ),
    )(*args)
    return out[1] if last else out if first else out[0]


def thirds(value):
    high = rounded(value)
    middle = rounded(value - high)
    return high, middle, value - high - middle


def plan_rows(listed, plan):
    near, boxes = listed.shape
    half = near // 2
    rank = lax.axis_index("tx") * lax.axis_size("ty") + lax.axis_index("ty")
    n = listed[...] - (rank - 1) * boxes
    taken = jnp.zeros((1, boxes), jnp.int32)
    left = jnp.zeros((1, boxes), jnp.int32)
    first = [jnp.full((1, boxes), boxes, jnp.int32) for _ in range(half)]
    rest = [jnp.full((1, boxes), 3 * boxes, jnp.int32) for _ in range(near)]
    for k in range(near):
        row = n[k : k + 1, :]
        take = (row >= boxes) & (row < 2 * boxes) & (taken < half)
        first = [jnp.where(take & (taken == j), row - boxes, v) for j, v in enumerate(first)]
        rest = [jnp.where(take | (left != j), v, row) for j, v in enumerate(rest)]
        step = jnp.where(take, 1, 0)
        taken = taken + step
        left = left + 1 - step
    for j, v in enumerate(first + rest):
        plan[j : j + 1, :] = v
    over = left > half
    flags = jnp.broadcast_to(jnp.where(over, 1.0, 0.0), (8, boxes)).astype(BF16)
    down = lax.broadcasted_iota(jnp.int32, (boxes, boxes), 0)
    across = lax.broadcasted_iota(jnp.int32, (boxes, boxes), 1)
    before = jnp.where(down < across, 1.0, 0.0).astype(BF16)
    offset = jnp.dot(flags, before, preferred_element_type=F32)[0:1, :]
    count = jnp.dot(flags, jnp.ones((boxes, boxes), BF16), preferred_element_type=F32)[0:1, :]
    hit = jnp.where((down.astype(F32) == offset) & over, 1.0, 0.0).astype(BF16)
    names = lax.broadcasted_iota(jnp.int32, (8, boxes), 1).astype(F32).astype(BF16)
    found = lax.dot_general(names, hit, (((1,), (1,)), ((), ())), preferred_element_type=F32)[0:1, :]
    count = count.astype(jnp.int32)
    plan[half + near : half + near + 1, :] = jnp.where(across[0:1, :] < count, found.astype(jnp.int32), boxes)
    plan[half + near + 1 : half + near + 2, :] = count


def pieces_of(ref, group):
    window = (pl.ds(pl.multiple_of(8 * group, 8), 8), slice(None))
    x, y, z, pot, flux = (ref[(f,) + window] for f in range(5))
    pieces = []
    total = None
    for v in (x, y, z):
        high = rounded(v)
        low = rounded(v - high)
        kept = high + low
        pieces.append((high, low))
        total = kept * kept if total is None else total + kept * kept
    return pieces, total, pot, flux


def padded_rows(values):
    return values + [jnp.zeros_like(values[0])] * (USED - len(values))


def moment_side(ref, n):
    pitch = ref.shape[0] // STORED
    rows = ref[pl.ds(USED * pitch + n, 8, stride=pitch), :]
    zeros = jnp.zeros((8, LANES), F32)
    return jnp.concatenate([zeros, rows] + [zeros] * (FEATURES // 8 - 2), axis=0).astype(BF16)


def strided(ref, n, stored):
    pitch = ref.shape[0] // stored
    rows = [ref[pl.ds(8 * g * pitch + n, 8, stride=pitch), :] for g in range(USED // 8)]
    return jnp.concatenate(rows + [jnp.zeros((8, LANES), F32)] * ((FEATURES - USED) // 8), axis=0)


def store_sources(refs, sfeat, sflux):
    pitch = sfeat.shape[0] // STORED
    ones = jnp.ones((8, LANES), F32)
    zeros = jnp.zeros((8, LANES), F32)
    boxes = refs[0].shape[1]
    for which, ref in enumerate(refs):

        def store(group, carry):
            pieces, total, pot, flux = pieces_of(ref, group)
            source = []
            for high, low in pieces:
                source += [-2.0 * high, -2.0 * low, -2.0 * high, -2.0 * low]
            z = pieces[2][0] + pieces[2][1]
            rows = padded_rows(source + list(thirds(total)) + [ones, ones, ones])
            rows += [pot, zeros, pot, zeros] + list(thirds(-pot * z)) + [zeros]
            start = pl.multiple_of(which * boxes + 8 * group, 8)
            for k, v in enumerate(rows):
                sfeat[pl.ds(pl.multiple_of(k * pitch + start, 8), 8), :] = v
            sflux[pl.ds(start, 8), :] = flux
            return carry

        lax.fori_loop(0, boxes // 8, store, 0, unroll=2)
    start = len(refs) * boxes
    for k in range(STORED):
        sfeat[k * pitch + start : k * pitch + start + 8, :] = ones if k == 12 else zeros
    sflux[start : start + 8, :] = zeros


def store_targets(own, tfeat, turned):
    boxes = own.shape[1]
    pitch = tfeat.shape[0] // USED
    ones = jnp.ones((8, LANES), F32)

    def store(group, carry):
        pieces, total, _, _ = pieces_of(own, group)
        target = []
        for high, low in pieces:
            target += [high, high, low, low]
        for k, v in enumerate(padded_rows(target + [ones, ones, ones] + list(thirds(total + 0.04)))):
            tfeat[pl.ds(pl.multiple_of(k * pitch + 8 * group, 8), 8), :] = v
        return carry

    lax.fori_loop(0, boxes // 8, store, 0, unroll=2)
    turned[boxes] = jnp.zeros((LANES, FEATURES), BF16)

    def turn(i, carry):
        for u in range(8):
            turned[8 * i + u] = strided(tfeat, 8 * i + u, USED).T.astype(BF16)
        return carry

    lax.fori_loop(0, boxes // 8, turn, 0)


def run_items(target_of, source_of, half, iterations, turned, sfeat, sflux, sums, totals):
    empty_row = sums.shape[0] - 8

    def apply(item, total):
        target = target_of(item)
        sides = [strided(sfeat, source_of(item, k), STORED).astype(BF16) for k in range(half)]
        sides += [moment_side(sfeat, source_of(item, k)) for k in range(half)]
        squared = jnp.dot(turned[target], jnp.concatenate(sides, axis=1), preferred_element_type=F32)
        fluxes = [
            jnp.broadcast_to(sflux[pl.ds(source_of(item, k), 1), :], (8, LANES)) for k in range(half)
        ]
        for t in range(LANES // 8):
            rows = slice(8 * t, 8 * t + 8)
            value = None
            for k, flux in enumerate(fluxes):
                inverse = lax.rsqrt(squared[rows, LANES * k : LANES * (k + 1)])
                moment = squared[rows, LANES * (half + k) : LANES * (half + k + 1)]
                part = inverse * (flux - (inverse * inverse) * moment)
                value = part if value is None else value + part
            total[rows, :] = value

    def reduce(item, total, live):
        target = jnp.where(live, target_of(jnp.maximum(item, 0)), empty_row)
        sums[pl.ds(target, 1), :] += jnp.sum(total[...].T, axis=0, keepdims=True)

    def step(i, carry):
        for u in range(GROUP):
            reduce(GROUP * (i - 1) + u, totals.at[u], i > 0)
        for u in range(GROUP):
            apply(GROUP * i + u, totals.at[u])
        return carry

    totals[...] = jnp.zeros(totals.shape, F32)
    lax.fori_loop(0, iterations, step, 0)
    for u in range(GROUP):
        reduce(GROUP * (iterations - 1) + u, totals.at[u], iterations > 0)


def near_own_kernel(near, plan, own, sums, turned, tfeat, sfeat, sflux, totals):
    boxes = own.shape[1]
    half = near // 2
    sums[...] = jnp.zeros(sums.shape, F32)
    store_targets(own, tfeat, turned)
    store_sources([own], sfeat, sflux)

    def target_of(item):
        return jnp.minimum(item, boxes - 1)

    def source_of(item, k):
        return plan[k, jnp.minimum(item, boxes - 1)]

    run_items(
        target_of, source_of, half, boxes // GROUP, turned, sfeat, sflux, sums, totals
    )


def near_other_kernel(
    near, plan, own, lower, upper, tile, sums_in, turned, out, sums, sfeat, sflux, totals
):
    boxes = lower.shape[1]
    half = near // 2
    sums[...] = sums_in[...]
    store_sources([lower, own, upper], sfeat, sflux)
    items = boxes + plan[half + near + 1, 0]

    def box_of(item):
        extra = plan[half + near, jnp.clip(item - boxes, 0, boxes - 1)]
        return jnp.where(item < boxes, item, extra)

    def target_of(item):
        return jnp.where(item < items, box_of(item), boxes)

    def source_of(item, k):
        row = jnp.where(item < boxes, half, 2 * half) + k
        return plan[row, jnp.minimum(box_of(item), boxes - 1)]

    iterations = (items + GROUP - 1) // GROUP
    run_items(
        target_of, source_of, half, iterations, turned, sfeat, sflux, sums, totals
    )
    out[0:boxes, :] = sums[0:boxes, :] * (1.0 / math.sqrt(near * LANES))

    _, rows, cols = tile.shape
    out[boxes : boxes + EXTRA, :] = jnp.zeros((EXTRA, LANES), F32)
    place = boxes
    for f in (1, 2):
        for r in (rows - 2, rows - 1):
            for c in range(cols // LANES):
                out[place : place + 1, :] = tile[f, r : r + 1, LANES * c : LANES * c + LANES]
                place += 1
    place = boxes + EXTRA - 8
    for f in (1, 2):
        turned_cols = tile[f, :, cols - LANES : cols].T
        out[place : place + 2, 0:rows] = turned_cols[LANES - 2 : LANES, :]
        place += 2


def item_scratch(sources):
    return [
        pltpu.VMEM((STORED * (sources + 8), LANES), F32),
        pltpu.VMEM((sources + 8, LANES), F32),
        pltpu.VMEM((GROUP, LANES, LANES), F32),
    ]


def near_cost(boxes, near):
    pairs = boxes * near * LANES * LANES // 2
    return pl.CostEstimate(
        flops=pairs * 2 * FEATURES * 4, transcendentals=pairs, bytes_accessed=4 * 16 * boxes * LANES
    )


def near_own(plan, own, near):
    boxes = own.shape[1]
    assert boxes == LANES and boxes % GROUP == 0 and near % 2 == 0
    vmem = pl.BlockSpec(memory_space=pltpu.VMEM)
    smem = pl.BlockSpec(memory_space=pltpu.SMEM)
    return pl.pallas_call(
        lambda *refs: near_own_kernel(near, *refs),
        out_shape=(
            pltpu.VMEM((boxes + 8, LANES), F32),
            pltpu.VMEM((boxes + 1, LANES, FEATURES), BF16),
        ),
        in_specs=[smem, vmem],
        out_specs=(vmem,) * 2,
        scratch_shapes=[pltpu.VMEM((USED * (boxes + 8), LANES), F32)] + item_scratch(boxes),
        compiler_params=pltpu.CompilerParams(vmem_limit_bytes=VMEM_LIMIT),
        name="near_own",
        cost_estimate=near_cost(boxes, near),
    )(plan, pinned(own))


def near_other(plan, own, lower, upper, tile, sums, turned, near):
    boxes = lower.shape[1]
    vmem = pl.BlockSpec(memory_space=pltpu.VMEM)
    smem = pl.BlockSpec(memory_space=pltpu.SMEM)
    return pl.pallas_call(
        lambda *refs: near_other_kernel(near, *refs),
        out_shape=pltpu.VMEM((boxes + EXTRA, LANES), F32),
        in_specs=[smem] + [vmem] * 6,
        out_specs=vmem,
        scratch_shapes=[pltpu.VMEM((boxes + 8, LANES), F32)] + item_scratch(3 * boxes),
        compiler_params=pltpu.CompilerParams(vmem_limit_bytes=VMEM_LIMIT),
        name="near_other",
        cost_estimate=near_cost(boxes, near),
    )(plan, *map(pinned, (own, lower, upper, tile, sums, turned)))


def lookup(slot, base, table, pieces, active, out):
    rows, cols = slot.shape
    high_count = rows * cols // WIDE
    across = cols // LANES
    whole = jnp.concatenate([table[0:high_count, :], table[high_count : 2 * high_count, :]], axis=1)
    top = rounded(whole)
    pieces[0:high_count, :] = top.astype(BF16)
    pieces[high_count : 2 * high_count, :] = (whole - top).astype(BF16)

    def window_of(unit):
        row, col = unit // across * 8, unit % across * LANES
        if not isinstance(unit, int):
            row, col = pl.multiple_of(row, 8), pl.multiple_of(col, LANES)
        return pl.ds(row, 8), pl.ds(col, LANES)

    def there(unit):
        high, _ = box_split(slot[window_of(unit)] - base, high_count)
        return (high >= 0.0) & (high < high_count)

    def add(i, carry):
        window = window_of(active[i])
        high, low = box_split(slot[window] - base, high_count)
        low_iota = lax.broadcasted_iota(jnp.int32, (WIDE, LANES), 0).astype(F32)
        high_iota = lax.broadcasted_iota(jnp.int32, (high_count, LANES), 0).astype(F32)
        hits = jnp.concatenate(
            [jnp.where(low_iota == low[s : s + 1, :], 1.0, 0.0).astype(BF16) for s in range(8)],
            axis=1,
        )
        picked = jnp.dot(pieces[...], hits, preferred_element_type=F32)
        lines = []
        for s in range(8):
            part = slice(LANES * s, LANES * s + LANES)
            both = picked[0:high_count, part] + picked[high_count : 2 * high_count, part]
            mine = high_iota == high[s : s + 1, :]
            lines.append(jnp.sum(jnp.where(mine, both, 0.0), axis=0, keepdims=True))
        out[window] += jnp.concatenate(lines, axis=0)
        return carry

    lax.fori_loop(0, list_active(there, rows // 8 * across, active), add, 0)


def base_of(node_count, steps):
    rank = ahead("tx", -steps[0]) * lax.axis_size("ty") + ahead("ty", -steps[1])
    return (rank * node_count).astype(F32)


def own_kernel(tile, table, out, pieces, active):
    out[...] = jnp.zeros(out.shape, F32)
    lookup(tile.at[0], base_of(out.shape[0] * out.shape[1], (0, 0)), table, pieces, active, out)


def row_kernel(tile, ahead_x, partial, behind_x, out, slopes, pieces, active, padded):
    _, rows, cols = tile.shape
    boxes = rows * cols // LANES
    out[...] = partial[...]
    lookup(tile.at[0], base_of(rows * cols, (1, 0)), behind_x, pieces, active, out)
    for f in (1, 2):
        padded[8 : 8 + rows, :] = tile[f]
        for r in range(2):
            for c in range(cols // LANES):
                source = boxes + ((f - 1) * 2 + r) * (cols // LANES) + c
                padded[6 + r : 7 + r, LANES * c : LANES * c + LANES] = behind_x[source : source + 1, :]
        padded[8 + rows : 10 + rows, :] = ahead_x[f, 0:2, :]
        slopes[f - 1] = (
            padded[6 : 6 + rows, :]
            - 8.0 * padded[7 : 7 + rows, :]
            + 8.0 * padded[9 : 9 + rows, :]
            - padded[10 : 10 + rows, :]
        ) / 12.0


def col_kernel(tile, ahead_y, partial, behind_y, out, slopes, pieces, active):
    _, rows, cols = tile.shape
    boxes = rows * cols // LANES
    out[...] = partial[...]
    lookup(tile.at[0], base_of(rows * cols, (0, 1)), behind_y, pieces, active, out)
    left_cols = behind_y[boxes + EXTRA - 8 : boxes + EXTRA, 0:rows].T
    col = lax.broadcasted_iota(jnp.int32, (rows, cols), 1)
    for f in (1, 2):
        here = tile[f]
        left = left_cols[:, 2 * (f - 1) : 2 * f]
        right = ahead_y[f, :, 0:2]
        less_1 = jnp.where(col == 0, left[:, 1:2], pltpu.roll(here, 1, 1))
        less_2 = jnp.where(
            col == 0, left[:, 0:1], jnp.where(col == 1, left[:, 1:2], pltpu.roll(here, 2, 1))
        )
        more_1 = jnp.where(col == cols - 1, right[:, 0:1], pltpu.roll(here, cols - 1, 1))
        more_2 = jnp.where(
            col == cols - 2,
            right[:, 0:1],
            jnp.where(col == cols - 1, right[:, 1:2], pltpu.roll(here, cols - 2, 1)),
        )
        slopes[f - 1] = (less_2 - 8.0 * less_1 + 8.0 * more_1 - more_2) / 12.0


def last_kernel(tile, row_slopes, col_slopes, partial, behind_xy, elev_rate, pot_rate, pieces, active, total):
    _, rows, cols = tile.shape
    total[...] = partial[...]
    lookup(tile.at[0], base_of(rows * cols, (1, 1)), behind_xy, pieces, active, total)
    elev_x, pot_x = row_slopes[0], row_slopes[1]
    elev_y, pot_y = col_slopes[0], col_slopes[1]
    vertical = total[...]
    lift = 1.0 + elev_x * elev_x + elev_y * elev_y
    elev_rate[...] = vertical * lift - (pot_x * elev_x + pot_y * elev_y)
    pot_rate[...] = (
        -tile[1] - 0.5 * (pot_x * pot_x + pot_y * pot_y) + 0.5 * vertical * vertical * lift
    )


def lookup_call(kernel, name, out_shape, args, scratch):
    _, rows, cols = args[0].shape
    vmem = pl.BlockSpec(memory_space=pltpu.VMEM)
    return pl.pallas_call(
        kernel,
        out_shape=out_shape,
        in_specs=[vmem] * len(args),
        out_specs=(vmem,) * len(out_shape),
        scratch_shapes=[
            pltpu.VMEM((2 * rows * cols // WIDE, WIDE), BF16),
            pltpu.SMEM((rows * cols // (8 * LANES),), jnp.int32),
        ]
        + scratch,
        compiler_params=pltpu.CompilerParams(vmem_limit_bytes=VMEM_LIMIT),
        name=name,
        cost_estimate=pl.CostEstimate(
            flops=rows * cols * rows * cols, transcendentals=0, bytes_accessed=4 * 8 * rows * cols
        ),
    )(*map(pinned, args))


def look_up_all(tile, ahead_x, ahead_y, value, behind_x, behind_y, behind_xy):
    _, rows, cols = tile.shape
    values = pltpu.VMEM((rows, cols), F32)
    slopes = pltpu.VMEM((2, rows, cols), F32)
    (partial,) = lookup_call(own_kernel, "lookup_own", (values,), (tile, value), [])
    partial, row_slopes = lookup_call(
        row_kernel,
        "lookup_x",
        (values, slopes),
        (tile, ahead_x, partial, behind_x),
        [pltpu.VMEM((rows + 16, cols), F32)],
    )
    partial, col_slopes = lookup_call(
        col_kernel, "lookup_y", (values, slopes), (tile, ahead_y, partial, behind_y), []
    )
    shape = jax.ShapeDtypeStruct((rows, cols), F32)
    return lookup_call(
        last_kernel,
        "lookup_xy",
        (shape, shape),
        (tile, row_slopes, col_slopes, partial, behind_xy),
        [pltpu.VMEM((rows, cols), F32)],
    )


def pack_kernel(owner, place, elevation, potential, flux, tile, owner_here, place_here, arrived):
    copies = [
        pltpu.make_async_copy(source, target, arrived.at[i])
        for i, (source, target) in enumerate(
            (
                (owner, owner_here),
                (place, place_here),
                (elevation, tile.at[1]),
                (potential, tile.at[2]),
                (flux, tile.at[3]),
            )
        )
    ]
    for copy in copies:
        copy.start()
    copies[0].wait()
    copies[1].wait()
    node_count = owner.shape[0] * owner.shape[1]
    tile[0] = (owner_here[...] * node_count + place_here[...]).astype(F32)
    for copy in copies[2:]:
        copy.wait()


def pack(owner, place, elevation, potential, flux):
    return pl.pallas_call(
        pack_kernel,
        out_shape=pltpu.VMEM((4,) + owner.shape, F32),
        in_specs=[pl.BlockSpec(memory_space=pltpu.HBM)] * 5,
        out_specs=pl.BlockSpec(memory_space=pltpu.VMEM),
        scratch_shapes=[pltpu.VMEM(owner.shape, jnp.int32)] * 2 + [pltpu.SemaphoreType.DMA((5,))],
        compiler_params=pltpu.CompilerParams(vmem_limit_bytes=VMEM_LIMIT),
        name="pack",
    )(owner, place, elevation, potential, flux)


def shards(potential, elevation, normal_flux, box_owner, box_place, near_boxes):
    rows, cols = potential.shape
    count_tx = lax.axis_size("tx")
    count_ty = lax.axis_size("ty")
    node_count = rows * cols
    boxes = node_count // LANES
    near = near_boxes.shape[1]
    assert node_count % WIDE == 0 and cols <= 256 and rows <= 128
    assert 4 * (cols // LANES) <= EXTRA - 8
    assert node_count * count_tx * count_ty < 2**24

    tile = pack(box_owner, box_place, elevation, potential, normal_flux)
    ahead_x = shifted(tile, "tx", -1)
    ahead_y = shifted(tile, "ty", -1)
    ahead_xy = shifted(ahead_y, "tx", -1)
    tile, ahead_x, ahead_y, ahead_xy = map(pinned, (tile, ahead_x, ahead_y, ahead_xy))

    sizes = (rows * count_tx, cols * count_ty)
    acc, plan = scatter((0, 0), tile, None, False, *sizes, near_boxes.T)
    acc = scatter((1, 0), ahead_x, acc, False, *sizes)
    acc = scatter((0, 1), ahead_y, acc, False, *sizes)
    boxed = scatter((1, 1), ahead_xy, acc, True, *sizes)

    total = count_tx * count_ty
    both = ("tx", "ty")
    lower = lax.ppermute(boxed, both, [(i, i + 1) for i in range(total - 1)])
    upper = lax.ppermute(boxed, both, [(i + 1, i) for i in range(total - 1)])

    sums, turned = near_own(plan, boxed, near)
    value = near_other(plan, boxed, lower, upper, tile, sums, turned, near)

    behind_x = shifted(value, "tx", 1)
    behind_y = shifted(value, "ty", 1)
    diagonal = [
        (i * count_ty + j, (i + 1) % count_tx * count_ty + (j + 1) % count_ty)
        for i in range(count_tx)
        for j in range(count_ty)
    ]
    behind_xy = lax.ppermute(value, both, diagonal)
    return look_up_all(tile, ahead_x, ahead_y, value, behind_x, behind_y, behind_xy)


def solution(mesh):
    in_specs = (
        P("tx", "ty"),
        P("tx", "ty"),
        P("tx", "ty"),
        P("tx", "ty"),
        P("tx", "ty"),
        P(("tx", "ty"), None),
    )
    out_specs = (P("tx", "ty"), P("tx", "ty"))
    return jax.shard_map(shards, mesh=mesh, in_specs=in_specs, out_specs=out_specs, check_vma=False)
```

```python
import math

import jax
import jax.numpy as jnp
from jax import lax
from jax.experimental import pallas as pl
from jax.experimental.pallas import tpu as pltpu
from jax.sharding import PartitionSpec as P

LANES = 128
WIDE = 256
PIECES = 6
FEATURES = 32
USED = 24
STORED = USED + 8
EXTRA = 16
GROUP = 8
VMEM_LIMIT = 24 << 20
BF16 = jnp.bfloat16
F32 = jnp.float32


def shifted(value, axis, steps):
    count = lax.axis_size(axis)
    pairs = [(source, (source + steps) % count) for source in range(count)]
    return lax.ppermute(value, axis, pairs)


def ahead(axis, steps):
    index = lax.axis_index(axis) + steps
    count = lax.axis_size(axis)
    return jnp.where(index < 0, index + count, jnp.where(index >= count, index - count, index))


def pinned(value):
    return pltpu.with_memory_space_constraint(value, pltpu.VMEM)


def rounded(value):
    return value.astype(BF16).astype(F32)


def box_split(rel, high_count):
    box = jnp.floor(rel * (1.0 / LANES))
    second = box >= high_count
    high = jnp.where(second, box - high_count, box)
    low = rel - box * LANES
    return high, jnp.where(second, low + LANES, low)


def list_active(test, count, active):
    flags = [jnp.max(jnp.where(test(unit), 1.0, 0.0)) > 0.0 for unit in range(count)]
    found = jnp.int32(0)
    for unit, flag in enumerate(flags):
        active[found] = unit
        found = found + jnp.where(flag, 1, 0)
    return found


def scatter_kernel(first, last, sizes, steps, tile, *refs):
    active = refs[-1]
    if first:
        listed, acc, plan = refs[:3]
        plan_rows(listed, plan)
    else:
        acc_in, acc = refs[:2]
    rows, cols, high_count, node_rows, node_cols = sizes
    p = lax.axis_index("tx")
    q = lax.axis_index("ty")
    base = ((p * lax.axis_size("ty") + q) * (rows * cols)).astype(F32)
    off_i = float(steps[0] * rows)
    off_j = float((steps[1] - 1) * cols)
    acc[...] = jnp.zeros(acc.shape, F32) if first else acc_in[...]
    across = cols // LANES

    def window_of(unit):
        row, col = unit // across * 8, unit % across * LANES
        if not isinstance(unit, int):
            row, col = pl.multiple_of(row, 8), pl.multiple_of(col, LANES)
        return row, col, (pl.ds(row, 8), pl.ds(col, LANES))

    def mine(unit):
        high, _ = box_split(tile[(0,) + window_of(unit)[2]] - base, high_count)
        return (high >= 0.0) & (high < high_count)

    def sides(i, live):
        row0, col0, window = window_of(active[jnp.where(live, i, 0)])
        high, low = box_split(tile[(0,) + window] - base, high_count)
        high = jnp.where(live, high, -1.0)
        z = 0.25 * tile[(1,) + window]
        z_high = rounded(z)
        z_low = z - z_high
        pot = tile[(2,) + window]
        flux = tile[(3,) + window]
        shift = col0.astype(F32) + off_j
        col_index = lax.broadcasted_iota(jnp.int32, (high_count, LANES), 1).astype(F32) + shift
        high_iota = lax.broadcasted_iota(jnp.int32, (high_count, LANES), 0).astype(F32)
        low_iota = lax.broadcasted_iota(jnp.int32, (WIDE, LANES), 0).astype(F32)
        lefts = []
        rights = []
        for s in range(8):

            def row(v):
                return v[s : s + 1, :]

            hit = high_iota == row(high)
            row_index = jnp.full((1, LANES), (row0 + s).astype(F32) + off_i, F32)
            values = [row_index, col_index, row(z_high), row(z_low), row(pot), row(flux)]
            lefts.append(
                jnp.concatenate([jnp.where(hit, v, 0.0).astype(BF16) for v in values], axis=0)
            )
            rights.append(jnp.where(low_iota == row(low), 1.0, 0.0).astype(BF16))
        return lefts, rights

    def add(i, carry):
        lefts, rights = sides(2 * i, True)
        more = sides(2 * i + 1, 2 * i + 1 < count)
        acc[...] += lax.dot_general(
            jnp.concatenate(lefts + more[0], axis=1),
            jnp.concatenate(rights + more[1], axis=1),
            (((1,), (1,)), ((), ())),
            preferred_element_type=F32,
        )
        return carry

    count = list_active(mine, rows // 8 * across, active)

    lax.fori_loop(0, (count + 1) // 2, add, 0)

    if last:
        boxed = refs[-2]
        h = high_count
        row0 = (p * rows).astype(F32)
        col0 = ((q + 1) * cols).astype(F32)
        i = acc[0:h] + row0
        i = jnp.where(i >= node_rows, i - node_rows, i)
        j = acc[h : 2 * h] + col0
        j = jnp.where(j >= node_cols, j - node_cols, j)
        fields = [
            (i + 0.5) / node_rows,
            (j + 0.5) / node_cols,
            acc[2 * h : 3 * h] + acc[3 * h : 4 * h],
            acc[4 * h : 5 * h],
            acc[5 * h : 6 * h],
        ]
        for k, f in enumerate(fields):
            boxed[k, 0:h, :] = f[:, :LANES]
            boxed[k, h : 2 * h, :] = f[:, LANES:]


def scatter(steps, tile, acc, last, node_rows, node_cols, listed=None):
    _, rows, cols = tile.shape
    high_count = rows * cols // WIDE
    first = acc is None
    vmem = pl.BlockSpec(memory_space=pltpu.VMEM)
    out_shape = [pltpu.VMEM((PIECES * high_count, WIDE), F32)]
    if last:
        out_shape.append(pltpu.VMEM((5, 2 * high_count, LANES), F32))
    if first:
        near, boxes = listed.shape
        out_shape.append(jax.ShapeDtypeStruct(((near // 2 + near + 2 + 7) // 8 * 8, boxes), jnp.int32))
    args = (tile, listed) if first else (tile, pinned(acc))
    out = pl.pallas_call(
        lambda *refs: scatter_kernel(
            first, last, (rows, cols, high_count, node_rows, node_cols), steps, *refs
        ),
        out_shape=out_shape,
        in_specs=[vmem] * len(args),
        out_specs=[vmem] * len(out_shape),
        scratch_shapes=[pltpu.SMEM((rows * cols // (8 * LANES),), jnp.int32)],
        compiler_params=pltpu.CompilerParams(vmem_limit_bytes=VMEM_LIMIT),
        name="scatter_last" if last else "scatter_first" if first else "scatter",
        cost_estimate=pl.CostEstimate(
            flops=2 * PIECES * high_count * WIDE * rows * cols // 2,
            transcendentals=0,
            bytes_accessed=4 * (2 * PIECES * high_count * WIDE + 4 * rows * cols),
        ),
    )(*args)
    return out[1] if last else out if first else out[0]


def thirds(value):
    high = rounded(value)
    middle = rounded(value - high)
    return high, middle, value - high - middle


def plan_rows(listed, plan):
    near, boxes = listed.shape
    half = near // 2
    rank = lax.axis_index("tx") * lax.axis_size("ty") + lax.axis_index("ty")
    n = listed[...] - (rank - 1) * boxes
    taken = jnp.zeros((1, boxes), jnp.int32)
    left = jnp.zeros((1, boxes), jnp.int32)
    first = [jnp.full((1, boxes), boxes, jnp.int32) for _ in range(half)]
    rest = [jnp.full((1, boxes), 3 * boxes, jnp.int32) for _ in range(near)]
    for k in range(near):
        row = n[k : k + 1, :]
        take = (row >= boxes) & (row < 2 * boxes) & (taken < half)
        first = [jnp.where(take & (taken == j), row - boxes, v) for j, v in enumerate(first)]
        rest = [jnp.where(take | (left != j), v, row) for j, v in enumerate(rest)]
        step = jnp.where(take, 1, 0)
        taken = taken + step
        left = left + 1 - step
    for j, v in enumerate(first + rest):
        plan[j : j + 1, :] = v
    over = left > half
    flags = jnp.broadcast_to(jnp.where(over, 1.0, 0.0), (8, boxes)).astype(BF16)
    down = lax.broadcasted_iota(jnp.int32, (boxes, boxes), 0)
    across = lax.broadcasted_iota(jnp.int32, (boxes, boxes), 1)
    before = jnp.where(down < across, 1.0, 0.0).astype(BF16)
    offset = jnp.dot(flags, before, preferred_element_type=F32)[0:1, :]
    count = jnp.dot(flags, jnp.ones((boxes, boxes), BF16), preferred_element_type=F32)[0:1, :]
    hit = jnp.where((down.astype(F32) == offset) & over, 1.0, 0.0).astype(BF16)
    names = lax.broadcasted_iota(jnp.int32, (8, boxes), 1).astype(F32).astype(BF16)
    found = lax.dot_general(names, hit, (((1,), (1,)), ((), ())), preferred_element_type=F32)[0:1, :]
    count = count.astype(jnp.int32)
    plan[half + near : half + near + 1, :] = jnp.where(across[0:1, :] < count, found.astype(jnp.int32), boxes)
    plan[half + near + 1 : half + near + 2, :] = count


def pieces_of(ref, group):
    window = (pl.ds(pl.multiple_of(8 * group, 8), 8), slice(None))
    x, y, z, pot, flux = (ref[(f,) + window] for f in range(5))
    pieces = []
    total = None
    for v in (x, y, z):
        high = rounded(v)
        low = rounded(v - high)
        kept = high + low
        pieces.append((high, low))
        total = kept * kept if total is None else total + kept * kept
    return pieces, total, pot, flux


def padded_rows(values):
    return values + [jnp.zeros_like(values[0])] * (USED - len(values))


def moment_side(ref, n):
    pitch = ref.shape[0] // STORED
    rows = ref[pl.ds(USED * pitch + n, 8, stride=pitch), :]
    zeros = jnp.zeros((8, LANES), F32)
    return jnp.concatenate([zeros, rows] + [zeros] * (FEATURES // 8 - 2), axis=0).astype(BF16)


def strided(ref, n, stored):
    pitch = ref.shape[0] // stored
    rows = [ref[pl.ds(8 * g * pitch + n, 8, stride=pitch), :] for g in range(USED // 8)]
    return jnp.concatenate(rows + [jnp.zeros((8, LANES), F32)] * ((FEATURES - USED) // 8), axis=0)


def store_sources(refs, sfeat, sflux):
    pitch = sfeat.shape[0] // STORED
    ones = jnp.ones((8, LANES), F32)
    zeros = jnp.zeros((8, LANES), F32)
    boxes = refs[0].shape[1]
    for which, ref in enumerate(refs):

        def store(group, carry):
            pieces, total, pot, flux = pieces_of(ref, group)
            source = []
            for high, low in pieces:
                source += [-2.0 * high, -2.0 * low, -2.0 * high, -2.0 * low]
            z = pieces[2][0] + pieces[2][1]
            rows = padded_rows(source + list(thirds(total)) + [ones, ones, ones])
            rows += [pot, zeros, pot, zeros] + list(thirds(-pot * z)) + [zeros]
            start = pl.multiple_of(which * boxes + 8 * group, 8)
            for k, v in enumerate(rows):
                sfeat[pl.ds(pl.multiple_of(k * pitch + start, 8), 8), :] = v
            sflux[pl.ds(start, 8), :] = flux
            return carry

        lax.fori_loop(0, boxes // 8, store, 0, unroll=2)
    start = len(refs) * boxes
    for k in range(STORED):
        sfeat[k * pitch + start : k * pitch + start + 8, :] = ones if k == 12 else zeros
    sflux[start : start + 8, :] = zeros


def store_targets(own, tfeat, turned):
    boxes = own.shape[1]
    pitch = tfeat.shape[0] // USED
    ones = jnp.ones((8, LANES), F32)

    def store(group, carry):
        pieces, total, _, _ = pieces_of(own, group)
        target = []
        for high, low in pieces:
            target += [high, high, low, low]
        for k, v in enumerate(padded_rows(target + [ones, ones, ones] + list(thirds(total + 0.04)))):
            tfeat[pl.ds(pl.multiple_of(k * pitch + 8 * group, 8), 8), :] = v
        return carry

    lax.fori_loop(0, boxes // 8, store, 0, unroll=2)
    turned[boxes] = jnp.zeros((LANES, FEATURES), BF16)

    def turn(i, carry):
        for u in range(8):
            turned[8 * i + u] = strided(tfeat, 8 * i + u, USED).T.astype(BF16)
        return carry

    lax.fori_loop(0, boxes // 8, turn, 0)


def run_items(target_of, source_of, half, iterations, turned, sfeat, sflux, sums, totals):
    empty_row = sums.shape[0] - 8

    def apply(item, total):
        target = target_of(item)
        sides = [strided(sfeat, source_of(item, k), STORED).astype(BF16) for k in range(half)]
        sides += [moment_side(sfeat, source_of(item, k)) for k in range(half)]
        squared = jnp.dot(turned[target], jnp.concatenate(sides, axis=1), preferred_element_type=F32)
        fluxes = [
            jnp.broadcast_to(sflux[pl.ds(source_of(item, k), 1), :], (8, LANES)) for k in range(half)
        ]
        for t in range(LANES // 8):
            rows = slice(8 * t, 8 * t + 8)
            value = None
            for k, flux in enumerate(fluxes):
                inverse = lax.rsqrt(squared[rows, LANES * k : LANES * (k + 1)])
                moment = squared[rows, LANES * (half + k) : LANES * (half + k + 1)]
                part = inverse * (flux - (inverse * inverse) * moment)
                value = part if value is None else value + part
            total[rows, :] = value

    def reduce(item, total, live):
        target = jnp.where(live, target_of(jnp.maximum(item, 0)), empty_row)
        sums[pl.ds(target, 1), :] += jnp.sum(total[...].T, axis=0, keepdims=True)

    def step(i, carry):
        for u in range(GROUP):
            reduce(GROUP * (i - 1) + u, totals.at[u], i > 0)
        for u in range(GROUP):
            apply(GROUP * i + u, totals.at[u])
        return carry

    totals[...] = jnp.zeros(totals.shape, F32)
    lax.fori_loop(0, iterations, step, 0)
    for u in range(GROUP):
        reduce(GROUP * (iterations - 1) + u, totals.at[u], iterations > 0)


def near_own_kernel(near, plan, own, sums, turned, tfeat, sfeat, sflux, totals):
    boxes = own.shape[1]
    half = near // 2
    sums[...] = jnp.zeros(sums.shape, F32)
    store_targets(own, tfeat, turned)
    store_sources([own], sfeat, sflux)

    def target_of(item):
        return jnp.minimum(item, boxes - 1)

    def source_of(item, k):
        return plan[k, jnp.minimum(item, boxes - 1)]

    run_items(
        target_of, source_of, half, boxes // GROUP, turned, sfeat, sflux, sums, totals
    )


def near_other_kernel(
    near, plan, own, lower, upper, tile, sums_in, turned, out, sums, sfeat, sflux, totals
):
    boxes = lower.shape[1]
    half = near // 2
    sums[...] = sums_in[...]
    store_sources([lower, own, upper], sfeat, sflux)
    items = boxes + plan[half + near + 1, 0]

    def box_of(item):
        extra = plan[half + near, jnp.clip(item - boxes, 0, boxes - 1)]
        return jnp.where(item < boxes, item, extra)

    def target_of(item):
        return jnp.where(item < items, box_of(item), boxes)

    def source_of(item, k):
        row = jnp.where(item < boxes, half, 2 * half) + k
        return plan[row, jnp.minimum(box_of(item), boxes - 1)]

    iterations = (items + GROUP - 1) // GROUP
    run_items(
        target_of, source_of, half, iterations, turned, sfeat, sflux, sums, totals
    )
    out[0:boxes, :] = sums[0:boxes, :] * (1.0 / math.sqrt(near * LANES))

    _, rows, cols = tile.shape
    out[boxes : boxes + EXTRA, :] = jnp.zeros((EXTRA, LANES), F32)
    place = boxes
    for f in (1, 2):
        for r in (rows - 2, rows - 1):
            for c in range(cols // LANES):
                out[place : place + 1, :] = tile[f, r : r + 1, LANES * c : LANES * c + LANES]
                place += 1
    place = boxes + EXTRA - 8
    for f in (1, 2):
        turned_cols = tile[f, :, cols - LANES : cols].T
        out[place : place + 2, 0:rows] = turned_cols[LANES - 2 : LANES, :]
        place += 2


def item_scratch(sources):
    return [
        pltpu.VMEM((STORED * (sources + 8), LANES), F32),
        pltpu.VMEM((sources + 8, LANES), F32),
        pltpu.VMEM((GROUP, LANES, LANES), F32),
    ]


def near_cost(boxes, near):
    pairs = boxes * near * LANES * LANES // 2
    return pl.CostEstimate(
        flops=pairs * 2 * FEATURES * 4, transcendentals=pairs, bytes_accessed=4 * 16 * boxes * LANES
    )


def near_own(plan, own, near):
    boxes = own.shape[1]
    assert boxes == LANES and boxes % GROUP == 0 and near % 2 == 0
    vmem = pl.BlockSpec(memory_space=pltpu.VMEM)
    smem = pl.BlockSpec(memory_space=pltpu.SMEM)
    return pl.pallas_call(
        lambda *refs: near_own_kernel(near, *refs),
        out_shape=(
            pltpu.VMEM((boxes + 8, LANES), F32),
            pltpu.VMEM((boxes + 1, LANES, FEATURES), BF16),
        ),
        in_specs=[smem, vmem],
        out_specs=(vmem,) * 2,
        scratch_shapes=[pltpu.VMEM((USED * (boxes + 8), LANES), F32)] + item_scratch(boxes),
        compiler_params=pltpu.CompilerParams(vmem_limit_bytes=VMEM_LIMIT),
        name="near_own",
        cost_estimate=near_cost(boxes, near),
    )(plan, pinned(own))


def near_other(plan, own, lower, upper, tile, sums, turned, near):
    boxes = lower.shape[1]
    vmem = pl.BlockSpec(memory_space=pltpu.VMEM)
    smem = pl.BlockSpec(memory_space=pltpu.SMEM)
    return pl.pallas_call(
        lambda *refs: near_other_kernel(near, *refs),
        out_shape=pltpu.VMEM((boxes + EXTRA, LANES), F32),
        in_specs=[smem] + [vmem] * 6,
        out_specs=vmem,
        scratch_shapes=[pltpu.VMEM((boxes + 8, LANES), F32)] + item_scratch(3 * boxes),
        compiler_params=pltpu.CompilerParams(vmem_limit_bytes=VMEM_LIMIT),
        name="near_other",
        cost_estimate=near_cost(boxes, near),
    )(plan, *map(pinned, (own, lower, upper, tile, sums, turned)))


def lookup(slot, base, table, pieces, active, out):
    rows, cols = slot.shape
    high_count = rows * cols // WIDE
    across = cols // LANES
    whole = jnp.concatenate([table[0:high_count, :], table[high_count : 2 * high_count, :]], axis=1)
    top = rounded(whole)
    pieces[0:high_count, :] = top.astype(BF16)
    pieces[high_count : 2 * high_count, :] = (whole - top).astype(BF16)

    def window_of(unit):
        row, col = unit // across * 8, unit % across * LANES
        if not isinstance(unit, int):
            row, col = pl.multiple_of(row, 8), pl.multiple_of(col, LANES)
        return pl.ds(row, 8), pl.ds(col, LANES)

    def there(unit):
        high, _ = box_split(slot[window_of(unit)] - base, high_count)
        return (high >= 0.0) & (high < high_count)

    def nodes_of(i, live):
        window = window_of(active[jnp.where(live, i, 0)])
        high, low = box_split(slot[window] - base, high_count)
        return window, jnp.where(live, high, -1.0), low

    def add(i, carry):
        low_iota = lax.broadcasted_iota(jnp.int32, (WIDE, LANES), 0).astype(F32)
        high_iota = lax.broadcasted_iota(jnp.int32, (high_count, LANES), 0).astype(F32)
        both = (nodes_of(2 * i, True), nodes_of(2 * i + 1, 2 * i + 1 < count))
        hits = [
            jnp.where(low_iota == low[s : s + 1, :], 1.0, 0.0).astype(BF16)
            for _, _, low in both
            for s in range(8)
        ]
        picked = jnp.dot(pieces[...], jnp.concatenate(hits, axis=1), preferred_element_type=F32)
        for half, (window, high, _) in enumerate(both):
            lines = []
            for s in range(8):
                start = LANES * (8 * half + s)
                part = slice(start, start + LANES)
                value = picked[0:high_count, part] + picked[high_count : 2 * high_count, part]
                mine = high_iota == high[s : s + 1, :]
                lines.append(jnp.sum(jnp.where(mine, value, 0.0), axis=0, keepdims=True))
            out[window] += jnp.concatenate(lines, axis=0)
        return carry

    count = list_active(there, rows // 8 * across, active)
    lax.fori_loop(0, (count + 1) // 2, add, 0)


def base_of(node_count, steps):
    rank = ahead("tx", -steps[0]) * lax.axis_size("ty") + ahead("ty", -steps[1])
    return (rank * node_count).astype(F32)


def own_kernel(tile, table, out, pieces, active):
    out[...] = jnp.zeros(out.shape, F32)
    lookup(tile.at[0], base_of(out.shape[0] * out.shape[1], (0, 0)), table, pieces, active, out)


def row_kernel(tile, ahead_x, partial, behind_x, out, slopes, pieces, active, padded):
    _, rows, cols = tile.shape
    boxes = rows * cols // LANES
    out[...] = partial[...]
    lookup(tile.at[0], base_of(rows * cols, (1, 0)), behind_x, pieces, active, out)
    for f in (1, 2):
        padded[8 : 8 + rows, :] = tile[f]
        for r in range(2):
            for c in range(cols // LANES):
                source = boxes + ((f - 1) * 2 + r) * (cols // LANES) + c
                padded[6 + r : 7 + r, LANES * c : LANES * c + LANES] = behind_x[source : source + 1, :]
        padded[8 + rows : 10 + rows, :] = ahead_x[f, 0:2, :]
        slopes[f - 1] = (
            padded[6 : 6 + rows, :]
            - 8.0 * padded[7 : 7 + rows, :]
            + 8.0 * padded[9 : 9 + rows, :]
            - padded[10 : 10 + rows, :]
        ) / 12.0


def col_kernel(tile, ahead_y, partial, behind_y, out, slopes, pieces, active):
    _, rows, cols = tile.shape
    boxes = rows * cols // LANES
    out[...] = partial[...]
    lookup(tile.at[0], base_of(rows * cols, (0, 1)), behind_y, pieces, active, out)
    left_cols = behind_y[boxes + EXTRA - 8 : boxes + EXTRA, 0:rows].T
    col = lax.broadcasted_iota(jnp.int32, (rows, cols), 1)
    for f in (1, 2):
        here = tile[f]
        left = left_cols[:, 2 * (f - 1) : 2 * f]
        right = ahead_y[f, :, 0:2]
        less_1 = jnp.where(col == 0, left[:, 1:2], pltpu.roll(here, 1, 1))
        less_2 = jnp.where(
            col == 0, left[:, 0:1], jnp.where(col == 1, left[:, 1:2], pltpu.roll(here, 2, 1))
        )
        more_1 = jnp.where(col == cols - 1, right[:, 0:1], pltpu.roll(here, cols - 1, 1))
        more_2 = jnp.where(
            col == cols - 2,
            right[:, 0:1],
            jnp.where(col == cols - 1, right[:, 1:2], pltpu.roll(here, cols - 2, 1)),
        )
        slopes[f - 1] = (less_2 - 8.0 * less_1 + 8.0 * more_1 - more_2) / 12.0


def last_kernel(tile, row_slopes, col_slopes, partial, behind_xy, elev_rate, pot_rate, pieces, active, total):
    _, rows, cols = tile.shape
    total[...] = partial[...]
    lookup(tile.at[0], base_of(rows * cols, (1, 1)), behind_xy, pieces, active, total)
    elev_x, pot_x = row_slopes[0], row_slopes[1]
    elev_y, pot_y = col_slopes[0], col_slopes[1]
    vertical = total[...]
    lift = 1.0 + elev_x * elev_x + elev_y * elev_y
    elev_rate[...] = vertical * lift - (pot_x * elev_x + pot_y * elev_y)
    pot_rate[...] = (
        -tile[1] - 0.5 * (pot_x * pot_x + pot_y * pot_y) + 0.5 * vertical * vertical * lift
    )


def lookup_call(kernel, name, out_shape, args, scratch):
    _, rows, cols = args[0].shape
    vmem = pl.BlockSpec(memory_space=pltpu.VMEM)
    return pl.pallas_call(
        kernel,
        out_shape=out_shape,
        in_specs=[vmem] * len(args),
        out_specs=(vmem,) * len(out_shape),
        scratch_shapes=[
            pltpu.VMEM((2 * rows * cols // WIDE, WIDE), BF16),
            pltpu.SMEM((rows * cols // (8 * LANES),), jnp.int32),
        ]
        + scratch,
        compiler_params=pltpu.CompilerParams(vmem_limit_bytes=VMEM_LIMIT),
        name=name,
        cost_estimate=pl.CostEstimate(
            flops=rows * cols * rows * cols, transcendentals=0, bytes_accessed=4 * 8 * rows * cols
        ),
    )(*map(pinned, args))


def look_up_all(tile, ahead_x, ahead_y, value, behind_x, behind_y, behind_xy):
    _, rows, cols = tile.shape
    values = pltpu.VMEM((rows, cols), F32)
    slopes = pltpu.VMEM((2, rows, cols), F32)
    (partial,) = lookup_call(own_kernel, "lookup_own", (values,), (tile, value), [])
    partial, row_slopes = lookup_call(
        row_kernel,
        "lookup_x",
        (values, slopes),
        (tile, ahead_x, partial, behind_x),
        [pltpu.VMEM((rows + 16, cols), F32)],
    )
    partial, col_slopes = lookup_call(
        col_kernel, "lookup_y", (values, slopes), (tile, ahead_y, partial, behind_y), []
    )
    shape = jax.ShapeDtypeStruct((rows, cols), F32)
    return lookup_call(
        last_kernel,
        "lookup_xy",
        (shape, shape),
        (tile, row_slopes, col_slopes, partial, behind_xy),
        [pltpu.VMEM((rows, cols), F32)],
    )


def shards(potential, elevation, normal_flux, box_owner, box_place, near_boxes):
    rows, cols = potential.shape
    count_tx = lax.axis_size("tx")
    count_ty = lax.axis_size("ty")
    node_count = rows * cols
    boxes = node_count // LANES
    near = near_boxes.shape[1]
    assert node_count % WIDE == 0 and cols <= 256 and rows <= 128
    assert 4 * (cols // LANES) <= EXTRA - 8
    assert node_count * count_tx * count_ty < 2**24

    slot = (box_owner * node_count + box_place).astype(F32)
    tile = jnp.stack([slot, elevation, potential, normal_flux])
    ahead_x = shifted(tile, "tx", -1)
    ahead_y = shifted(tile, "ty", -1)
    ahead_xy = shifted(ahead_y, "tx", -1)
    tile, ahead_x, ahead_y, ahead_xy = map(pinned, (tile, ahead_x, ahead_y, ahead_xy))

    sizes = (rows * count_tx, cols * count_ty)
    acc, plan = scatter((0, 0), tile, None, False, *sizes, near_boxes.T)
    acc = scatter((1, 0), ahead_x, acc, False, *sizes)
    acc = scatter((0, 1), ahead_y, acc, False, *sizes)
    boxed = scatter((1, 1), ahead_xy, acc, True, *sizes)

    total = count_tx * count_ty
    both = ("tx", "ty")
    lower = lax.ppermute(boxed, both, [(i, i + 1) for i in range(total - 1)])
    upper = lax.ppermute(boxed, both, [(i + 1, i) for i in range(total - 1)])

    sums, turned = near_own(plan, boxed, near)
    value = near_other(plan, boxed, lower, upper, tile, sums, turned, near)

    behind_x = shifted(value, "tx", 1)
    behind_y = shifted(value, "ty", 1)
    diagonal = [
        (i * count_ty + j, (i + 1) % count_tx * count_ty + (j + 1) % count_ty)
        for i in range(count_tx)
        for j in range(count_ty)
    ]
    behind_xy = lax.ppermute(value, both, diagonal)
    return look_up_all(tile, ahead_x, ahead_y, value, behind_x, behind_y, behind_xy)


def solution(mesh):
    in_specs = (
        P("tx", "ty"),
        P("tx", "ty"),
        P("tx", "ty"),
        P("tx", "ty"),
        P("tx", "ty"),
        P(("tx", "ty"), None),
    )
    out_specs = (P("tx", "ty"), P("tx", "ty"))
    return jax.shard_map(shards, mesh=mesh, in_specs=in_specs, out_specs=out_specs, check_vma=False)
```

```python
import math

import jax
import jax.numpy as jnp
from jax import lax
from jax.experimental import pallas as pl
from jax.experimental.pallas import tpu as pltpu
from jax.sharding import PartitionSpec as P

LANES = 128
WIDE = 256
PIECES = 6
FEATURES = 32
USED = 24
STORED = USED + 8
EXTRA = 16
UNITS = 5
OWN_GROUP = 16
OTHER_GROUP = 16
VMEM_LIMIT = 24 << 20
BF16 = jnp.bfloat16
F32 = jnp.float32


def shifted(value, axis, steps):
    count = lax.axis_size(axis)
    pairs = [(source, (source + steps) % count) for source in range(count)]
    return lax.ppermute(value, axis, pairs)


def ahead(axis, steps):
    index = lax.axis_index(axis) + steps
    count = lax.axis_size(axis)
    return jnp.where(index < 0, index + count, jnp.where(index >= count, index - count, index))


def pinned(value):
    return pltpu.with_memory_space_constraint(value, pltpu.VMEM)


def rounded(value):
    return value.astype(BF16).astype(F32)


def box_split(rel, high_count):
    box = jnp.floor(rel * (1.0 / LANES))
    second = box >= high_count
    high = jnp.where(second, box - high_count, box)
    low = rel - box * LANES
    return high, jnp.where(second, low + LANES, low)


def list_active(test, count, active):
    flags = [jnp.max(jnp.where(test(unit), 1.0, 0.0)) > 0.0 for unit in range(count)]
    found = jnp.int32(0)
    for unit, flag in enumerate(flags):
        active[found] = unit
        found = found + jnp.where(flag, 1, 0)
    return found


def scatter_kernel(first, last, sizes, steps, tile, *refs):
    active = refs[-1]
    if first:
        listed, acc, plan = refs[:3]
        plan_rows(listed, plan)
    else:
        acc_in, acc = refs[:2]
    rows, cols, high_count, node_rows, node_cols = sizes
    p = lax.axis_index("tx")
    q = lax.axis_index("ty")
    base = ((p * lax.axis_size("ty") + q) * (rows * cols)).astype(F32)
    off_i = float(steps[0] * rows)
    off_j = float((steps[1] - 1) * cols)
    acc[...] = jnp.zeros(acc.shape, F32) if first else acc_in[...]
    across = cols // LANES

    def window_of(unit):
        row, col = unit // across * 8, unit % across * LANES
        if not isinstance(unit, int):
            row, col = pl.multiple_of(row, 8), pl.multiple_of(col, LANES)
        return row, col, (pl.ds(row, 8), pl.ds(col, LANES))

    def mine(unit):
        high, _ = box_split(tile[(0,) + window_of(unit)[2]] - base, high_count)
        return (high >= 0.0) & (high < high_count)

    def sides(i, live):
        row0, col0, window = window_of(active[jnp.where(live, i, 0)])
        high, low = box_split(tile[(0,) + window] - base, high_count)
        high = jnp.where(live, high, -1.0)
        z = 0.25 * tile[(1,) + window]
        z_high = rounded(z)
        z_low = z - z_high
        pot = tile[(2,) + window]
        flux = tile[(3,) + window]
        shift = col0.astype(F32) + off_j
        col_index = lax.broadcasted_iota(jnp.int32, (high_count, LANES), 1).astype(F32) + shift
        high_iota = lax.broadcasted_iota(jnp.int32, (high_count, LANES), 0).astype(F32)
        low_iota = lax.broadcasted_iota(jnp.int32, (WIDE, LANES), 0).astype(F32)
        lefts = []
        rights = []
        for s in range(8):

            def row(v):
                return v[s : s + 1, :]

            hit = high_iota == row(high)
            row_index = jnp.full((1, LANES), (row0 + s).astype(F32) + off_i, F32)
            values = [row_index, col_index, row(z_high), row(z_low), row(pot), row(flux)]
            lefts.append(
                jnp.concatenate([jnp.where(hit, v, 0.0).astype(BF16) for v in values], axis=0)
            )
            rights.append(jnp.where(low_iota == row(low), 1.0, 0.0).astype(BF16))
        return lefts, rights

    def add(i, carry):
        lefts, rights = [], []
        for u in range(UNITS):
            left, right = sides(UNITS * i + u, UNITS * i + u < count)
            lefts += left
            rights += right
        acc[...] += lax.dot_general(
            jnp.concatenate(lefts, axis=1),
            jnp.concatenate(rights, axis=1),
            (((1,), (1,)), ((), ())),
            preferred_element_type=F32,
        )
        return carry

    count = list_active(mine, rows // 8 * across, active)
    lax.fori_loop(0, (count + UNITS - 1) // UNITS, add, 0)

    if last:
        boxed = refs[-2]
        h = high_count
        row0 = (p * rows).astype(F32)
        col0 = ((q + 1) * cols).astype(F32)
        i = acc[0:h] + row0
        i = jnp.where(i >= node_rows, i - node_rows, i)
        j = acc[h : 2 * h] + col0
        j = jnp.where(j >= node_cols, j - node_cols, j)
        fields = [
            (i + 0.5) / node_rows,
            (j + 0.5) / node_cols,
            acc[2 * h : 3 * h] + acc[3 * h : 4 * h],
            acc[4 * h : 5 * h],
            acc[5 * h : 6 * h],
        ]
        for k, f in enumerate(fields):
            boxed[k, 0:h, :] = f[:, :LANES]
            boxed[k, h : 2 * h, :] = f[:, LANES:]


def scatter(steps, tile, acc, last, node_rows, node_cols, listed=None):
    _, rows, cols = tile.shape
    high_count = rows * cols // WIDE
    first = acc is None
    vmem = pl.BlockSpec(memory_space=pltpu.VMEM)
    out_shape = [pltpu.VMEM((PIECES * high_count, WIDE), F32)]
    if last:
        out_shape.append(pltpu.VMEM((5, 2 * high_count, LANES), F32))
    if first:
        near, boxes = listed.shape
        out_shape.append(jax.ShapeDtypeStruct(((near // 2 + near + 2 + 7) // 8 * 8, boxes), jnp.int32))
    args = (tile, listed) if first else (tile, pinned(acc))
    out = pl.pallas_call(
        lambda *refs: scatter_kernel(
            first, last, (rows, cols, high_count, node_rows, node_cols), steps, *refs
        ),
        out_shape=out_shape,
        in_specs=[vmem] * len(args),
        out_specs=[vmem] * len(out_shape),
        scratch_shapes=[pltpu.SMEM((rows * cols // (8 * LANES),), jnp.int32)],
        compiler_params=pltpu.CompilerParams(vmem_limit_bytes=VMEM_LIMIT),
        name="scatter_last" if last else "scatter_first" if first else "scatter",
        cost_estimate=pl.CostEstimate(
            flops=2 * PIECES * high_count * WIDE * rows * cols // 2,
            transcendentals=0,
            bytes_accessed=4 * (2 * PIECES * high_count * WIDE + 4 * rows * cols),
        ),
    )(*args)
    return out[1] if last else out if first else out[0]


def thirds(value):
    high = rounded(value)
    middle = rounded(value - high)
    return high, middle, value - high - middle


def plan_rows(listed, plan):
    near, boxes = listed.shape
    half = near // 2
    rank = lax.axis_index("tx") * lax.axis_size("ty") + lax.axis_index("ty")
    n = listed[...] - (rank - 1) * boxes
    taken = jnp.zeros((1, boxes), jnp.int32)
    left = jnp.zeros((1, boxes), jnp.int32)
    first = [jnp.full((1, boxes), boxes, jnp.int32) for _ in range(half)]
    rest = [jnp.full((1, boxes), 3 * boxes, jnp.int32) for _ in range(near)]
    for k in range(near):
        row = n[k : k + 1, :]
        take = (row >= boxes) & (row < 2 * boxes) & (taken < half)
        first = [jnp.where(take & (taken == j), row - boxes, v) for j, v in enumerate(first)]
        rest = [jnp.where(take | (left != j), v, row) for j, v in enumerate(rest)]
        step = jnp.where(take, 1, 0)
        taken = taken + step
        left = left + 1 - step
    for j, v in enumerate(first + rest):
        plan[j : j + 1, :] = v
    over = left > half
    flags = jnp.broadcast_to(jnp.where(over, 1.0, 0.0), (8, boxes)).astype(BF16)
    down = lax.broadcasted_iota(jnp.int32, (boxes, boxes), 0)
    across = lax.broadcasted_iota(jnp.int32, (boxes, boxes), 1)
    before = jnp.where(down < across, 1.0, 0.0).astype(BF16)
    offset = jnp.dot(flags, before, preferred_element_type=F32)[0:1, :]
    count = jnp.dot(flags, jnp.ones((boxes, boxes), BF16), preferred_element_type=F32)[0:1, :]
    hit = jnp.where((down.astype(F32) == offset) & over, 1.0, 0.0).astype(BF16)
    names = lax.broadcasted_iota(jnp.int32, (8, boxes), 1).astype(F32).astype(BF16)
    found = lax.dot_general(names, hit, (((1,), (1,)), ((), ())), preferred_element_type=F32)[0:1, :]
    count = count.astype(jnp.int32)
    plan[half + near : half + near + 1, :] = jnp.where(across[0:1, :] < count, found.astype(jnp.int32), boxes)
    plan[half + near + 1 : half + near + 2, :] = count


def pieces_of(ref, group):
    window = (pl.ds(pl.multiple_of(8 * group, 8), 8), slice(None))
    x, y, z, pot, flux = (ref[(f,) + window] for f in range(5))
    pieces = []
    total = None
    for v in (x, y, z):
        high = rounded(v)
        low = rounded(v - high)
        kept = high + low
        pieces.append((high, low))
        total = kept * kept if total is None else total + kept * kept
    return pieces, total, pot, flux


def padded_rows(values):
    return values + [jnp.zeros_like(values[0])] * (USED - len(values))


def moment_side(ref, n):
    pitch = ref.shape[0] // STORED
    rows = ref[pl.ds(USED * pitch + n, 8, stride=pitch), :]
    zeros = jnp.zeros((8, LANES), F32)
    return jnp.concatenate([zeros, rows] + [zeros] * (FEATURES // 8 - 2), axis=0).astype(BF16)


def strided(ref, n, stored):
    pitch = ref.shape[0] // stored
    rows = [ref[pl.ds(8 * g * pitch + n, 8, stride=pitch), :] for g in range(USED // 8)]
    return jnp.concatenate(rows + [jnp.zeros((8, LANES), F32)] * ((FEATURES - USED) // 8), axis=0)


def store_sources(refs, sfeat, sflux):
    pitch = sfeat.shape[0] // STORED
    ones = jnp.ones((8, LANES), F32)
    zeros = jnp.zeros((8, LANES), F32)
    boxes = refs[0].shape[1]
    for which, ref in enumerate(refs):

        def store(group, carry):
            pieces, total, pot, flux = pieces_of(ref, group)
            source = []
            for high, low in pieces:
                source += [-2.0 * high, -2.0 * low, -2.0 * high, -2.0 * low]
            z = pieces[2][0] + pieces[2][1]
            rows = padded_rows(source + list(thirds(total)) + [ones, ones, ones])
            rows += [pot, zeros, pot, zeros] + list(thirds(-pot * z)) + [zeros]
            start = pl.multiple_of(which * boxes + 8 * group, 8)
            for k, v in enumerate(rows):
                sfeat[pl.ds(pl.multiple_of(k * pitch + start, 8), 8), :] = v
            sflux[pl.ds(start, 8), :] = flux
            return carry

        lax.fori_loop(0, boxes // 8, store, 0, unroll=2)
    start = len(refs) * boxes
    for k in range(STORED):
        sfeat[k * pitch + start : k * pitch + start + 8, :] = ones if k == 12 else zeros
    sflux[start : start + 8, :] = zeros


def store_targets(own, tfeat, turned):
    boxes = own.shape[1]
    pitch = tfeat.shape[0] // USED
    ones = jnp.ones((8, LANES), F32)

    def store(group, carry):
        pieces, total, _, _ = pieces_of(own, group)
        target = []
        for high, low in pieces:
            target += [high, high, low, low]
        for k, v in enumerate(padded_rows(target + [ones, ones, ones] + list(thirds(total + 0.04)))):
            tfeat[pl.ds(pl.multiple_of(k * pitch + 8 * group, 8), 8), :] = v
        return carry

    lax.fori_loop(0, boxes // 8, store, 0, unroll=2)
    turned[boxes] = jnp.zeros((LANES, FEATURES), BF16)

    def turn(i, carry):
        for u in range(8):
            turned[8 * i + u] = strided(tfeat, 8 * i + u, USED).T.astype(BF16)
        return carry

    lax.fori_loop(0, boxes // 8, turn, 0)


def run_items(target_of, source_of, half, iterations, turned, sfeat, sflux, sums, totals):
    empty_row = sums.shape[0] - 8
    group = totals.shape[0]

    def apply(item, total):
        target = target_of(item)
        sides = [strided(sfeat, source_of(item, k), STORED).astype(BF16) for k in range(half)]
        sides += [moment_side(sfeat, source_of(item, k)) for k in range(half)]
        squared = jnp.dot(turned[target], jnp.concatenate(sides, axis=1), preferred_element_type=F32)
        fluxes = [
            jnp.broadcast_to(sflux[pl.ds(source_of(item, k), 1), :], (8, LANES)) for k in range(half)
        ]
        for t in range(LANES // 8):
            rows = slice(8 * t, 8 * t + 8)
            value = None
            for k, flux in enumerate(fluxes):
                inverse = lax.rsqrt(squared[rows, LANES * k : LANES * (k + 1)])
                moment = squared[rows, LANES * (half + k) : LANES * (half + k + 1)]
                part = inverse * (flux - (inverse * inverse) * moment)
                value = part if value is None else value + part
            total[rows, :] = value

    def reduce(item, total, live):
        target = jnp.where(live, target_of(jnp.maximum(item, 0)), empty_row)
        sums[pl.ds(target, 1), :] += jnp.sum(total[...].T, axis=0, keepdims=True)

    def step(i, carry):
        for u in range(group):
            reduce(group * (i - 1) + u, totals.at[u], i > 0)
        for u in range(group):
            apply(group * i + u, totals.at[u])
        return carry

    totals[...] = jnp.zeros(totals.shape, F32)
    lax.fori_loop(0, iterations, step, 0)
    for u in range(group):
        reduce(group * (iterations - 1) + u, totals.at[u], iterations > 0)


def near_own_kernel(near, plan, own, sums, turned, tfeat, sfeat, sflux, totals):
    boxes = own.shape[1]
    half = near // 2
    sums[...] = jnp.zeros(sums.shape, F32)
    store_targets(own, tfeat, turned)
    store_sources([own], sfeat, sflux)

    def target_of(item):
        return jnp.minimum(item, boxes - 1)

    def source_of(item, k):
        return plan[k, jnp.minimum(item, boxes - 1)]

    run_items(
        target_of, source_of, half, boxes // OWN_GROUP, turned, sfeat, sflux, sums, totals
    )


def near_other_kernel(
    near, plan, own, lower, upper, tile, sums_in, turned, out, sums, sfeat, sflux, totals
):
    boxes = lower.shape[1]
    half = near // 2
    sums[...] = sums_in[...]
    store_sources([lower, own, upper], sfeat, sflux)
    items = boxes + plan[half + near + 1, 0]

    def box_of(item):
        extra = plan[half + near, jnp.clip(item - boxes, 0, boxes - 1)]
        return jnp.where(item < boxes, item, extra)

    def target_of(item):
        return jnp.where(item < items, box_of(item), boxes)

    def source_of(item, k):
        row = jnp.where(item < boxes, half, 2 * half) + k
        return plan[row, jnp.minimum(box_of(item), boxes - 1)]

    iterations = (items + OTHER_GROUP - 1) // OTHER_GROUP
    run_items(
        target_of, source_of, half, iterations, turned, sfeat, sflux, sums, totals
    )
    out[0:boxes, :] = sums[0:boxes, :] * (1.0 / math.sqrt(near * LANES))

    _, rows, cols = tile.shape
    out[boxes : boxes + EXTRA, :] = jnp.zeros((EXTRA, LANES), F32)
    place = boxes
    for f in (1, 2):
        for r in (rows - 2, rows - 1):
            for c in range(cols // LANES):
                out[place : place + 1, :] = tile[f, r : r + 1, LANES * c : LANES * c + LANES]
                place += 1
    place = boxes + EXTRA - 8
    for f in (1, 2):
        turned_cols = tile[f, :, cols - LANES : cols].T
        out[place : place + 2, 0:rows] = turned_cols[LANES - 2 : LANES, :]
        place += 2


def item_scratch(sources, group):
    return [
        pltpu.VMEM((STORED * (sources + 8), LANES), F32),
        pltpu.VMEM((sources + 8, LANES), F32),
        pltpu.VMEM((group, LANES, LANES), F32),
    ]


def near_cost(boxes, near):
    pairs = boxes * near * LANES * LANES // 2
    return pl.CostEstimate(
        flops=pairs * 2 * FEATURES * 4, transcendentals=pairs, bytes_accessed=4 * 16 * boxes * LANES
    )


def near_own(plan, own, near):
    boxes = own.shape[1]
    assert boxes == LANES and boxes % OWN_GROUP == 0 and near % 2 == 0
    vmem = pl.BlockSpec(memory_space=pltpu.VMEM)
    smem = pl.BlockSpec(memory_space=pltpu.SMEM)
    return pl.pallas_call(
        lambda *refs: near_own_kernel(near, *refs),
        out_shape=(
            pltpu.VMEM((boxes + 8, LANES), F32),
            pltpu.VMEM((boxes + 1, LANES, FEATURES), BF16),
        ),
        in_specs=[smem, vmem],
        out_specs=(vmem,) * 2,
        scratch_shapes=[pltpu.VMEM((USED * (boxes + 8), LANES), F32)] + item_scratch(boxes, OWN_GROUP),
        compiler_params=pltpu.CompilerParams(vmem_limit_bytes=VMEM_LIMIT),
        name="near_own",
        cost_estimate=near_cost(boxes, near),
    )(plan, pinned(own))


def near_other(plan, own, lower, upper, tile, sums, turned, near):
    boxes = lower.shape[1]
    vmem = pl.BlockSpec(memory_space=pltpu.VMEM)
    smem = pl.BlockSpec(memory_space=pltpu.SMEM)
    return pl.pallas_call(
        lambda *refs: near_other_kernel(near, *refs),
        out_shape=pltpu.VMEM((boxes + EXTRA, LANES), F32),
        in_specs=[smem] + [vmem] * 6,
        out_specs=vmem,
        scratch_shapes=[pltpu.VMEM((boxes + 8, LANES), F32)] + item_scratch(3 * boxes, OTHER_GROUP),
        compiler_params=pltpu.CompilerParams(vmem_limit_bytes=VMEM_LIMIT),
        name="near_other",
        cost_estimate=near_cost(boxes, near),
    )(plan, *map(pinned, (own, lower, upper, tile, sums, turned)))


def lookup(slot, base, table, pieces, active, out):
    rows, cols = slot.shape
    high_count = rows * cols // WIDE
    across = cols // LANES
    whole = jnp.concatenate([table[0:high_count, :], table[high_count : 2 * high_count, :]], axis=1)
    top = rounded(whole)
    pieces[0:high_count, :] = top.astype(BF16)
    pieces[high_count : 2 * high_count, :] = (whole - top).astype(BF16)

    def window_of(unit):
        row, col = unit // across * 8, unit % across * LANES
        if not isinstance(unit, int):
            row, col = pl.multiple_of(row, 8), pl.multiple_of(col, LANES)
        return pl.ds(row, 8), pl.ds(col, LANES)

    def there(unit):
        high, _ = box_split(slot[window_of(unit)] - base, high_count)
        return (high >= 0.0) & (high < high_count)

    def nodes_of(i, live):
        window = window_of(active[jnp.where(live, i, 0)])
        high, low = box_split(slot[window] - base, high_count)
        return window, jnp.where(live, high, -1.0), low

    def add(i, carry):
        low_iota = lax.broadcasted_iota(jnp.int32, (WIDE, LANES), 0).astype(F32)
        high_iota = lax.broadcasted_iota(jnp.int32, (high_count, LANES), 0).astype(F32)
        units = [nodes_of(UNITS * i + u, UNITS * i + u < count) for u in range(UNITS)]
        hits = [
            jnp.where(low_iota == low[s : s + 1, :], 1.0, 0.0).astype(BF16)
            for _, _, low in units
            for s in range(8)
        ]
        picked = jnp.dot(pieces[...], jnp.concatenate(hits, axis=1), preferred_element_type=F32)
        for u, (window, high, _) in enumerate(units):
            lines = []
            for s in range(8):
                start = LANES * (8 * u + s)
                part = slice(start, start + LANES)
                value = picked[0:high_count, part] + picked[high_count : 2 * high_count, part]
                mine = high_iota == high[s : s + 1, :]
                lines.append(jnp.sum(jnp.where(mine, value, 0.0), axis=0, keepdims=True))
            out[window] += jnp.concatenate(lines, axis=0)
        return carry

    count = list_active(there, rows // 8 * across, active)
    lax.fori_loop(0, (count + UNITS - 1) // UNITS, add, 0)


def base_of(node_count, steps):
    rank = ahead("tx", -steps[0]) * lax.axis_size("ty") + ahead("ty", -steps[1])
    return (rank * node_count).astype(F32)


def own_kernel(tile, table, out, pieces, active):
    out[...] = jnp.zeros(out.shape, F32)
    lookup(tile.at[0], base_of(out.shape[0] * out.shape[1], (0, 0)), table, pieces, active, out)


def row_kernel(tile, ahead_x, partial, behind_x, out, slopes, pieces, active, padded):
    _, rows, cols = tile.shape
    boxes = rows * cols // LANES
    out[...] = partial[...]
    lookup(tile.at[0], base_of(rows * cols, (1, 0)), behind_x, pieces, active, out)
    for f in (1, 2):
        padded[8 : 8 + rows, :] = tile[f]
        for r in range(2):
            for c in range(cols // LANES):
                source = boxes + ((f - 1) * 2 + r) * (cols // LANES) + c
                padded[6 + r : 7 + r, LANES * c : LANES * c + LANES] = behind_x[source : source + 1, :]
        padded[8 + rows : 10 + rows, :] = ahead_x[f, 0:2, :]
        slopes[f - 1] = (
            padded[6 : 6 + rows, :]
            - 8.0 * padded[7 : 7 + rows, :]
            + 8.0 * padded[9 : 9 + rows, :]
            - padded[10 : 10 + rows, :]
        ) / 12.0


def col_kernel(tile, ahead_y, partial, behind_y, out, slopes, pieces, active):
    _, rows, cols = tile.shape
    boxes = rows * cols // LANES
    out[...] = partial[...]
    lookup(tile.at[0], base_of(rows * cols, (0, 1)), behind_y, pieces, active, out)
    left_cols = behind_y[boxes + EXTRA - 8 : boxes + EXTRA, 0:rows].T
    col = lax.broadcasted_iota(jnp.int32, (rows, cols), 1)
    for f in (1, 2):
        here = tile[f]
        left = left_cols[:, 2 * (f - 1) : 2 * f]
        right = ahead_y[f, :, 0:2]
        less_1 = jnp.where(col == 0, left[:, 1:2], pltpu.roll(here, 1, 1))
        less_2 = jnp.where(
            col == 0, left[:, 0:1], jnp.where(col == 1, left[:, 1:2], pltpu.roll(here, 2, 1))
        )
        more_1 = jnp.where(col == cols - 1, right[:, 0:1], pltpu.roll(here, cols - 1, 1))
        more_2 = jnp.where(
            col == cols - 2,
            right[:, 0:1],
            jnp.where(col == cols - 1, right[:, 1:2], pltpu.roll(here, cols - 2, 1)),
        )
        slopes[f - 1] = (less_2 - 8.0 * less_1 + 8.0 * more_1 - more_2) / 12.0


def last_kernel(tile, row_slopes, col_slopes, partial, behind_xy, elev_rate, pot_rate, pieces, active, total):
    _, rows, cols = tile.shape
    total[...] = partial[...]
    lookup(tile.at[0], base_of(rows * cols, (1, 1)), behind_xy, pieces, active, total)
    elev_x, pot_x = row_slopes[0], row_slopes[1]
    elev_y, pot_y = col_slopes[0], col_slopes[1]
    vertical = total[...]
    lift = 1.0 + elev_x * elev_x + elev_y * elev_y
    elev_rate[...] = vertical * lift - (pot_x * elev_x + pot_y * elev_y)
    pot_rate[...] = (
        -tile[1] - 0.5 * (pot_x * pot_x + pot_y * pot_y) + 0.5 * vertical * vertical * lift
    )


def lookup_call(kernel, name, out_shape, args, scratch):
    _, rows, cols = args[0].shape
    vmem = pl.BlockSpec(memory_space=pltpu.VMEM)
    return pl.pallas_call(
        kernel,
        out_shape=out_shape,
        in_specs=[vmem] * len(args),
        out_specs=(vmem,) * len(out_shape),
        scratch_shapes=[
            pltpu.VMEM((2 * rows * cols // WIDE, WIDE), BF16),
            pltpu.SMEM((rows * cols // (8 * LANES),), jnp.int32),
        ]
        + scratch,
        compiler_params=pltpu.CompilerParams(vmem_limit_bytes=VMEM_LIMIT),
        name=name,
        cost_estimate=pl.CostEstimate(
            flops=rows * cols * rows * cols, transcendentals=0, bytes_accessed=4 * 8 * rows * cols
        ),
    )(*map(pinned, args))


def look_up_all(tile, ahead_x, ahead_y, value, behind_x, behind_y, behind_xy):
    _, rows, cols = tile.shape
    values = pltpu.VMEM((rows, cols), F32)
    slopes = pltpu.VMEM((2, rows, cols), F32)
    (partial,) = lookup_call(own_kernel, "lookup_own", (values,), (tile, value), [])
    partial, row_slopes = lookup_call(
        row_kernel,
        "lookup_x",
        (values, slopes),
        (tile, ahead_x, partial, behind_x),
        [pltpu.VMEM((rows + 16, cols), F32)],
    )
    partial, col_slopes = lookup_call(
        col_kernel, "lookup_y", (values, slopes), (tile, ahead_y, partial, behind_y), []
    )
    shape = jax.ShapeDtypeStruct((rows, cols), F32)
    return lookup_call(
        last_kernel,
        "lookup_xy",
        (shape, shape),
        (tile, row_slopes, col_slopes, partial, behind_xy),
        [pltpu.VMEM((rows, cols), F32)],
    )


def shards(potential, elevation, normal_flux, box_owner, box_place, near_boxes):
    rows, cols = potential.shape
    count_tx = lax.axis_size("tx")
    count_ty = lax.axis_size("ty")
    node_count = rows * cols
    boxes = node_count // LANES
    near = near_boxes.shape[1]
    assert node_count % WIDE == 0 and cols <= 256 and rows <= 128
    assert 4 * (cols // LANES) <= EXTRA - 8
    assert node_count * count_tx * count_ty < 2**24

    slot = (box_owner * node_count + box_place).astype(F32)
    tile = jnp.stack([slot, elevation, potential, normal_flux])
    ahead_x = shifted(tile, "tx", -1)
    ahead_y = shifted(tile, "ty", -1)
    ahead_xy = shifted(ahead_y, "tx", -1)
    tile, ahead_x, ahead_y, ahead_xy = map(pinned, (tile, ahead_x, ahead_y, ahead_xy))

    sizes = (rows * count_tx, cols * count_ty)
    acc, plan = scatter((0, 0), tile, None, False, *sizes, near_boxes.T)
    acc = scatter((1, 0), ahead_x, acc, False, *sizes)
    acc = scatter((0, 1), ahead_y, acc, False, *sizes)
    boxed = scatter((1, 1), ahead_xy, acc, True, *sizes)

    total = count_tx * count_ty
    both = ("tx", "ty")
    lower = lax.ppermute(boxed, both, [(i, i + 1) for i in range(total - 1)])
    upper = lax.ppermute(boxed, both, [(i + 1, i) for i in range(total - 1)])

    sums, turned = near_own(plan, boxed, near)
    value = near_other(plan, boxed, lower, upper, tile, sums, turned, near)

    behind_x = shifted(value, "tx", 1)
    behind_y = shifted(value, "ty", 1)
    diagonal = [
        (i * count_ty + j, (i + 1) % count_tx * count_ty + (j + 1) % count_ty)
        for i in range(count_tx)
        for j in range(count_ty)
    ]
    behind_xy = lax.ppermute(value, both, diagonal)
    return look_up_all(tile, ahead_x, ahead_y, value, behind_x, behind_y, behind_xy)


def solution(mesh):
    in_specs = (
        P("tx", "ty"),
        P("tx", "ty"),
        P("tx", "ty"),
        P("tx", "ty"),
        P("tx", "ty"),
        P(("tx", "ty"), None),
    )
    out_specs = (P("tx", "ty"), P("tx", "ty"))
    return jax.shard_map(shards, mesh=mesh, in_specs=in_specs, out_specs=out_specs, check_vma=False)
```

```python
import math

import jax
import jax.numpy as jnp
from jax import lax
from jax.experimental import pallas as pl
from jax.experimental.pallas import tpu as pltpu
from jax.sharding import PartitionSpec as P

LANES = 128
WIDE = 256
PIECES = 6
FEATURES = 32
USED = 24
STORED = USED + 8
EXTRA = 16
UNITS = 5
OWN_GROUP = 16
OTHER_GROUP = 16
VMEM_LIMIT = 24 << 20
BF16 = jnp.bfloat16
F32 = jnp.float32


def shifted(value, axis, steps):
    count = lax.axis_size(axis)
    pairs = [(source, (source + steps) % count) for source in range(count)]
    return lax.ppermute(value, axis, pairs)


def ahead(axis, steps):
    index = lax.axis_index(axis) + steps
    count = lax.axis_size(axis)
    return jnp.where(index < 0, index + count, jnp.where(index >= count, index - count, index))


def pinned(value):
    return pltpu.with_memory_space_constraint(value, pltpu.VMEM)


def rounded(value):
    return value.astype(BF16).astype(F32)


def box_split(rel, high_count):
    box = jnp.floor(rel * (1.0 / LANES))
    second = box >= high_count
    high = jnp.where(second, box - high_count, box)
    low = rel - box * LANES
    return high, jnp.where(second, low + LANES, low)


def list_active(test, count, active):
    flags = [jnp.max(jnp.where(test(unit), 1.0, 0.0)) > 0.0 for unit in range(count)]
    found = jnp.int32(0)
    for unit, flag in enumerate(flags):
        active[found] = unit
        found = found + jnp.where(flag, 1, 0)
    return found


def scatter_kernel(first, last, sizes, steps, tile, *refs):
    active = refs[-1]
    if first:
        listed, acc, plan = refs[:3]
        plan_rows(listed, plan)
    else:
        acc_in, acc = refs[:2]
    rows, cols, high_count, node_rows, node_cols = sizes
    p = lax.axis_index("tx")
    q = lax.axis_index("ty")
    base = ((p * lax.axis_size("ty") + q) * (rows * cols)).astype(F32)
    off_i = float(steps[0] * rows)
    off_j = float((steps[1] - 1) * cols)
    acc[...] = jnp.zeros(acc.shape, F32) if first else acc_in[...]
    across = cols // LANES

    def window_of(unit):
        row, col = unit // across * 8, unit % across * LANES
        if not isinstance(unit, int):
            row, col = pl.multiple_of(row, 8), pl.multiple_of(col, LANES)
        return row, col, (pl.ds(row, 8), pl.ds(col, LANES))

    def mine(unit):
        high, _ = box_split(tile[(0,) + window_of(unit)[2]] - base, high_count)
        return (high >= 0.0) & (high < high_count)

    def sides(i, live):
        row0, col0, window = window_of(active[jnp.where(live, i, 0)])
        high, low = box_split(tile[(0,) + window] - base, high_count)
        high = jnp.where(live, high, -1.0)
        z = 0.25 * tile[(1,) + window]
        z_high = rounded(z)
        z_low = z - z_high
        pot = tile[(2,) + window]
        flux = tile[(3,) + window]
        shift = col0.astype(F32) + off_j
        col_index = lax.broadcasted_iota(jnp.int32, (high_count, LANES), 1).astype(F32) + shift
        high_iota = lax.broadcasted_iota(jnp.int32, (high_count, LANES), 0).astype(F32)
        low_iota = lax.broadcasted_iota(jnp.int32, (WIDE, LANES), 0).astype(F32)
        lefts = []
        rights = []
        for s in range(8):

            def row(v):
                return v[s : s + 1, :]

            hit = high_iota == row(high)
            row_index = jnp.full((1, LANES), (row0 + s).astype(F32) + off_i, F32)
            values = [row_index, col_index, row(z_high), row(z_low), row(pot), row(flux)]
            lefts.append(
                jnp.concatenate([jnp.where(hit, v, 0.0).astype(BF16) for v in values], axis=0)
            )
            rights.append(jnp.where(low_iota == row(low), 1.0, 0.0).astype(BF16))
        return lefts, rights

    def add(i, carry):
        lefts, rights = [], []
        for u in range(UNITS):
            left, right = sides(UNITS * i + u, UNITS * i + u < count)
            lefts += left
            rights += right
        acc[...] += lax.dot_general(
            jnp.concatenate(lefts, axis=1),
            jnp.concatenate(rights, axis=1),
            (((1,), (1,)), ((), ())),
            preferred_element_type=F32,
        )
        return carry

    count = list_active(mine, rows // 8 * across, active)
    lax.fori_loop(0, (count + UNITS - 1) // UNITS, add, 0)

    if last:
        boxed = refs[-2]
        h = high_count
        row0 = (p * rows).astype(F32)
        col0 = ((q + 1) * cols).astype(F32)
        i = acc[0:h] + row0
        i = jnp.where(i >= node_rows, i - node_rows, i)
        j = acc[h : 2 * h] + col0
        j = jnp.where(j >= node_cols, j - node_cols, j)
        fields = [
            (i + 0.5) / node_rows,
            (j + 0.5) / node_cols,
            acc[2 * h : 3 * h] + acc[3 * h : 4 * h],
            acc[4 * h : 5 * h],
            acc[5 * h : 6 * h],
        ]
        for k, f in enumerate(fields):
            boxed[k, 0:h, :] = f[:, :LANES]
            boxed[k, h : 2 * h, :] = f[:, LANES:]


def scatter(steps, tile, acc, last, node_rows, node_cols, listed=None):
    _, rows, cols = tile.shape
    high_count = rows * cols // WIDE
    first = acc is None
    vmem = pl.BlockSpec(memory_space=pltpu.VMEM)
    out_shape = [pltpu.VMEM((PIECES * high_count, WIDE), F32)]
    if last:
        out_shape.append(pltpu.VMEM((5, 2 * high_count, LANES), F32))
    if first:
        near, boxes = listed.shape
        out_shape.append(jax.ShapeDtypeStruct(((2 * near + 7) // 8 * 8, boxes), jnp.int32))
    args = (tile, listed) if first else (tile, pinned(acc))
    out = pl.pallas_call(
        lambda *refs: scatter_kernel(
            first, last, (rows, cols, high_count, node_rows, node_cols), steps, *refs
        ),
        out_shape=out_shape,
        in_specs=[vmem] * len(args),
        out_specs=[vmem] * len(out_shape),
        scratch_shapes=[pltpu.SMEM((rows * cols // (8 * LANES),), jnp.int32)],
        compiler_params=pltpu.CompilerParams(vmem_limit_bytes=VMEM_LIMIT),
        name="scatter_last" if last else "scatter_first" if first else "scatter",
        cost_estimate=pl.CostEstimate(
            flops=2 * PIECES * high_count * WIDE * rows * cols // 2,
            transcendentals=0,
            bytes_accessed=4 * (2 * PIECES * high_count * WIDE + 4 * rows * cols),
        ),
    )(*args)
    return out[1] if last else out if first else out[0]


def thirds(value):
    high = rounded(value)
    middle = rounded(value - high)
    return high, middle, value - high - middle


def plan_rows(listed, plan):
    near, boxes = listed.shape
    half = near // 2
    rank = lax.axis_index("tx") * lax.axis_size("ty") + lax.axis_index("ty")
    n = listed[...] - (rank - 1) * boxes
    taken = jnp.zeros((1, boxes), jnp.int32)
    left = jnp.zeros((1, boxes), jnp.int32)
    first = [jnp.full((1, boxes), boxes, jnp.int32) for _ in range(half)]
    rest = [jnp.full((1, boxes), 3 * boxes, jnp.int32) for _ in range(near)]
    for k in range(near):
        row = n[k : k + 1, :]
        take = (row >= boxes) & (row < 2 * boxes) & (taken < half)
        first = [jnp.where(take & (taken == j), row - boxes, v) for j, v in enumerate(first)]
        rest = [jnp.where(take | (left != j), v, row) for j, v in enumerate(rest)]
        step = jnp.where(take, 1, 0)
        taken = taken + step
        left = left + 1 - step
    for j, v in enumerate(first + rest):
        plan[j : j + 1, :] = v
    down = lax.broadcasted_iota(jnp.int32, (boxes, boxes), 0)
    across = lax.broadcasted_iota(jnp.int32, (boxes, boxes), 1)
    before = jnp.where(down < across, 1.0, 0.0).astype(BF16)
    names = lax.broadcasted_iota(jnp.int32, (8, boxes), 1).astype(F32).astype(BF16)
    for pair in range(half // 2):
        over = left > half + 2 * pair
        flags = jnp.broadcast_to(jnp.where(over, 1.0, 0.0), (8, boxes)).astype(BF16)
        offset = jnp.dot(flags, before, preferred_element_type=F32)[0:1, :]
        count = jnp.dot(flags, jnp.ones((boxes, boxes), BF16), preferred_element_type=F32)[0:1, :]
        hit = jnp.where((down.astype(F32) == offset) & over, 1.0, 0.0).astype(BF16)
        found = lax.dot_general(
            names, hit, (((1,), (1,)), ((), ())), preferred_element_type=F32
        )[0:1, :].astype(jnp.int32)
        count = count.astype(jnp.int32)
        place = half + near + 2 * pair
        plan[place : place + 1, :] = jnp.where(across[0:1, :] < count, found, boxes)
        plan[place + 1 : place + 2, :] = count


def pieces_of(ref, group):
    window = (pl.ds(pl.multiple_of(8 * group, 8), 8), slice(None))
    x, y, z, pot, flux = (ref[(f,) + window] for f in range(5))
    pieces = []
    total = None
    for v in (x, y, z):
        high = rounded(v)
        low = rounded(v - high)
        kept = high + low
        pieces.append((high, low))
        total = kept * kept if total is None else total + kept * kept
    return pieces, total, pot, flux


def padded_rows(values):
    return values + [jnp.zeros_like(values[0])] * (USED - len(values))


def moment_side(ref, n):
    pitch = ref.shape[0] // STORED
    rows = ref[pl.ds(USED * pitch + n, 8, stride=pitch), :]
    zeros = jnp.zeros((8, LANES), F32)
    return jnp.concatenate([zeros, rows] + [zeros] * (FEATURES // 8 - 2), axis=0).astype(BF16)


def strided(ref, n, stored):
    pitch = ref.shape[0] // stored
    rows = [ref[pl.ds(8 * g * pitch + n, 8, stride=pitch), :] for g in range(USED // 8)]
    return jnp.concatenate(rows + [jnp.zeros((8, LANES), F32)] * ((FEATURES - USED) // 8), axis=0)


def store_sources(refs, sfeat, sflux):
    pitch = sfeat.shape[0] // STORED
    ones = jnp.ones((8, LANES), F32)
    zeros = jnp.zeros((8, LANES), F32)
    boxes = refs[0].shape[1]
    for which, ref in enumerate(refs):

        def store(group, carry):
            pieces, total, pot, flux = pieces_of(ref, group)
            source = []
            for high, low in pieces:
                source += [-2.0 * high, -2.0 * low, -2.0 * high, -2.0 * low]
            z = pieces[2][0] + pieces[2][1]
            rows = padded_rows(source + list(thirds(total)) + [ones, ones, ones])
            rows += [pot, zeros, pot, zeros] + list(thirds(-pot * z)) + [zeros]
            start = pl.multiple_of(which * boxes + 8 * group, 8)
            for k, v in enumerate(rows):
                sfeat[pl.ds(pl.multiple_of(k * pitch + start, 8), 8), :] = v
            sflux[pl.ds(start, 8), :] = flux
            return carry

        lax.fori_loop(0, boxes // 8, store, 0, unroll=2)
    start = len(refs) * boxes
    for k in range(STORED):
        sfeat[k * pitch + start : k * pitch + start + 8, :] = ones if k == 12 else zeros
    sflux[start : start + 8, :] = zeros


def store_targets(own, tfeat, turned):
    boxes = own.shape[1]
    pitch = tfeat.shape[0] // USED
    ones = jnp.ones((8, LANES), F32)

    def store(group, carry):
        pieces, total, _, _ = pieces_of(own, group)
        target = []
        for high, low in pieces:
            target += [high, high, low, low]
        for k, v in enumerate(padded_rows(target + [ones, ones, ones] + list(thirds(total + 0.04)))):
            tfeat[pl.ds(pl.multiple_of(k * pitch + 8 * group, 8), 8), :] = v
        return carry

    lax.fori_loop(0, boxes // 8, store, 0, unroll=2)
    turned[boxes] = jnp.zeros((LANES, FEATURES), BF16)

    def turn(i, carry):
        for u in range(16):
            turned[16 * i + u] = strided(tfeat, 16 * i + u, USED).T.astype(BF16)
        return carry

    lax.fori_loop(0, boxes // 16, turn, 0)


def run_items(target_of, source_of, half, iterations, turned, sfeat, sflux, sums, totals):
    empty_row = sums.shape[0] - 8
    group = totals.shape[0]

    def apply(item, total):
        target = target_of(item)
        sides = [strided(sfeat, source_of(item, k), STORED).astype(BF16) for k in range(half)]
        sides += [moment_side(sfeat, source_of(item, k)) for k in range(half)]
        squared = jnp.dot(turned[target], jnp.concatenate(sides, axis=1), preferred_element_type=F32)
        fluxes = [
            jnp.broadcast_to(sflux[pl.ds(source_of(item, k), 1), :], (8, LANES)) for k in range(half)
        ]
        for t in range(LANES // 8):
            rows = slice(8 * t, 8 * t + 8)
            value = None
            for k, flux in enumerate(fluxes):
                inverse = lax.rsqrt(squared[rows, LANES * k : LANES * (k + 1)])
                moment = squared[rows, LANES * (half + k) : LANES * (half + k + 1)]
                part = inverse * (flux - (inverse * inverse) * moment)
                value = part if value is None else value + part
            total[rows, :] = value

    def reduce(item, total, live):
        target = jnp.where(live, target_of(jnp.maximum(item, 0)), empty_row)
        sums[pl.ds(target, 1), :] += jnp.sum(total[...].T, axis=0, keepdims=True)

    def step(i, carry):
        for u in range(group):
            reduce(group * (i - 1) + u, totals.at[u], i > 0)
        for u in range(group):
            apply(group * i + u, totals.at[u])
        return carry

    totals[...] = jnp.zeros(totals.shape, F32)
    lax.fori_loop(0, iterations, step, 0)
    for u in range(group):
        reduce(group * (iterations - 1) + u, totals.at[u], iterations > 0)


def near_own_kernel(near, plan, own, sums, turned, tfeat, sfeat, sflux, totals):
    boxes = own.shape[1]
    half = near // 2
    sums[...] = jnp.zeros(sums.shape, F32)
    store_targets(own, tfeat, turned)
    store_sources([own], sfeat, sflux)

    def target_of(item):
        return jnp.minimum(item, boxes - 1)

    def source_of(item, k):
        return plan[k, jnp.minimum(item, boxes - 1)]

    run_items(
        target_of, source_of, half, boxes // OWN_GROUP, turned, sfeat, sflux, sums, totals
    )


def near_other_kernel(
    near, plan, own, lower, upper, tile, sums_in, turned, out, sums, sfeat, sflux, totals
):
    boxes = lower.shape[1]
    half = near // 2
    sums[...] = sums_in[...]
    store_sources([lower, own, upper], sfeat, sflux)

    def main_target(item):
        return jnp.clip(item, 0, boxes - 1)

    def main_source(item, k):
        return plan[half + k, main_target(item)]

    run_items(
        main_target, main_source, half, boxes // OTHER_GROUP, turned, sfeat, sflux, sums, totals
    )

    counts = [plan[half + near + 2 * pair + 1, 0] for pair in range(half // 2)]

    def extra(item):
        box, row, start = jnp.int32(boxes), jnp.int32(2 * half), jnp.int32(0)
        for pair, count in enumerate(counts):
            inside = (item >= start) & (item < start + count)
            name = plan[half + near + 2 * pair, jnp.clip(item - start, 0, boxes - 1)]
            box = jnp.where(inside, name, box)
            row = jnp.where(inside, 2 * half + 2 * pair, row)
            start = start + count
        return box, row

    def extra_source(item, k):
        box, row = extra(item)
        return plan[row + k, jnp.minimum(box, boxes - 1)]

    iterations = (sum(counts) + OTHER_GROUP - 1) // OTHER_GROUP
    run_items(
        lambda item: extra(item)[0], extra_source, 2, iterations, turned, sfeat, sflux, sums, totals
    )
    out[0:boxes, :] = sums[0:boxes, :] * (1.0 / math.sqrt(near * LANES))

    _, rows, cols = tile.shape
    out[boxes : boxes + EXTRA, :] = jnp.zeros((EXTRA, LANES), F32)
    place = boxes
    for f in (1, 2):
        for r in (rows - 2, rows - 1):
            for c in range(cols // LANES):
                out[place : place + 1, :] = tile[f, r : r + 1, LANES * c : LANES * c + LANES]
                place += 1
    place = boxes + EXTRA - 8
    for f in (1, 2):
        turned_cols = tile[f, :, cols - LANES : cols].T
        out[place : place + 2, 0:rows] = turned_cols[LANES - 2 : LANES, :]
        place += 2


def item_scratch(sources, group):
    return [
        pltpu.VMEM((STORED * (sources + 8), LANES), F32),
        pltpu.VMEM((sources + 8, LANES), F32),
        pltpu.VMEM((group, LANES, LANES), F32),
    ]


def near_cost(boxes, near):
    pairs = boxes * near * LANES * LANES // 2
    return pl.CostEstimate(
        flops=pairs * 2 * FEATURES * 4, transcendentals=pairs, bytes_accessed=4 * 16 * boxes * LANES
    )


def near_own(plan, own, near):
    boxes = own.shape[1]
    assert boxes == LANES and boxes % OWN_GROUP == 0 and near % 4 == 0
    assert boxes % OTHER_GROUP == 0
    vmem = pl.BlockSpec(memory_space=pltpu.VMEM)
    smem = pl.BlockSpec(memory_space=pltpu.SMEM)
    return pl.pallas_call(
        lambda *refs: near_own_kernel(near, *refs),
        out_shape=(
            pltpu.VMEM((boxes + 8, LANES), F32),
            pltpu.VMEM((boxes + 1, LANES, FEATURES), BF16),
        ),
        in_specs=[smem, vmem],
        out_specs=(vmem,) * 2,
        scratch_shapes=[pltpu.VMEM((USED * (boxes + 8), LANES), F32)] + item_scratch(boxes, OWN_GROUP),
        compiler_params=pltpu.CompilerParams(vmem_limit_bytes=VMEM_LIMIT),
        name="near_own",
        cost_estimate=near_cost(boxes, near),
    )(plan, pinned(own))


def near_other(plan, own, lower, upper, tile, sums, turned, near):
    boxes = lower.shape[1]
    vmem = pl.BlockSpec(memory_space=pltpu.VMEM)
    smem = pl.BlockSpec(memory_space=pltpu.SMEM)
    return pl.pallas_call(
        lambda *refs: near_other_kernel(near, *refs),
        out_shape=pltpu.VMEM((boxes + EXTRA, LANES), F32),
        in_specs=[smem] + [vmem] * 6,
        out_specs=vmem,
        scratch_shapes=[pltpu.VMEM((boxes + 8, LANES), F32)] + item_scratch(3 * boxes, OTHER_GROUP),
        compiler_params=pltpu.CompilerParams(vmem_limit_bytes=VMEM_LIMIT),
        name="near_other",
        cost_estimate=near_cost(boxes, near),
    )(plan, *map(pinned, (own, lower, upper, tile, sums, turned)))


def lookup(slot, base, table, pieces, active, out):
    rows, cols = slot.shape
    high_count = rows * cols // WIDE
    across = cols // LANES
    whole = jnp.concatenate([table[0:high_count, :], table[high_count : 2 * high_count, :]], axis=1)
    top = rounded(whole)
    pieces[0:high_count, :] = top.astype(BF16)
    pieces[high_count : 2 * high_count, :] = (whole - top).astype(BF16)

    def window_of(unit):
        row, col = unit // across * 8, unit % across * LANES
        if not isinstance(unit, int):
            row, col = pl.multiple_of(row, 8), pl.multiple_of(col, LANES)
        return pl.ds(row, 8), pl.ds(col, LANES)

    def there(unit):
        high, _ = box_split(slot[window_of(unit)] - base, high_count)
        return (high >= 0.0) & (high < high_count)

    def nodes_of(i, live):
        window = window_of(active[jnp.where(live, i, 0)])
        high, low = box_split(slot[window] - base, high_count)
        return window, jnp.where(live, high, -1.0), low

    def add(i, carry):
        low_iota = lax.broadcasted_iota(jnp.int32, (WIDE, LANES), 0).astype(F32)
        high_iota = lax.broadcasted_iota(jnp.int32, (high_count, LANES), 0).astype(F32)
        units = [nodes_of(UNITS * i + u, UNITS * i + u < count) for u in range(UNITS)]
        hits = [
            jnp.where(low_iota == low[s : s + 1, :], 1.0, 0.0).astype(BF16)
            for _, _, low in units
            for s in range(8)
        ]
        picked = jnp.dot(pieces[...], jnp.concatenate(hits, axis=1), preferred_element_type=F32)
        for u, (window, high, _) in enumerate(units):
            lines = []
            for s in range(8):
                start = LANES * (8 * u + s)
                part = slice(start, start + LANES)
                value = picked[0:high_count, part] + picked[high_count : 2 * high_count, part]
                mine = high_iota == high[s : s + 1, :]
                lines.append(jnp.sum(jnp.where(mine, value, 0.0), axis=0, keepdims=True))
            out[window] += jnp.concatenate(lines, axis=0)
        return carry

    count = list_active(there, rows // 8 * across, active)
    lax.fori_loop(0, (count + UNITS - 1) // UNITS, add, 0)


def base_of(node_count, steps):
    rank = ahead("tx", -steps[0]) * lax.axis_size("ty") + ahead("ty", -steps[1])
    return (rank * node_count).astype(F32)


def own_kernel(tile, table, out, pieces, active):
    out[...] = jnp.zeros(out.shape, F32)
    lookup(tile.at[0], base_of(out.shape[0] * out.shape[1], (0, 0)), table, pieces, active, out)


def row_kernel(tile, ahead_x, partial, behind_x, out, slopes, pieces, active, padded):
    _, rows, cols = tile.shape
    boxes = rows * cols // LANES
    out[...] = partial[...]
    lookup(tile.at[0], base_of(rows * cols, (1, 0)), behind_x, pieces, active, out)
    for f in (1, 2):
        padded[8 : 8 + rows, :] = tile[f]
        for r in range(2):
            for c in range(cols // LANES):
                source = boxes + ((f - 1) * 2 + r) * (cols // LANES) + c
                padded[6 + r : 7 + r, LANES * c : LANES * c + LANES] = behind_x[source : source + 1, :]
        padded[8 + rows : 10 + rows, :] = ahead_x[f, 0:2, :]
        slopes[f - 1] = (
            padded[6 : 6 + rows, :]
            - 8.0 * padded[7 : 7 + rows, :]
            + 8.0 * padded[9 : 9 + rows, :]
            - padded[10 : 10 + rows, :]
        ) / 12.0


def col_kernel(tile, ahead_y, partial, behind_y, out, slopes, pieces, active):
    _, rows, cols = tile.shape
    boxes = rows * cols // LANES
    out[...] = partial[...]
    lookup(tile.at[0], base_of(rows * cols, (0, 1)), behind_y, pieces, active, out)
    left_cols = behind_y[boxes + EXTRA - 8 : boxes + EXTRA, 0:rows].T
    col = lax.broadcasted_iota(jnp.int32, (rows, cols), 1)
    for f in (1, 2):
        here = tile[f]
        left = left_cols[:, 2 * (f - 1) : 2 * f]
        right = ahead_y[f, :, 0:2]
        less_1 = jnp.where(col == 0, left[:, 1:2], pltpu.roll(here, 1, 1))
        less_2 = jnp.where(
            col == 0, left[:, 0:1], jnp.where(col == 1, left[:, 1:2], pltpu.roll(here, 2, 1))
        )
        more_1 = jnp.where(col == cols - 1, right[:, 0:1], pltpu.roll(here, cols - 1, 1))
        more_2 = jnp.where(
            col == cols - 2,
            right[:, 0:1],
            jnp.where(col == cols - 1, right[:, 1:2], pltpu.roll(here, cols - 2, 1)),
        )
        slopes[f - 1] = (less_2 - 8.0 * less_1 + 8.0 * more_1 - more_2) / 12.0


def last_kernel(tile, row_slopes, col_slopes, partial, behind_xy, elev_rate, pot_rate, pieces, active, total):
    _, rows, cols = tile.shape
    total[...] = partial[...]
    lookup(tile.at[0], base_of(rows * cols, (1, 1)), behind_xy, pieces, active, total)
    elev_x, pot_x = row_slopes[0], row_slopes[1]
    elev_y, pot_y = col_slopes[0], col_slopes[1]
    vertical = total[...]
    lift = 1.0 + elev_x * elev_x + elev_y * elev_y
    elev_rate[...] = vertical * lift - (pot_x * elev_x + pot_y * elev_y)
    pot_rate[...] = (
        -tile[1] - 0.5 * (pot_x * pot_x + pot_y * pot_y) + 0.5 * vertical * vertical * lift
    )


def lookup_call(kernel, name, out_shape, args, scratch):
    _, rows, cols = args[0].shape
    vmem = pl.BlockSpec(memory_space=pltpu.VMEM)
    return pl.pallas_call(
        kernel,
        out_shape=out_shape,
        in_specs=[vmem] * len(args),
        out_specs=(vmem,) * len(out_shape),
        scratch_shapes=[
            pltpu.VMEM((2 * rows * cols // WIDE, WIDE), BF16),
            pltpu.SMEM((rows * cols // (8 * LANES),), jnp.int32),
        ]
        + scratch,
        compiler_params=pltpu.CompilerParams(vmem_limit_bytes=VMEM_LIMIT),
        name=name,
        cost_estimate=pl.CostEstimate(
            flops=rows * cols * rows * cols, transcendentals=0, bytes_accessed=4 * 8 * rows * cols
        ),
    )(*map(pinned, args))


def look_up_all(tile, ahead_x, ahead_y, value, behind_x, behind_y, behind_xy):
    _, rows, cols = tile.shape
    values = pltpu.VMEM((rows, cols), F32)
    slopes = pltpu.VMEM((2, rows, cols), F32)
    (partial,) = lookup_call(own_kernel, "lookup_own", (values,), (tile, value), [])
    partial, row_slopes = lookup_call(
        row_kernel,
        "lookup_x",
        (values, slopes),
        (tile, ahead_x, partial, behind_x),
        [pltpu.VMEM((rows + 16, cols), F32)],
    )
    partial, col_slopes = lookup_call(
        col_kernel, "lookup_y", (values, slopes), (tile, ahead_y, partial, behind_y), []
    )
    shape = jax.ShapeDtypeStruct((rows, cols), F32)
    return lookup_call(
        last_kernel,
        "lookup_xy",
        (shape, shape),
        (tile, row_slopes, col_slopes, partial, behind_xy),
        [pltpu.VMEM((rows, cols), F32)],
    )


def shards(potential, elevation, normal_flux, box_owner, box_place, near_boxes):
    rows, cols = potential.shape
    count_tx = lax.axis_size("tx")
    count_ty = lax.axis_size("ty")
    node_count = rows * cols
    boxes = node_count // LANES
    near = near_boxes.shape[1]
    assert node_count % WIDE == 0 and cols <= 256 and rows <= 128
    assert 4 * (cols // LANES) <= EXTRA - 8
    assert node_count * count_tx * count_ty < 2**24

    slot = (box_owner * node_count + box_place).astype(F32)
    tile = jnp.stack([slot, elevation, potential, normal_flux])
    ahead_x = shifted(tile, "tx", -1)
    ahead_y = shifted(tile, "ty", -1)
    ahead_xy = shifted(ahead_y, "tx", -1)
    tile, ahead_x, ahead_y, ahead_xy = map(pinned, (tile, ahead_x, ahead_y, ahead_xy))

    sizes = (rows * count_tx, cols * count_ty)
    acc, plan = scatter((0, 0), tile, None, False, *sizes, near_boxes.T)
    acc = scatter((1, 0), ahead_x, acc, False, *sizes)
    acc = scatter((0, 1), ahead_y, acc, False, *sizes)
    boxed = scatter((1, 1), ahead_xy, acc, True, *sizes)

    total = count_tx * count_ty
    both = ("tx", "ty")
    lower = lax.ppermute(boxed, both, [(i, i + 1) for i in range(total - 1)])
    upper = lax.ppermute(boxed, both, [(i + 1, i) for i in range(total - 1)])

    sums, turned = near_own(plan, boxed, near)
    value = near_other(plan, boxed, lower, upper, tile, sums, turned, near)

    behind_x = shifted(value, "tx", 1)
    behind_y = shifted(value, "ty", 1)
    diagonal = [
        (i * count_ty + j, (i + 1) % count_tx * count_ty + (j + 1) % count_ty)
        for i in range(count_tx)
        for j in range(count_ty)
    ]
    behind_xy = lax.ppermute(value, both, diagonal)
    return look_up_all(tile, ahead_x, ahead_y, value, behind_x, behind_y, behind_xy)


def solution(mesh):
    in_specs = (
        P("tx", "ty"),
        P("tx", "ty"),
        P("tx", "ty"),
        P("tx", "ty"),
        P("tx", "ty"),
        P(("tx", "ty"), None),
    )
    out_specs = (P("tx", "ty"), P("tx", "ty"))
    return jax.shard_map(shards, mesh=mesh, in_specs=in_specs, out_specs=out_specs, check_vma=False)
```

```python
import math

import jax
import jax.numpy as jnp
from jax import lax
from jax.experimental import pallas as pl
from jax.experimental.pallas import tpu as pltpu
from jax.sharding import PartitionSpec as P

LANES = 128
WIDE = 256
PIECES = 6
FEATURES = 32
USED = 24
STORED = USED + 8
EXTRA = 16
UNITS = 5
OWN_GROUP = 16
OTHER_GROUP = 16
VMEM_LIMIT = 24 << 20
BF16 = jnp.bfloat16
F32 = jnp.float32


def shifted(value, axis, steps):
    count = lax.axis_size(axis)
    pairs = [(source, (source + steps) % count) for source in range(count)]
    return lax.ppermute(value, axis, pairs)


def ahead(axis, steps):
    index = lax.axis_index(axis) + steps
    count = lax.axis_size(axis)
    return jnp.where(index < 0, index + count, jnp.where(index >= count, index - count, index))


def pinned(value):
    return pltpu.with_memory_space_constraint(value, pltpu.VMEM)


def rounded(value):
    return value.astype(BF16).astype(F32)


def box_split(rel, high_count):
    box = jnp.floor(rel * (1.0 / LANES))
    second = box >= high_count
    high = jnp.where(second, box - high_count, box)
    low = rel - box * LANES
    return high, jnp.where(second, low + LANES, low)


def list_active(test, count, active):
    flags = [jnp.max(jnp.where(test(unit), 1.0, 0.0)) > 0.0 for unit in range(count)]
    found = jnp.int32(0)
    for unit, flag in enumerate(flags):
        active[found] = unit
        found = found + jnp.where(flag, 1, 0)
    return found


def scatter_kernel(first, last, sizes, steps, tile, *refs):
    active = refs[-1]
    if first:
        listed, acc, plan = refs[:3]
        plan_rows(listed, plan)
    else:
        acc_in, acc = refs[:2]
    rows, cols, high_count, node_rows, node_cols = sizes
    p = lax.axis_index("tx")
    q = lax.axis_index("ty")
    base = ((p * lax.axis_size("ty") + q) * (rows * cols)).astype(F32)
    off_i = float(steps[0] * rows)
    off_j = float((steps[1] - 1) * cols)
    acc[...] = jnp.zeros(acc.shape, F32) if first else acc_in[...]
    across = cols // LANES

    def window_of(unit):
        row, col = unit // across * 8, unit % across * LANES
        if not isinstance(unit, int):
            row, col = pl.multiple_of(row, 8), pl.multiple_of(col, LANES)
        return row, col, (pl.ds(row, 8), pl.ds(col, LANES))

    def mine(unit):
        high, _ = box_split(tile[(0,) + window_of(unit)[2]] - base, high_count)
        return (high >= 0.0) & (high < high_count)

    def sides(i, live):
        row0, col0, window = window_of(active[jnp.where(live, i, 0)])
        high, low = box_split(tile[(0,) + window] - base, high_count)
        high = jnp.where(live, high, -1.0)
        z = 0.25 * tile[(1,) + window]
        z_high = rounded(z)
        z_low = z - z_high
        pot = tile[(2,) + window]
        flux = tile[(3,) + window]
        shift = col0.astype(F32) + off_j
        col_index = lax.broadcasted_iota(jnp.int32, (high_count, LANES), 1).astype(F32) + shift
        high_iota = lax.broadcasted_iota(jnp.int32, (high_count, LANES), 0).astype(F32)
        low_iota = lax.broadcasted_iota(jnp.int32, (WIDE, LANES), 0).astype(F32)
        lefts = []
        rights = []
        for s in range(8):

            def row(v):
                return v[s : s + 1, :]

            hit = high_iota == row(high)
            row_index = jnp.full((1, LANES), (row0 + s).astype(F32) + off_i, F32)
            values = [row_index, col_index, row(z_high), row(z_low), row(pot), row(flux)]
            lefts.append(
                jnp.concatenate([jnp.where(hit, v, 0.0).astype(BF16) for v in values], axis=0)
            )
            rights.append(jnp.where(low_iota == row(low), 1.0, 0.0).astype(BF16))
        return lefts, rights

    def add(i, carry):
        lefts, rights = [], []
        for u in range(UNITS):
            left, right = sides(UNITS * i + u, UNITS * i + u < count)
            lefts += left
            rights += right
        acc[...] += lax.dot_general(
            jnp.concatenate(lefts, axis=1),
            jnp.concatenate(rights, axis=1),
            (((1,), (1,)), ((), ())),
            preferred_element_type=F32,
        )
        return carry

    count = list_active(mine, rows // 8 * across, active)
    lax.fori_loop(0, (count + UNITS - 1) // UNITS, add, 0)

    if last:
        boxed = refs[-2]
        h = high_count
        row0 = (p * rows).astype(F32)
        col0 = ((q + 1) * cols).astype(F32)
        i = acc[0:h] + row0
        i = jnp.where(i >= node_rows, i - node_rows, i)
        j = acc[h : 2 * h] + col0
        j = jnp.where(j >= node_cols, j - node_cols, j)
        fields = [
            (i + 0.5) / node_rows,
            (j + 0.5) / node_cols,
            acc[2 * h : 3 * h] + acc[3 * h : 4 * h],
            acc[4 * h : 5 * h],
            acc[5 * h : 6 * h],
        ]
        for k, f in enumerate(fields):
            boxed[k, 0:h, :] = f[:, :LANES]
            boxed[k, h : 2 * h, :] = f[:, LANES:]


def scatter(steps, tile, acc, last, node_rows, node_cols, listed=None):
    _, rows, cols = tile.shape
    high_count = rows * cols // WIDE
    first = acc is None
    vmem = pl.BlockSpec(memory_space=pltpu.VMEM)
    out_shape = [pltpu.VMEM((PIECES * high_count, WIDE), F32)]
    if last:
        out_shape.append(pltpu.VMEM((5, 2 * high_count, LANES), F32))
    if first:
        near, boxes = listed.shape
        out_shape.append(jax.ShapeDtypeStruct(((2 * near + 7) // 8 * 8, boxes), jnp.int32))
    args = (tile, listed) if first else (tile, pinned(acc))
    out = pl.pallas_call(
        lambda *refs: scatter_kernel(
            first, last, (rows, cols, high_count, node_rows, node_cols), steps, *refs
        ),
        out_shape=out_shape,
        in_specs=[vmem] * len(args),
        out_specs=[vmem] * len(out_shape),
        scratch_shapes=[pltpu.SMEM((rows * cols // (8 * LANES),), jnp.int32)],
        compiler_params=pltpu.CompilerParams(vmem_limit_bytes=VMEM_LIMIT),
        name="scatter_last" if last else "scatter_first" if first else "scatter",
        cost_estimate=pl.CostEstimate(
            flops=2 * PIECES * high_count * WIDE * rows * cols // 2,
            transcendentals=0,
            bytes_accessed=4 * (2 * PIECES * high_count * WIDE + 4 * rows * cols),
        ),
    )(*args)
    return out[1] if last else out if first else out[0]


def thirds(value):
    high = rounded(value)
    middle = rounded(value - high)
    return high, middle, value - high - middle


def plan_rows(listed, plan):
    near, boxes = listed.shape
    half = near // 2
    rank = lax.axis_index("tx") * lax.axis_size("ty") + lax.axis_index("ty")
    n = listed[...] - (rank - 1) * boxes
    taken = jnp.zeros((1, boxes), jnp.int32)
    left = jnp.zeros((1, boxes), jnp.int32)
    first = [jnp.full((1, boxes), boxes, jnp.int32) for _ in range(half)]
    rest = [jnp.full((1, boxes), 3 * boxes, jnp.int32) for _ in range(near)]
    for k in range(near):
        row = n[k : k + 1, :]
        take = (row >= boxes) & (row < 2 * boxes) & (taken < half)
        first = [jnp.where(take & (taken == j), row - boxes, v) for j, v in enumerate(first)]
        rest = [jnp.where(take | (left != j), v, row) for j, v in enumerate(rest)]
        step = jnp.where(take, 1, 0)
        taken = taken + step
        left = left + 1 - step
    for j, v in enumerate(first + rest):
        plan[j : j + 1, :] = v
    down = lax.broadcasted_iota(jnp.int32, (boxes, boxes), 0)
    across = lax.broadcasted_iota(jnp.int32, (boxes, boxes), 1)
    before = jnp.where(down < across, 1.0, 0.0).astype(BF16)
    names = lax.broadcasted_iota(jnp.int32, (8, boxes), 1).astype(F32).astype(BF16)
    for pair in range(half // 2):
        over = left > half + 2 * pair
        flags = jnp.broadcast_to(jnp.where(over, 1.0, 0.0), (8, boxes)).astype(BF16)
        offset = jnp.dot(flags, before, preferred_element_type=F32)[0:1, :]
        count = jnp.dot(flags, jnp.ones((boxes, boxes), BF16), preferred_element_type=F32)[0:1, :]
        hit = jnp.where((down.astype(F32) == offset) & over, 1.0, 0.0).astype(BF16)
        found = lax.dot_general(
            names, hit, (((1,), (1,)), ((), ())), preferred_element_type=F32
        )[0:1, :].astype(jnp.int32)
        count = count.astype(jnp.int32)
        place = half + near + 2 * pair
        plan[place : place + 1, :] = jnp.where(across[0:1, :] < count, found, boxes)
        plan[place + 1 : place + 2, :] = count


def pieces_of(ref, group):
    window = (pl.ds(pl.multiple_of(8 * group, 8), 8), slice(None))
    x, y, z, pot, flux = (ref[(f,) + window] for f in range(5))
    pieces = []
    total = None
    for v in (x, y, z):
        high = rounded(v)
        low = rounded(v - high)
        kept = high + low
        pieces.append((high, low))
        total = kept * kept if total is None else total + kept * kept
    return pieces, total, pot, flux


def padded_rows(values):
    return values + [jnp.zeros_like(values[0])] * (USED - len(values))


def moment_side(ref, n):
    pitch = ref.shape[0] // STORED
    rows = ref[pl.ds(USED * pitch + n, 8, stride=pitch), :]
    zeros = jnp.zeros((8, LANES), F32)
    return jnp.concatenate([zeros, rows] + [zeros] * (FEATURES // 8 - 2), axis=0).astype(BF16)


def strided(ref, n, stored):
    pitch = ref.shape[0] // stored
    rows = [ref[pl.ds(8 * g * pitch + n, 8, stride=pitch), :] for g in range(USED // 8)]
    return jnp.concatenate(rows + [jnp.zeros((8, LANES), F32)] * ((FEATURES - USED) // 8), axis=0)


def store_sources(refs, sfeat, sflux):
    pitch = sfeat.shape[0] // STORED
    ones = jnp.ones((8, LANES), F32)
    zeros = jnp.zeros((8, LANES), F32)
    boxes = refs[0].shape[1]
    for which, ref in enumerate(refs):

        def store(group, carry):
            pieces, total, pot, flux = pieces_of(ref, group)
            source = []
            for high, low in pieces:
                source += [-2.0 * high, -2.0 * low, -2.0 * high, -2.0 * low]
            z = pieces[2][0] + pieces[2][1]
            rows = padded_rows(source + list(thirds(total)) + [ones, ones, ones])
            rows += [pot, zeros, pot, zeros] + list(thirds(-pot * z)) + [zeros]
            start = pl.multiple_of(which * boxes + 8 * group, 8)
            for k, v in enumerate(rows):
                sfeat[pl.ds(pl.multiple_of(k * pitch + start, 8), 8), :] = v
            sflux[pl.ds(start, 8), :] = flux
            return carry

        lax.fori_loop(0, boxes // 8, store, 0, unroll=2)
    start = len(refs) * boxes
    for k in range(STORED):
        sfeat[k * pitch + start : k * pitch + start + 8, :] = ones if k == 12 else zeros
    sflux[start : start + 8, :] = zeros


def store_targets(own, tfeat, turned):
    boxes = own.shape[1]
    pitch = tfeat.shape[0] // USED
    ones = jnp.ones((8, LANES), F32)

    def store(group, carry):
        pieces, total, _, _ = pieces_of(own, group)
        target = []
        for high, low in pieces:
            target += [high, high, low, low]
        for k, v in enumerate(padded_rows(target + [ones, ones, ones] + list(thirds(total + 0.04)))):
            tfeat[pl.ds(pl.multiple_of(k * pitch + 8 * group, 8), 8), :] = v
        return carry

    lax.fori_loop(0, boxes // 8, store, 0, unroll=2)
    turned[boxes] = jnp.zeros((LANES, FEATURES), BF16)

    def turn(i, carry):
        for u in range(16):
            turned[16 * i + u] = strided(tfeat, 16 * i + u, USED).T.astype(BF16)
        return carry

    lax.fori_loop(0, boxes // 16, turn, 0)


def run_items(target_of, source_of, half, iterations, turned, sfeat, sflux, sums, totals):
    empty_row = sums.shape[0] - 8
    group = totals.shape[0]

    def apply(item, total):
        target = target_of(item)
        sides = [strided(sfeat, source_of(item, k), STORED).astype(BF16) for k in range(half)]
        sides += [moment_side(sfeat, source_of(item, k)) for k in range(half)]
        squared = jnp.dot(turned[target], jnp.concatenate(sides, axis=1), preferred_element_type=F32)
        fluxes = [
            jnp.broadcast_to(sflux[pl.ds(source_of(item, k), 1), :], (8, LANES)) for k in range(half)
        ]
        for t in range(LANES // 8):
            rows = slice(8 * t, 8 * t + 8)
            value = None
            for k, flux in enumerate(fluxes):
                inverse = lax.rsqrt(squared[rows, LANES * k : LANES * (k + 1)])
                moment = squared[rows, LANES * (half + k) : LANES * (half + k + 1)]
                part = inverse * (flux - (inverse * inverse) * moment)
                value = part if value is None else value + part
            total[rows, :] = value

    def reduce(item, total, live):
        target = jnp.where(live, target_of(jnp.maximum(item, 0)), empty_row)
        sums[pl.ds(target, 1), :] += jnp.sum(total[...].T, axis=0, keepdims=True)

    def step(i, carry):
        for u in range(group):
            reduce(group * (i - 1) + u, totals.at[u], i > 0)
        for u in range(group):
            apply(group * i + u, totals.at[u])
        return carry

    totals[...] = jnp.zeros(totals.shape, F32)
    lax.fori_loop(0, iterations, step, 0)
    for u in range(group):
        reduce(group * (iterations - 1) + u, totals.at[u], iterations > 0)


def near_own_kernel(near, plan, own, sums, turned, tfeat, sfeat, sflux, totals):
    boxes = own.shape[1]
    half = near // 2
    sums[...] = jnp.zeros(sums.shape, F32)
    store_targets(own, tfeat, turned)
    store_sources([own], sfeat, sflux)

    def target_of(item):
        return jnp.minimum(item, boxes - 1)

    def source_of(item, k):
        return plan[k, jnp.minimum(item, boxes - 1)]

    run_items(
        target_of, source_of, half, boxes // OWN_GROUP, turned, sfeat, sflux, sums, totals
    )


def near_other_kernel(
    near, plan, own, lower, upper, tile, sums_in, turned, out, sums, sfeat, sflux, totals
):
    boxes = lower.shape[1]
    half = near // 2
    sums[...] = sums_in[...]
    store_sources([lower, own, upper], sfeat, sflux)

    def main_target(item):
        return jnp.clip(item, 0, boxes - 1)

    def main_source(item, k):
        return plan[half + k, main_target(item)]

    run_items(
        main_target, main_source, half, boxes // OTHER_GROUP, turned, sfeat, sflux, sums, totals
    )

    counts = [plan[half + near + 2 * pair + 1, 0] for pair in range(half // 2)]

    def extra(item):
        box, row, start = jnp.int32(boxes), jnp.int32(2 * half), jnp.int32(0)
        for pair, count in enumerate(counts):
            inside = (item >= start) & (item < start + count)
            name = plan[half + near + 2 * pair, jnp.clip(item - start, 0, boxes - 1)]
            box = jnp.where(inside, name, box)
            row = jnp.where(inside, 2 * half + 2 * pair, row)
            start = start + count
        return box, row

    def extra_source(item, k):
        box, row = extra(item)
        return plan[row + k, jnp.minimum(box, boxes - 1)]

    iterations = (sum(counts) + OTHER_GROUP - 1) // OTHER_GROUP
    run_items(
        lambda item: extra(item)[0], extra_source, 2, iterations, turned, sfeat, sflux, sums, totals
    )
    out[0:boxes, :] = sums[0:boxes, :] * (1.0 / math.sqrt(near * LANES))

    _, rows, cols = tile.shape
    out[boxes : boxes + EXTRA, :] = jnp.zeros((EXTRA, LANES), F32)
    place = boxes
    for f in (1, 2):
        for r in (rows - 2, rows - 1):
            for c in range(cols // LANES):
                out[place : place + 1, :] = tile[f, r : r + 1, LANES * c : LANES * c + LANES]
                place += 1
    place = boxes + EXTRA - 8
    for f in (1, 2):
        turned_cols = tile[f, :, cols - LANES : cols].T
        out[place : place + 2, 0:rows] = turned_cols[LANES - 2 : LANES, :]
        place += 2


def item_scratch(sources, group):
    return [
        pltpu.VMEM((STORED * (sources + 8), LANES), F32),
        pltpu.VMEM((sources + 8, LANES), F32),
        pltpu.VMEM((group, LANES, LANES), F32),
    ]


def near_cost(boxes, near):
    pairs = boxes * near * LANES * LANES // 2
    return pl.CostEstimate(
        flops=pairs * 2 * FEATURES * 4, transcendentals=pairs, bytes_accessed=4 * 16 * boxes * LANES
    )


def near_own(plan, own, near):
    boxes = own.shape[1]
    assert boxes == LANES and boxes % OWN_GROUP == 0 and near % 4 == 0
    assert boxes % OTHER_GROUP == 0
    vmem = pl.BlockSpec(memory_space=pltpu.VMEM)
    smem = pl.BlockSpec(memory_space=pltpu.SMEM)
    return pl.pallas_call(
        lambda *refs: near_own_kernel(near, *refs),
        out_shape=(
            pltpu.VMEM((boxes + 8, LANES), F32),
            pltpu.VMEM((boxes + 1, LANES, FEATURES), BF16),
        ),
        in_specs=[smem, vmem],
        out_specs=(vmem,) * 2,
        scratch_shapes=[pltpu.VMEM((USED * (boxes + 8), LANES), F32)] + item_scratch(boxes, OWN_GROUP),
        compiler_params=pltpu.CompilerParams(vmem_limit_bytes=VMEM_LIMIT),
        name="near_own",
        cost_estimate=near_cost(boxes, near),
    )(plan, pinned(own))


def near_other(plan, own, lower, upper, tile, sums, turned, near):
    boxes = lower.shape[1]
    vmem = pl.BlockSpec(memory_space=pltpu.VMEM)
    smem = pl.BlockSpec(memory_space=pltpu.SMEM)
    return pl.pallas_call(
        lambda *refs: near_other_kernel(near, *refs),
        out_shape=pltpu.VMEM((boxes + EXTRA, LANES), F32),
        in_specs=[smem] + [vmem] * 6,
        out_specs=vmem,
        scratch_shapes=[pltpu.VMEM((boxes + 8, LANES), F32)] + item_scratch(3 * boxes, OTHER_GROUP),
        compiler_params=pltpu.CompilerParams(vmem_limit_bytes=VMEM_LIMIT),
        name="near_other",
        cost_estimate=near_cost(boxes, near),
    )(plan, *map(pinned, (own, lower, upper, tile, sums, turned)))


def lookup(slot, base, table, pieces, active, out):
    rows, cols = slot.shape
    high_count = rows * cols // WIDE
    across = cols // LANES
    whole = jnp.concatenate([table[0:high_count, :], table[high_count : 2 * high_count, :]], axis=1)
    top = rounded(whole)
    pieces[0:high_count, :] = top.astype(BF16)
    pieces[high_count : 2 * high_count, :] = (whole - top).astype(BF16)

    def window_of(unit):
        row, col = unit // across * 8, unit % across * LANES
        if not isinstance(unit, int):
            row, col = pl.multiple_of(row, 8), pl.multiple_of(col, LANES)
        return pl.ds(row, 8), pl.ds(col, LANES)

    def there(unit):
        high, _ = box_split(slot[window_of(unit)] - base, high_count)
        return (high >= 0.0) & (high < high_count)

    def nodes_of(i, live):
        window = window_of(active[jnp.where(live, i, 0)])
        high, low = box_split(slot[window] - base, high_count)
        return window, jnp.where(live, high, -1.0), low

    def add(i, carry):
        low_iota = lax.broadcasted_iota(jnp.int32, (WIDE, LANES), 0).astype(F32)
        high_iota = lax.broadcasted_iota(jnp.int32, (high_count, LANES), 0).astype(F32)
        units = [nodes_of(UNITS * i + u, UNITS * i + u < count) for u in range(UNITS)]
        hits = [
            jnp.where(low_iota == low[s : s + 1, :], 1.0, 0.0).astype(BF16)
            for _, _, low in units
            for s in range(8)
        ]
        picked = jnp.dot(pieces[...], jnp.concatenate(hits, axis=1), preferred_element_type=F32)
        for u, (window, high, _) in enumerate(units):
            lines = []
            for s in range(8):
                start = LANES * (8 * u + s)
                part = slice(start, start + LANES)
                value = picked[0:high_count, part] + picked[high_count : 2 * high_count, part]
                mine = high_iota == high[s : s + 1, :]
                lines.append(jnp.sum(jnp.where(mine, value, 0.0), axis=0, keepdims=True))
            out[window] += jnp.concatenate(lines, axis=0)
        return carry

    count = list_active(there, rows // 8 * across, active)
    lax.fori_loop(0, (count + UNITS - 1) // UNITS, add, 0)


def base_of(node_count, steps):
    rank = ahead("tx", -steps[0]) * lax.axis_size("ty") + ahead("ty", -steps[1])
    return (rank * node_count).astype(F32)


def own_kernel(tile, table, out, pieces, active):
    out[...] = jnp.zeros(out.shape, F32)
    lookup(tile.at[0], base_of(out.shape[0] * out.shape[1], (0, 0)), table, pieces, active, out)


def row_kernel(tile, ahead_x, partial, behind_x, out, slopes, pieces, active, padded):
    _, rows, cols = tile.shape
    boxes = rows * cols // LANES
    out[...] = partial[...]
    lookup(tile.at[0], base_of(rows * cols, (1, 0)), behind_x, pieces, active, out)
    for f in (1, 2):
        padded[8 : 8 + rows, :] = tile[f]
        for r in range(2):
            for c in range(cols // LANES):
                source = boxes + ((f - 1) * 2 + r) * (cols // LANES) + c
                padded[6 + r : 7 + r, LANES * c : LANES * c + LANES] = behind_x[source : source + 1, :]
        padded[8 + rows : 10 + rows, :] = ahead_x[f, 0:2, :]
        slopes[f - 1] = (
            padded[6 : 6 + rows, :]
            - 8.0 * padded[7 : 7 + rows, :]
            + 8.0 * padded[9 : 9 + rows, :]
            - padded[10 : 10 + rows, :]
        ) / 12.0


def col_kernel(tile, ahead_y, partial, behind_y, out, slopes, pieces, active):
    _, rows, cols = tile.shape
    boxes = rows * cols // LANES
    out[...] = partial[...]
    lookup(tile.at[0], base_of(rows * cols, (0, 1)), behind_y, pieces, active, out)
    left_cols = behind_y[boxes + EXTRA - 8 : boxes + EXTRA, 0:rows].T
    col = lax.broadcasted_iota(jnp.int32, (rows, cols), 1)
    for f in (1, 2):
        here = tile[f]
        left = left_cols[:, 2 * (f - 1) : 2 * f]
        right = ahead_y[f, :, 0:2]
        less_1 = jnp.where(col == 0, left[:, 1:2], pltpu.roll(here, 1, 1))
        less_2 = jnp.where(
            col == 0, left[:, 0:1], jnp.where(col == 1, left[:, 1:2], pltpu.roll(here, 2, 1))
        )
        more_1 = jnp.where(col == cols - 1, right[:, 0:1], pltpu.roll(here, cols - 1, 1))
        more_2 = jnp.where(
            col == cols - 2,
            right[:, 0:1],
            jnp.where(col == cols - 1, right[:, 1:2], pltpu.roll(here, cols - 2, 1)),
        )
        slopes[f - 1] = (less_2 - 8.0 * less_1 + 8.0 * more_1 - more_2) / 12.0


def last_kernel(tile, row_slopes, col_slopes, partial, behind_xy, elev_rate, pot_rate, pieces, active, total):
    _, rows, cols = tile.shape
    total[...] = partial[...]
    lookup(tile.at[0], base_of(rows * cols, (1, 1)), behind_xy, pieces, active, total)
    elev_x, pot_x = row_slopes[0], row_slopes[1]
    elev_y, pot_y = col_slopes[0], col_slopes[1]
    vertical = total[...]
    lift = 1.0 + elev_x * elev_x + elev_y * elev_y
    elev_rate[...] = vertical * lift - (pot_x * elev_x + pot_y * elev_y)
    pot_rate[...] = (
        -tile[1] - 0.5 * (pot_x * pot_x + pot_y * pot_y) + 0.5 * vertical * vertical * lift
    )


def lookup_call(kernel, name, out_shape, args, scratch):
    _, rows, cols = args[0].shape
    vmem = pl.BlockSpec(memory_space=pltpu.VMEM)
    return pl.pallas_call(
        kernel,
        out_shape=out_shape,
        in_specs=[vmem] * len(args),
        out_specs=(vmem,) * len(out_shape),
        scratch_shapes=[
            pltpu.VMEM((2 * rows * cols // WIDE, WIDE), BF16),
            pltpu.SMEM((rows * cols // (8 * LANES),), jnp.int32),
        ]
        + scratch,
        compiler_params=pltpu.CompilerParams(vmem_limit_bytes=VMEM_LIMIT),
        name=name,
        cost_estimate=pl.CostEstimate(
            flops=rows * cols * rows * cols, transcendentals=0, bytes_accessed=4 * 8 * rows * cols
        ),
    )(*map(pinned, args))


def look_up_all(tile, ahead_x, ahead_y, value, behind_x, behind_y, behind_xy):
    _, rows, cols = tile.shape
    values = pltpu.VMEM((rows, cols), F32)
    slopes = pltpu.VMEM((2, rows, cols), F32)
    (partial,) = lookup_call(own_kernel, "lookup_own", (values,), (tile, value), [])
    partial, row_slopes = lookup_call(
        row_kernel,
        "lookup_x",
        (values, slopes),
        (tile, ahead_x, partial, behind_x),
        [pltpu.VMEM((rows + 16, cols), F32)],
    )
    partial, col_slopes = lookup_call(
        col_kernel, "lookup_y", (values, slopes), (tile, ahead_y, partial, behind_y), []
    )
    shape = jax.ShapeDtypeStruct((rows, cols), F32)
    return lookup_call(
        last_kernel,
        "lookup_xy",
        (shape, shape),
        (tile, row_slopes, col_slopes, partial, behind_xy),
        [pltpu.VMEM((rows, cols), F32)],
    )


def shards(potential, elevation, normal_flux, box_owner, box_place, near_boxes):
    rows, cols = potential.shape
    count_tx = lax.axis_size("tx")
    count_ty = lax.axis_size("ty")
    node_count = rows * cols
    boxes = node_count // LANES
    near = near_boxes.shape[1]
    assert node_count % WIDE == 0 and cols <= 256 and rows <= 128
    assert 4 * (cols // LANES) <= EXTRA - 8
    assert node_count * count_tx * count_ty < 2**24

    slot = (box_owner * node_count + box_place).astype(F32)
    tile = jnp.stack([slot, elevation, potential, normal_flux])
    ahead_x = shifted(tile, "tx", -1)
    ahead_y = shifted(tile, "ty", -1)
    ahead_xy = shifted(ahead_y, "tx", -1)
    tile, ahead_x, ahead_y, ahead_xy = map(pinned, (tile, ahead_x, ahead_y, ahead_xy))

    sizes = (rows * count_tx, cols * count_ty)
    acc, plan = scatter((0, 0), tile, None, False, *sizes, near_boxes.T)
    acc = scatter((1, 0), ahead_x, acc, False, *sizes)
    acc = scatter((0, 1), ahead_y, acc, False, *sizes)
    boxed = scatter((1, 1), ahead_xy, acc, True, *sizes)

    total = count_tx * count_ty
    both = ("tx", "ty")
    lower = lax.ppermute(boxed, both, [(i, i + 1) for i in range(total - 1)])
    upper = lax.ppermute(boxed, both, [(i + 1, i) for i in range(total - 1)])

    sums, turned = near_own(plan, boxed, near)
    value = near_other(plan, boxed, lower, upper, tile, sums, turned, near)

    behind_x = shifted(value, "tx", 1)
    behind_y = shifted(value, "ty", 1)
    behind_xy = shifted(behind_y, "tx", 1)
    return look_up_all(tile, ahead_x, ahead_y, value, behind_x, behind_y, behind_xy)


def solution(mesh):
    in_specs = (
        P("tx", "ty"),
        P("tx", "ty"),
        P("tx", "ty"),
        P("tx", "ty"),
        P("tx", "ty"),
        P(("tx", "ty"), None),
    )
    out_specs = (P("tx", "ty"), P("tx", "ty"))
    return jax.shard_map(shards, mesh=mesh, in_specs=in_specs, out_specs=out_specs, check_vma=False)
```

```python
import math

import jax
import jax.numpy as jnp
from jax import lax
from jax.experimental import pallas as pl
from jax.experimental.pallas import tpu as pltpu
from jax.sharding import PartitionSpec as P

LANES = 128
WIDE = 256
PIECES = 6
FEATURES = 32
USED = 24
STORED = USED + 8
EXTRA = 16
UNITS = 5
OWN_GROUP = 16
OTHER_GROUP = 32
EXTRA_GROUP = 16
VMEM_LIMIT = 24 << 20
BF16 = jnp.bfloat16
F32 = jnp.float32


def shifted(value, axis, steps):
    count = lax.axis_size(axis)
    pairs = [(source, (source + steps) % count) for source in range(count)]
    return lax.ppermute(value, axis, pairs)


def ahead(axis, steps):
    index = lax.axis_index(axis) + steps
    count = lax.axis_size(axis)
    return jnp.where(index < 0, index + count, jnp.where(index >= count, index - count, index))


def pinned(value):
    return pltpu.with_memory_space_constraint(value, pltpu.VMEM)


def rounded(value):
    return value.astype(BF16).astype(F32)


def box_split(rel, high_count):
    box = jnp.floor(rel * (1.0 / LANES))
    second = box >= high_count
    high = jnp.where(second, box - high_count, box)
    low = rel - box * LANES
    return high, jnp.where(second, low + LANES, low)


def list_active(test, count, active):
    flags = [jnp.max(jnp.where(test(unit), 1.0, 0.0)) > 0.0 for unit in range(count)]
    found = jnp.int32(0)
    for unit, flag in enumerate(flags):
        active[found] = unit
        found = found + jnp.where(flag, 1, 0)
    return found


def scatter_kernel(first, last, sizes, steps, tile, *refs):
    active = refs[-1]
    if first:
        listed, acc, plan = refs[:3]
        plan_rows(listed, plan)
    else:
        acc_in, acc = refs[:2]
    rows, cols, high_count, node_rows, node_cols = sizes
    p = lax.axis_index("tx")
    q = lax.axis_index("ty")
    base = ((p * lax.axis_size("ty") + q) * (rows * cols)).astype(F32)
    off_i = float(steps[0] * rows)
    off_j = float((steps[1] - 1) * cols)
    acc[...] = jnp.zeros(acc.shape, F32) if first else acc_in[...]
    across = cols // LANES

    def window_of(unit):
        row, col = unit // across * 8, unit % across * LANES
        if not isinstance(unit, int):
            row, col = pl.multiple_of(row, 8), pl.multiple_of(col, LANES)
        return row, col, (pl.ds(row, 8), pl.ds(col, LANES))

    def mine(unit):
        high, _ = box_split(tile[(0,) + window_of(unit)[2]] - base, high_count)
        return (high >= 0.0) & (high < high_count)

    def sides(i, live):
        row0, col0, window = window_of(active[jnp.where(live, i, 0)])
        high, low = box_split(tile[(0,) + window] - base, high_count)
        high = jnp.where(live, high, -1.0)
        z = 0.25 * tile[(1,) + window]
        z_high = rounded(z)
        z_low = z - z_high
        pot = tile[(2,) + window]
        flux = tile[(3,) + window]
        shift = col0.astype(F32) + off_j
        col_index = lax.broadcasted_iota(jnp.int32, (high_count, LANES), 1).astype(F32) + shift
        high_iota = lax.broadcasted_iota(jnp.int32, (high_count, LANES), 0).astype(F32)
        low_iota = lax.broadcasted_iota(jnp.int32, (WIDE, LANES), 0).astype(F32)
        lefts = []
        rights = []
        for s in range(8):

            def row(v):
                return v[s : s + 1, :]

            hit = high_iota == row(high)
            row_index = jnp.full((1, LANES), (row0 + s).astype(F32) + off_i, F32)
            values = [row_index, col_index, row(z_high), row(z_low), row(pot), row(flux)]
            lefts.append(
                jnp.concatenate([jnp.where(hit, v, 0.0).astype(BF16) for v in values], axis=0)
            )
            rights.append(jnp.where(low_iota == row(low), 1.0, 0.0).astype(BF16))
        return lefts, rights

    def add(i, carry):
        lefts, rights = [], []
        for u in range(UNITS):
            left, right = sides(UNITS * i + u, UNITS * i + u < count)
            lefts += left
            rights += right
        acc[...] += lax.dot_general(
            jnp.concatenate(lefts, axis=1),
            jnp.concatenate(rights, axis=1),
            (((1,), (1,)), ((), ())),
            preferred_element_type=F32,
        )
        return carry

    count = list_active(mine, rows // 8 * across, active)
    lax.fori_loop(0, (count + UNITS - 1) // UNITS, add, 0)

    if last:
        boxed = refs[-2]
        h = high_count
        row0 = (p * rows).astype(F32)
        col0 = ((q + 1) * cols).astype(F32)
        i = acc[0:h] + row0
        i = jnp.where(i >= node_rows, i - node_rows, i)
        j = acc[h : 2 * h] + col0
        j = jnp.where(j >= node_cols, j - node_cols, j)
        fields = [
            (i + 0.5) / node_rows,
            (j + 0.5) / node_cols,
            acc[2 * h : 3 * h] + acc[3 * h : 4 * h],
            acc[4 * h : 5 * h],
            acc[5 * h : 6 * h],
        ]
        for k, f in enumerate(fields):
            boxed[k, 0:h, :] = f[:, :LANES]
            boxed[k, h : 2 * h, :] = f[:, LANES:]


def scatter(steps, tile, acc, last, node_rows, node_cols, listed=None):
    _, rows, cols = tile.shape
    high_count = rows * cols // WIDE
    first = acc is None
    vmem = pl.BlockSpec(memory_space=pltpu.VMEM)
    out_shape = [pltpu.VMEM((PIECES * high_count, WIDE), F32)]
    if last:
        out_shape.append(pltpu.VMEM((5, 2 * high_count, LANES), F32))
    if first:
        near, boxes = listed.shape
        out_shape.append(jax.ShapeDtypeStruct(((2 * near + 7) // 8 * 8, boxes), jnp.int32))
    args = (tile, listed) if first else (tile, pinned(acc))
    out = pl.pallas_call(
        lambda *refs: scatter_kernel(
            first, last, (rows, cols, high_count, node_rows, node_cols), steps, *refs
        ),
        out_shape=out_shape,
        in_specs=[vmem] * len(args),
        out_specs=[vmem] * len(out_shape),
        scratch_shapes=[pltpu.SMEM((rows * cols // (8 * LANES),), jnp.int32)],
        compiler_params=pltpu.CompilerParams(vmem_limit_bytes=VMEM_LIMIT),
        name="scatter_last" if last else "scatter_first" if first else "scatter",
        cost_estimate=pl.CostEstimate(
            flops=2 * PIECES * high_count * WIDE * rows * cols // 2,
            transcendentals=0,
            bytes_accessed=4 * (2 * PIECES * high_count * WIDE + 4 * rows * cols),
        ),
    )(*args)
    return out[1] if last else out if first else out[0]


def thirds(value):
    high = rounded(value)
    middle = rounded(value - high)
    return high, middle, value - high - middle


def plan_rows(listed, plan):
    near, boxes = listed.shape
    half = near // 2
    rank = lax.axis_index("tx") * lax.axis_size("ty") + lax.axis_index("ty")
    n = listed[...] - (rank - 1) * boxes
    taken = jnp.zeros((1, boxes), jnp.int32)
    left = jnp.zeros((1, boxes), jnp.int32)
    first = [jnp.full((1, boxes), boxes, jnp.int32) for _ in range(half)]
    rest = [jnp.full((1, boxes), 3 * boxes, jnp.int32) for _ in range(near)]
    for k in range(near):
        row = n[k : k + 1, :]
        take = (row >= boxes) & (row < 2 * boxes) & (taken < half)
        first = [jnp.where(take & (taken == j), row - boxes, v) for j, v in enumerate(first)]
        rest = [jnp.where(take | (left != j), v, row) for j, v in enumerate(rest)]
        step = jnp.where(take, 1, 0)
        taken = taken + step
        left = left + 1 - step
    for j, v in enumerate(first + rest):
        plan[j : j + 1, :] = v
    down = lax.broadcasted_iota(jnp.int32, (boxes, boxes), 0)
    across = lax.broadcasted_iota(jnp.int32, (boxes, boxes), 1)
    before = jnp.where(down < across, 1.0, 0.0).astype(BF16)
    names = lax.broadcasted_iota(jnp.int32, (8, boxes), 1).astype(F32).astype(BF16)
    for pair in range(half // 2):
        over = left > half + 2 * pair
        flags = jnp.broadcast_to(jnp.where(over, 1.0, 0.0), (8, boxes)).astype(BF16)
        offset = jnp.dot(flags, before, preferred_element_type=F32)[0:1, :]
        count = jnp.dot(flags, jnp.ones((boxes, boxes), BF16), preferred_element_type=F32)[0:1, :]
        hit = jnp.where((down.astype(F32) == offset) & over, 1.0, 0.0).astype(BF16)
        found = lax.dot_general(
            names, hit, (((1,), (1,)), ((), ())), preferred_element_type=F32
        )[0:1, :].astype(jnp.int32)
        count = count.astype(jnp.int32)
        place = half + near + 2 * pair
        plan[place : place + 1, :] = jnp.where(across[0:1, :] < count, found, boxes)
        plan[place + 1 : place + 2, :] = count


def pieces_of(ref, group):
    window = (pl.ds(pl.multiple_of(8 * group, 8), 8), slice(None))
    x, y, z, pot, flux = (ref[(f,) + window] for f in range(5))
    pieces = []
    total = None
    for v in (x, y, z):
        high = rounded(v)
        low = rounded(v - high)
        kept = high + low
        pieces.append((high, low))
        total = kept * kept if total is None else total + kept * kept
    return pieces, total, pot, flux


def padded_rows(values):
    return values + [jnp.zeros_like(values[0])] * (USED - len(values))


def moment_side(ref, n):
    pitch = ref.shape[0] // STORED
    rows = ref[pl.ds(USED * pitch + n, 8, stride=pitch), :]
    zeros = jnp.zeros((8, LANES), F32)
    return jnp.concatenate([zeros, rows] + [zeros] * (FEATURES // 8 - 2), axis=0).astype(BF16)


def strided(ref, n, stored):
    pitch = ref.shape[0] // stored
    rows = [ref[pl.ds(8 * g * pitch + n, 8, stride=pitch), :] for g in range(USED // 8)]
    return jnp.concatenate(rows + [jnp.zeros((8, LANES), F32)] * ((FEATURES - USED) // 8), axis=0)


def store_sources(refs, sfeat, sflux):
    pitch = sfeat.shape[0] // STORED
    ones = jnp.ones((8, LANES), F32)
    zeros = jnp.zeros((8, LANES), F32)
    boxes = refs[0].shape[1]
    for which, ref in enumerate(refs):

        def store(group, carry):
            pieces, total, pot, flux = pieces_of(ref, group)
            source = []
            for high, low in pieces:
                source += [-2.0 * high, -2.0 * low, -2.0 * high, -2.0 * low]
            z = pieces[2][0] + pieces[2][1]
            rows = padded_rows(source + list(thirds(total)) + [ones, ones, ones])
            rows += [pot, zeros, pot, zeros] + list(thirds(-pot * z)) + [zeros]
            start = pl.multiple_of(which * boxes + 8 * group, 8)
            for k, v in enumerate(rows):
                sfeat[pl.ds(pl.multiple_of(k * pitch + start, 8), 8), :] = v
            sflux[pl.ds(start, 8), :] = flux
            return carry

        lax.fori_loop(0, boxes // 8, store, 0, unroll=2)
    start = len(refs) * boxes
    for k in range(STORED):
        sfeat[k * pitch + start : k * pitch + start + 8, :] = ones if k == 12 else zeros
    sflux[start : start + 8, :] = zeros


def store_targets(own, tfeat, turned):
    boxes = own.shape[1]
    pitch = tfeat.shape[0] // USED
    ones = jnp.ones((8, LANES), F32)

    def store(group, carry):
        pieces, total, _, _ = pieces_of(own, group)
        target = []
        for high, low in pieces:
            target += [high, high, low, low]
        for k, v in enumerate(padded_rows(target + [ones, ones, ones] + list(thirds(total + 0.04)))):
            tfeat[pl.ds(pl.multiple_of(k * pitch + 8 * group, 8), 8), :] = v
        return carry

    lax.fori_loop(0, boxes // 8, store, 0, unroll=2)
    turned[boxes] = jnp.zeros((LANES, FEATURES), BF16)

    def turn(i, carry):
        for u in range(16):
            turned[16 * i + u] = strided(tfeat, 16 * i + u, USED).T.astype(BF16)
        return carry

    lax.fori_loop(0, boxes // 16, turn, 0)


def run_items(target_of, source_of, half, iterations, turned, sfeat, sflux, sums, totals):
    empty_row = sums.shape[0] - 8
    group = totals.shape[0]

    def apply(item, total):
        target = target_of(item)
        sides = [strided(sfeat, source_of(item, k), STORED).astype(BF16) for k in range(half)]
        sides += [moment_side(sfeat, source_of(item, k)) for k in range(half)]
        squared = jnp.dot(turned[target], jnp.concatenate(sides, axis=1), preferred_element_type=F32)
        fluxes = [
            jnp.broadcast_to(sflux[pl.ds(source_of(item, k), 1), :], (8, LANES)) for k in range(half)
        ]
        for t in range(LANES // 8):
            rows = slice(8 * t, 8 * t + 8)
            value = None
            for k, flux in enumerate(fluxes):
                inverse = lax.rsqrt(squared[rows, LANES * k : LANES * (k + 1)])
                moment = squared[rows, LANES * (half + k) : LANES * (half + k + 1)]
                part = inverse * (flux - (inverse * inverse) * moment)
                value = part if value is None else value + part
            total[rows, :] = value

    def reduce(item, total, live):
        target = jnp.where(live, target_of(jnp.maximum(item, 0)), empty_row)
        sums[pl.ds(target, 1), :] += jnp.sum(total[...].T, axis=0, keepdims=True)

    def step(i, carry):
        for u in range(group):
            reduce(group * (i - 1) + u, totals.at[u], i > 0)
        for u in range(group):
            apply(group * i + u, totals.at[u])
        return carry

    totals[...] = jnp.zeros(totals.shape, F32)
    lax.fori_loop(0, iterations, step, 0)
    for u in range(group):
        reduce(group * (iterations - 1) + u, totals.at[u], iterations > 0)


def near_own_kernel(near, plan, own, sums, turned, tfeat, sfeat, sflux, totals):
    boxes = own.shape[1]
    half = near // 2
    sums[...] = jnp.zeros(sums.shape, F32)
    store_targets(own, tfeat, turned)
    store_sources([own], sfeat, sflux)

    def target_of(item):
        return jnp.minimum(item, boxes - 1)

    def source_of(item, k):
        return plan[k, jnp.minimum(item, boxes - 1)]

    run_items(
        target_of, source_of, half, boxes // OWN_GROUP, turned, sfeat, sflux, sums, totals
    )


def near_other_kernel(
    near, plan, own, lower, upper, tile, sums_in, turned, out, sums, sfeat, sflux, totals
):
    boxes = lower.shape[1]
    half = near // 2
    sums[...] = sums_in[...]
    store_sources([lower, own, upper], sfeat, sflux)

    def main_target(item):
        return jnp.clip(item, 0, boxes - 1)

    def main_source(item, k):
        return plan[half + k, main_target(item)]

    run_items(
        main_target, main_source, half, boxes // OTHER_GROUP, turned, sfeat, sflux, sums, totals
    )

    counts = [plan[half + near + 2 * pair + 1, 0] for pair in range(half // 2)]

    def extra(item):
        box, row, start = jnp.int32(boxes), jnp.int32(2 * half), jnp.int32(0)
        for pair, count in enumerate(counts):
            inside = (item >= start) & (item < start + count)
            name = plan[half + near + 2 * pair, jnp.clip(item - start, 0, boxes - 1)]
            box = jnp.where(inside, name, box)
            row = jnp.where(inside, 2 * half + 2 * pair, row)
            start = start + count
        return box, row

    def extra_source(item, k):
        box, row = extra(item)
        return plan[row + k, jnp.minimum(box, boxes - 1)]

    iterations = (sum(counts) + EXTRA_GROUP - 1) // EXTRA_GROUP
    some = totals.at[0:EXTRA_GROUP]
    run_items(
        lambda item: extra(item)[0], extra_source, 2, iterations, turned, sfeat, sflux, sums, some
    )
    out[0:boxes, :] = sums[0:boxes, :] * (1.0 / math.sqrt(near * LANES))

    _, rows, cols = tile.shape
    out[boxes : boxes + EXTRA, :] = jnp.zeros((EXTRA, LANES), F32)
    place = boxes
    for f in (1, 2):
        for r in (rows - 2, rows - 1):
            for c in range(cols // LANES):
                out[place : place + 1, :] = tile[f, r : r + 1, LANES * c : LANES * c + LANES]
                place += 1
    place = boxes + EXTRA - 8
    for f in (1, 2):
        turned_cols = tile[f, :, cols - LANES : cols].T
        out[place : place + 2, 0:rows] = turned_cols[LANES - 2 : LANES, :]
        place += 2


def item_scratch(sources, group):
    return [
        pltpu.VMEM((STORED * (sources + 8), LANES), F32),
        pltpu.VMEM((sources + 8, LANES), F32),
        pltpu.VMEM((group, LANES, LANES), F32),
    ]


def near_cost(boxes, near):
    pairs = boxes * near * LANES * LANES // 2
    return pl.CostEstimate(
        flops=pairs * 2 * FEATURES * 4, transcendentals=pairs, bytes_accessed=4 * 16 * boxes * LANES
    )


def near_own(plan, own, near):
    boxes = own.shape[1]
    assert boxes == LANES and boxes % OWN_GROUP == 0 and near % 4 == 0
    assert boxes % OTHER_GROUP == 0
    vmem = pl.BlockSpec(memory_space=pltpu.VMEM)
    smem = pl.BlockSpec(memory_space=pltpu.SMEM)
    return pl.pallas_call(
        lambda *refs: near_own_kernel(near, *refs),
        out_shape=(
            pltpu.VMEM((boxes + 8, LANES), F32),
            pltpu.VMEM((boxes + 1, LANES, FEATURES), BF16),
        ),
        in_specs=[smem, vmem],
        out_specs=(vmem,) * 2,
        scratch_shapes=[pltpu.VMEM((USED * (boxes + 8), LANES), F32)] + item_scratch(boxes, OWN_GROUP),
        compiler_params=pltpu.CompilerParams(vmem_limit_bytes=VMEM_LIMIT),
        name="near_own",
        cost_estimate=near_cost(boxes, near),
    )(plan, pinned(own))


def near_other(plan, own, lower, upper, tile, sums, turned, near):
    boxes = lower.shape[1]
    vmem = pl.BlockSpec(memory_space=pltpu.VMEM)
    smem = pl.BlockSpec(memory_space=pltpu.SMEM)
    return pl.pallas_call(
        lambda *refs: near_other_kernel(near, *refs),
        out_shape=pltpu.VMEM((boxes + EXTRA, LANES), F32),
        in_specs=[smem] + [vmem] * 6,
        out_specs=vmem,
        scratch_shapes=[pltpu.VMEM((boxes + 8, LANES), F32)] + item_scratch(3 * boxes, OTHER_GROUP),
        compiler_params=pltpu.CompilerParams(vmem_limit_bytes=VMEM_LIMIT),
        name="near_other",
        cost_estimate=near_cost(boxes, near),
    )(plan, *map(pinned, (own, lower, upper, tile, sums, turned)))


def lookup(slot, base, table, pieces, active, out):
    rows, cols = slot.shape
    high_count = rows * cols // WIDE
    across = cols // LANES
    whole = jnp.concatenate([table[0:high_count, :], table[high_count : 2 * high_count, :]], axis=1)
    top = rounded(whole)
    pieces[0:high_count, :] = top.astype(BF16)
    pieces[high_count : 2 * high_count, :] = (whole - top).astype(BF16)

    def window_of(unit):
        row, col = unit // across * 8, unit % across * LANES
        if not isinstance(unit, int):
            row, col = pl.multiple_of(row, 8), pl.multiple_of(col, LANES)
        return pl.ds(row, 8), pl.ds(col, LANES)

    def there(unit):
        high, _ = box_split(slot[window_of(unit)] - base, high_count)
        return (high >= 0.0) & (high < high_count)

    def nodes_of(i, live):
        window = window_of(active[jnp.where(live, i, 0)])
        high, low = box_split(slot[window] - base, high_count)
        return window, jnp.where(live, high, -1.0), low

    def add(i, carry):
        low_iota = lax.broadcasted_iota(jnp.int32, (WIDE, LANES), 0).astype(F32)
        high_iota = lax.broadcasted_iota(jnp.int32, (high_count, LANES), 0).astype(F32)
        units = [nodes_of(UNITS * i + u, UNITS * i + u < count) for u in range(UNITS)]
        hits = [
            jnp.where(low_iota == low[s : s + 1, :], 1.0, 0.0).astype(BF16)
            for _, _, low in units
            for s in range(8)
        ]
        picked = jnp.dot(pieces[...], jnp.concatenate(hits, axis=1), preferred_element_type=F32)
        for u, (window, high, _) in enumerate(units):
            lines = []
            for s in range(8):
                start = LANES * (8 * u + s)
                part = slice(start, start + LANES)
                value = picked[0:high_count, part] + picked[high_count : 2 * high_count, part]
                mine = high_iota == high[s : s + 1, :]
                lines.append(jnp.sum(jnp.where(mine, value, 0.0), axis=0, keepdims=True))
            out[window] += jnp.concatenate(lines, axis=0)
        return carry

    count = list_active(there, rows // 8 * across, active)
    lax.fori_loop(0, (count + UNITS - 1) // UNITS, add, 0)


def base_of(node_count, steps):
    rank = ahead("tx", -steps[0]) * lax.axis_size("ty") + ahead("ty", -steps[1])
    return (rank * node_count).astype(F32)


def own_kernel(tile, table, out, pieces, active):
    out[...] = jnp.zeros(out.shape, F32)
    lookup(tile.at[0], base_of(out.shape[0] * out.shape[1], (0, 0)), table, pieces, active, out)


def row_kernel(tile, ahead_x, partial, behind_x, out, slopes, pieces, active, padded):
    _, rows, cols = tile.shape
    boxes = rows * cols // LANES
    out[...] = partial[...]
    lookup(tile.at[0], base_of(rows * cols, (1, 0)), behind_x, pieces, active, out)
    for f in (1, 2):
        padded[8 : 8 + rows, :] = tile[f]
        for r in range(2):
            for c in range(cols // LANES):
                source = boxes + ((f - 1) * 2 + r) * (cols // LANES) + c
                padded[6 + r : 7 + r, LANES * c : LANES * c + LANES] = behind_x[source : source + 1, :]
        padded[8 + rows : 10 + rows, :] = ahead_x[f, 0:2, :]
        slopes[f - 1] = (
            padded[6 : 6 + rows, :]
            - 8.0 * padded[7 : 7 + rows, :]
            + 8.0 * padded[9 : 9 + rows, :]
            - padded[10 : 10 + rows, :]
        ) / 12.0


def col_kernel(tile, ahead_y, partial, behind_y, out, slopes, pieces, active):
    _, rows, cols = tile.shape
    boxes = rows * cols // LANES
    out[...] = partial[...]
    lookup(tile.at[0], base_of(rows * cols, (0, 1)), behind_y, pieces, active, out)
    left_cols = behind_y[boxes + EXTRA - 8 : boxes + EXTRA, 0:rows].T
    col = lax.broadcasted_iota(jnp.int32, (rows, cols), 1)
    for f in (1, 2):
        here = tile[f]
        left = left_cols[:, 2 * (f - 1) : 2 * f]
        right = ahead_y[f, :, 0:2]
        less_1 = jnp.where(col == 0, left[:, 1:2], pltpu.roll(here, 1, 1))
        less_2 = jnp.where(
            col == 0, left[:, 0:1], jnp.where(col == 1, left[:, 1:2], pltpu.roll(here, 2, 1))
        )
        more_1 = jnp.where(col == cols - 1, right[:, 0:1], pltpu.roll(here, cols - 1, 1))
        more_2 = jnp.where(
            col == cols - 2,
            right[:, 0:1],
            jnp.where(col == cols - 1, right[:, 1:2], pltpu.roll(here, cols - 2, 1)),
        )
        slopes[f - 1] = (less_2 - 8.0 * less_1 + 8.0 * more_1 - more_2) / 12.0


def last_kernel(tile, row_slopes, col_slopes, partial, behind_xy, elev_rate, pot_rate, pieces, active, total):
    _, rows, cols = tile.shape
    total[...] = partial[...]
    lookup(tile.at[0], base_of(rows * cols, (1, 1)), behind_xy, pieces, active, total)
    elev_x, pot_x = row_slopes[0], row_slopes[1]
    elev_y, pot_y = col_slopes[0], col_slopes[1]
    vertical = total[...]
    lift = 1.0 + elev_x * elev_x + elev_y * elev_y
    elev_rate[...] = vertical * lift - (pot_x * elev_x + pot_y * elev_y)
    pot_rate[...] = (
        -tile[1] - 0.5 * (pot_x * pot_x + pot_y * pot_y) + 0.5 * vertical * vertical * lift
    )


def lookup_call(kernel, name, out_shape, args, scratch):
    _, rows, cols = args[0].shape
    vmem = pl.BlockSpec(memory_space=pltpu.VMEM)
    return pl.pallas_call(
        kernel,
        out_shape=out_shape,
        in_specs=[vmem] * len(args),
        out_specs=(vmem,) * len(out_shape),
        scratch_shapes=[
            pltpu.VMEM((2 * rows * cols // WIDE, WIDE), BF16),
            pltpu.SMEM((rows * cols // (8 * LANES),), jnp.int32),
        ]
        + scratch,
        compiler_params=pltpu.CompilerParams(vmem_limit_bytes=VMEM_LIMIT),
        name=name,
        cost_estimate=pl.CostEstimate(
            flops=rows * cols * rows * cols, transcendentals=0, bytes_accessed=4 * 8 * rows * cols
        ),
    )(*map(pinned, args))


def look_up_all(tile, ahead_x, ahead_y, value, behind_x, behind_y, behind_xy):
    _, rows, cols = tile.shape
    values = pltpu.VMEM((rows, cols), F32)
    slopes = pltpu.VMEM((2, rows, cols), F32)
    (partial,) = lookup_call(own_kernel, "lookup_own", (values,), (tile, value), [])
    partial, row_slopes = lookup_call(
        row_kernel,
        "lookup_x",
        (values, slopes),
        (tile, ahead_x, partial, behind_x),
        [pltpu.VMEM((rows + 16, cols), F32)],
    )
    partial, col_slopes = lookup_call(
        col_kernel, "lookup_y", (values, slopes), (tile, ahead_y, partial, behind_y), []
    )
    shape = jax.ShapeDtypeStruct((rows, cols), F32)
    return lookup_call(
        last_kernel,
        "lookup_xy",
        (shape, shape),
        (tile, row_slopes, col_slopes, partial, behind_xy),
        [pltpu.VMEM((rows, cols), F32)],
    )


def shards(potential, elevation, normal_flux, box_owner, box_place, near_boxes):
    rows, cols = potential.shape
    count_tx = lax.axis_size("tx")
    count_ty = lax.axis_size("ty")
    node_count = rows * cols
    boxes = node_count // LANES
    near = near_boxes.shape[1]
    assert node_count % WIDE == 0 and cols <= 256 and rows <= 128
    assert 4 * (cols // LANES) <= EXTRA - 8
    assert node_count * count_tx * count_ty < 2**24

    slot = (box_owner * node_count + box_place).astype(F32)
    tile = jnp.stack([slot, elevation, potential, normal_flux])
    ahead_x = shifted(tile, "tx", -1)
    ahead_y = shifted(tile, "ty", -1)
    ahead_xy = shifted(ahead_y, "tx", -1)
    tile, ahead_x, ahead_y, ahead_xy = map(pinned, (tile, ahead_x, ahead_y, ahead_xy))

    sizes = (rows * count_tx, cols * count_ty)
    acc, plan = scatter((0, 0), tile, None, False, *sizes, near_boxes.T)
    acc = scatter((1, 0), ahead_x, acc, False, *sizes)
    acc = scatter((0, 1), ahead_y, acc, False, *sizes)
    boxed = scatter((1, 1), ahead_xy, acc, True, *sizes)

    total = count_tx * count_ty
    both = ("tx", "ty")
    lower = lax.ppermute(boxed, both, [(i, i + 1) for i in range(total - 1)])
    upper = lax.ppermute(boxed, both, [(i + 1, i) for i in range(total - 1)])

    sums, turned = near_own(plan, boxed, near)
    value = near_other(plan, boxed, lower, upper, tile, sums, turned, near)

    behind_x = shifted(value, "tx", 1)
    behind_y = shifted(value, "ty", 1)
    diagonal = [
        (i * count_ty + j, (i + 1) % count_tx * count_ty + (j + 1) % count_ty)
        for i in range(count_tx)
        for j in range(count_ty)
    ]
    behind_xy = lax.ppermute(value, both, diagonal)
    return look_up_all(tile, ahead_x, ahead_y, value, behind_x, behind_y, behind_xy)


def solution(mesh):
    in_specs = (
        P("tx", "ty"),
        P("tx", "ty"),
        P("tx", "ty"),
        P("tx", "ty"),
        P("tx", "ty"),
        P(("tx", "ty"), None),
    )
    out_specs = (P("tx", "ty"), P("tx", "ty"))
    return jax.shard_map(shards, mesh=mesh, in_specs=in_specs, out_specs=out_specs, check_vma=False)
```
